16 devices in a mesh: dp: 2 (over y, z), ctx: 8 (over x, core).
Axes of the slice: x: 4, y: 2, z: 1, core: 2. Of those that a mesh axis runs over, the one named last changes fastest.
The devices are a block of a 4x4x8 slice.
Arguments:
- x_seq: bfloat16 [1024, 2560], P(('dp', 'ctx')), parts along dimension 0
- pos_ids: int32 [1024], P(('dp', 'ctx')), parts along dimension 0
- seg_ids: int32 [1024], P(('dp', 'ctx')), parts along dimension 0
- w_dq: bfloat16 [2560, 768], replicated
- w_uq: bfloat16 [768, 2560], replicated
- w_qr: bfloat16 [768, 1280], replicated
- w_dkv: bfloat16 [2560, 256], replicated
- w_kr: bfloat16 [2560, 32], replicated
- w_uk: bfloat16 [256, 2560], replicated
- w_uv: bfloat16 [256, 2560], replicated
- w_out: bfloat16 [2560, 2560], replicated
- gain_q: bfloat16 [768], replicated
- gain_kv: bfloat16 [256], replicated
Outputs:
- output: bfloat16 [1024, 2560], P(('dp', 'ctx')), parts along dimension 0
There are 2 independent parts. The reference program is written for one: setup_inputs(seed, part) draws one part's arguments, and reference() takes and returns one part's arrays. A program takes and returns all parts, laid end to end along the dimension named above; an argument that names none is the same for every part.
All inputs are finite; a program needn't handle non-finite values.
Results may differ from the reference program's by a relative error of at most 0.00791805.
Values are sent between devices in bfloat16 or wider.
A program may use at most 768 MiB of HBM per device.

```python
import jax
import jax.numpy as jnp
from jax import lax

D_MODEL = 2560
NUM_HEADS = 40
Q_RANK = 768
KV_RANK = 256
NOPE_DIM = 64
ROPE_DIM = 32
V_DIM = 64
SEQ_DEV = 64
GROUP_SIZE = 8
NUM_DOCS = 4
NORM_EPS = 1e-6
SEQ_LEN = SEQ_DEV * GROUP_SIZE
HALF_DEV = SEQ_DEV // 2
NUM_BLOCKS = SEQ_LEN // SEQ_DEV


def draw_documents(doc_key):
    doc_cuts = jnp.sort(jax.random.permutation(doc_key, SEQ_LEN - 1)[:NUM_DOCS - 1] + 1).astype(jnp.int32)
    doc_starts = jnp.concatenate([jnp.zeros((1,), jnp.int32), doc_cuts])
    row_ids = jnp.arange(SEQ_LEN, dtype=jnp.int32)
    device_ids = row_ids // SEQ_DEV
    in_device = row_ids % SEQ_DEV
    piece_ids = jnp.where(in_device < HALF_DEV, device_ids, 2 * GROUP_SIZE - 1 - device_ids)
    token_ids = piece_ids * HALF_DEV + in_device % HALF_DEV
    seg_ids = jnp.sum((token_ids[:, None] >= doc_cuts[None, :]).astype(jnp.int32), axis=1)
    pos_ids = token_ids - doc_starts[seg_ids]
    return pos_ids.astype(jnp.int32), seg_ids.astype(jnp.int32)


def init_weight(rng_key, fan_in, fan_out):
    return (jax.random.normal(rng_key, (fan_in, fan_out), jnp.float32) * fan_in ** -0.5).astype(jnp.bfloat16)


def setup_inputs(seed: int = 0, part: int = 0) -> dict:
    root_key = jax.random.key(seed)
    part_key = jax.random.fold_in(root_key, part)
    data_keys = jax.random.split(part_key, 2)
    weight_keys = jax.random.split(root_key, 10)
    pos_ids, seg_ids = draw_documents(data_keys[1])
    x_seq = jax.random.normal(data_keys[0], (SEQ_LEN, D_MODEL), jnp.float32).astype(jnp.bfloat16)
    return {
        'x_seq': x_seq,
        'pos_ids': pos_ids,
        'seg_ids': seg_ids,
        'w_dq': init_weight(weight_keys[0], D_MODEL, Q_RANK),
        'w_uq': init_weight(weight_keys[1], Q_RANK, NUM_HEADS * NOPE_DIM),
        'w_qr': init_weight(weight_keys[2], Q_RANK, NUM_HEADS * ROPE_DIM),
        'w_dkv': init_weight(weight_keys[3], D_MODEL, KV_RANK),
        'w_kr': init_weight(weight_keys[4], D_MODEL, ROPE_DIM),
        'w_uk': init_weight(weight_keys[5], KV_RANK, NUM_HEADS * NOPE_DIM),
        'w_uv': init_weight(weight_keys[6], KV_RANK, NUM_HEADS * V_DIM),
        'w_out': init_weight(weight_keys[7], NUM_HEADS * V_DIM, D_MODEL),
        'gain_q': jax.random.uniform(weight_keys[8], (Q_RANK,), jnp.float32, 0.5, 1.5).astype(jnp.bfloat16),
        'gain_kv': jax.random.uniform(weight_keys[9], (KV_RANK,), jnp.float32, 0.5, 1.5).astype(jnp.bfloat16),
    }


def rms_norm(vals, gain):
    mean_sq = jnp.mean(vals * vals, axis=-1, keepdims=True)
    return (vals * lax.rsqrt(mean_sq + NORM_EPS) * gain.astype(jnp.float32)).astype(jnp.bfloat16)


def rope_tables(pos_ids):
    half_dim = ROPE_DIM // 2
    inv_freq = 10000.0 ** (-2.0 * jnp.arange(half_dim, dtype=jnp.float32) / ROPE_DIM)
    angles = pos_ids.astype(jnp.float32)[:, None] * inv_freq[None, :]
    return jnp.cos(angles), jnp.sin(angles)


def apply_rope(vals, cos_tab, sin_tab):
    half_dim = vals.shape[-1] // 2
    lead_half = vals[..., :half_dim]
    tail_half = vals[..., half_dim:]
    return jnp.concatenate([lead_half * cos_tab - tail_half * sin_tab, tail_half * cos_tab + lead_half * sin_tab], axis=-1)


def reference(x_seq, pos_ids, seg_ids, w_dq, w_uq, w_qr, w_dkv, w_kr, w_uk, w_uv, w_out, gain_q, gain_kv):
    cos_tab, sin_tab = rope_tables(pos_ids)
    c_q = rms_norm(jnp.dot(x_seq, w_dq, preferred_element_type=jnp.float32), gain_q)
    q_nope = jnp.dot(c_q, w_uq, preferred_element_type=jnp.float32).astype(jnp.bfloat16)
    q_rope = jnp.dot(c_q, w_qr, preferred_element_type=jnp.float32).reshape(SEQ_LEN, NUM_HEADS, ROPE_DIM)
    q_rope = apply_rope(q_rope, cos_tab[:, None, :], sin_tab[:, None, :]).astype(jnp.bfloat16)
    c_kv = rms_norm(jnp.dot(x_seq, w_dkv, preferred_element_type=jnp.float32), gain_kv)
    k_rope = apply_rope(jnp.dot(x_seq, w_kr, preferred_element_type=jnp.float32), cos_tab, sin_tab)
    k_rope = k_rope.astype(jnp.bfloat16).astype(jnp.float32)
    score_scale = (NOPE_DIM + ROPE_DIM) ** -0.5
    head_inputs = (
        q_nope.reshape(SEQ_LEN, NUM_HEADS, NOPE_DIM).transpose(1, 0, 2).reshape(NUM_HEADS, NUM_BLOCKS, SEQ_DEV, NOPE_DIM),
        q_rope.transpose(1, 0, 2).reshape(NUM_HEADS, NUM_BLOCKS, SEQ_DEV, ROPE_DIM),
        w_uk.reshape(KV_RANK, NUM_HEADS, NOPE_DIM).transpose(1, 0, 2),
        w_uv.reshape(KV_RANK, NUM_HEADS, V_DIM).transpose(1, 0, 2),
    )
    block_pos = pos_ids.reshape(NUM_BLOCKS, SEQ_DEV)
    block_seg = seg_ids.reshape(NUM_BLOCKS, SEQ_DEV)

    def one_head(head_args):
        q_nope_h, q_rope_h, w_uk_h, w_uv_h = head_args
        k_nope = jnp.dot(c_kv, w_uk_h, preferred_element_type=jnp.float32).astype(jnp.bfloat16).astype(jnp.float32)
        v_head = jnp.dot(c_kv, w_uv_h, preferred_element_type=jnp.float32).astype(jnp.bfloat16).astype(jnp.float32)

        def one_block(block_args):
            qn_blk, qr_blk, pos_blk, seg_blk = block_args
            scores = jnp.dot(qn_blk.astype(jnp.float32), k_nope.T) + jnp.dot(qr_blk.astype(jnp.float32), k_rope.T)
            allowed = (pos_ids[None, :] <= pos_blk[:, None]) & (seg_ids[None, :] == seg_blk[:, None])
            scores = jnp.where(allowed, scores * score_scale, -jnp.inf)
            weights = jnp.exp(scores - jnp.max(scores, axis=1, keepdims=True))
            return (jnp.dot(weights, v_head) / jnp.sum(weights, axis=1, keepdims=True)).astype(jnp.bfloat16)

        return lax.map(one_block, (q_nope_h, q_rope_h, block_pos, block_seg))

    head_out = lax.map(one_head, head_inputs)
    attn_out = head_out.reshape(NUM_HEADS, SEQ_LEN, V_DIM).transpose(1, 0, 2).reshape(SEQ_LEN, NUM_HEADS * V_DIM)
    return jnp.dot(attn_out, w_out, preferred_element_type=jnp.float32).astype(jnp.bfloat16)
```

```python
import functools
import math

import jax
import jax.numpy as jnp
import numpy as np
from jax import lax
from jax.experimental import pallas as pl
from jax.experimental.pallas import tpu as pltpu
from jax.sharding import PartitionSpec as P

NORM_EPS = 1e-6
MASKED = -1e30
LANES = 128
PACK_ROWS = 16
MESH = pl.DeviceIdType.MESH
NT = (((1,), (1,)), ((), ()))
TT = (((0,), (1,)), ((), ()))


def mm(a, b, dims=(((1,), (0,)), ((), ()))):
    return lax.dot_general(a, b, dims, preferred_element_type=jnp.float32)


def rms_norm(vals, gain):
    mean_sq = jnp.mean(vals * vals, axis=-1, keepdims=True)
    return (vals * lax.rsqrt(mean_sq + NORM_EPS) * gain).astype(jnp.bfloat16)


def iota(shape, dim):
    return lax.broadcasted_iota(jnp.int32, shape, dim)


def layer_kernel(n, x_h, pos_h, wdq_h, wuq_h, wqr_h, wdkv_h, wkr_h, wuk_h, wuv_h, wout_h, gq_h, gkv_h, y_h,
                 x_v, pos_v, wdq_v, wuq_v, wqr_v, wdkv_v, wkr_v, wuk_v, wuv_v, wout_v, gq_v, gkv_v,
                 lat, cq_v, qcat, kcat, kr_v, vt, bias_v, o_v, y_v, in_sem, y_sem, send_sem, recv_sem):
    rows, width = x_v.shape
    kv_rank = wdkv_v.shape[1]
    rope = wkr_v.shape[1]
    half_rope = rope // 2
    pairs = kcat.shape[0]
    nope = LANES // 2
    keys = n * rows
    half = rows // 2
    out_chunk = width // y_sem.shape[0]

    me = lax.axis_index("ctx")
    partner = me + 1 - 2 * lax.rem(me, 2)
    others = [lax.rem(me + 2 * k, n) for k in range(1, n // 2)]

    copies = []

    def fetch(src, dst):
        cp = pltpu.make_async_copy(src, dst, in_sem.at[len(copies)])
        cp.start()
        copies.append(cp)
        return cp

    get_pos = fetch(pos_h, pos_v)
    get_x = fetch(x_h, x_v)
    get_wkr = fetch(wkr_h, wkr_v)
    get_wdkv = fetch(wdkv_h, wdkv_v)
    get_gkv = fetch(gkv_h, gkv_v)
    get_gq = fetch(gq_h, gq_v)
    get_wdq = fetch(wdq_h, wdq_v)
    get_wuq = fetch(wuq_h, wuq_v)
    get_wqr = fetch(wqr_h, wqr_v)
    get_wuk = fetch(wuk_h, wuk_v)
    get_wuv = fetch(wuv_h, wuv_v)
    get_wout = [fetch(wout_h.at[:, pl.ds(c * out_chunk, out_chunk)], wout_v.at[:, pl.ds(c * out_chunk, out_chunk)])
                for c in range(y_sem.shape[0])]

    barrier = pltpu.get_barrier_semaphore()
    for peer in [partner] + others:
        pl.semaphore_signal(barrier, inc=1, device_id={"ctx": peer}, device_id_type=MESH)

    get_pos.wait()
    pos_row = pos_v[...].astype(jnp.float32)
    diag = iota((rows, rows), 0) == iota((rows, rows), 1)
    pos_col = jnp.sum(jnp.where(diag, jnp.broadcast_to(pos_row, (rows, rows)), 0.0), axis=1, keepdims=True)
    lane = iota((rows, LANES), 1)
    freq_id = lax.rem(lane, half_rope)
    inv_freq = jnp.zeros((rows, LANES), jnp.float32)
    for f in range(half_rope):
        inv_freq = jnp.where(freq_id == f, float(np.float32(10000.0 ** (-2.0 * f / rope))), inv_freq)
    angles = pos_col * inv_freq
    first = lax.rem(lane, rope) < half_rope
    cos_tab = jnp.cos(angles)
    sin_tab = jnp.sin(angles)
    sin_tab = jnp.where(first, -sin_tab, sin_tab)

    def rope_lanes(a):
        other = jnp.where(first, pltpu.roll(a, LANES - half_rope, 1), pltpu.roll(a, half_rope, 1))
        return (a * cos_tab + other * sin_tab).astype(jnp.bfloat16)

    q_row = iota((rows, LANES), 0)
    q_lane = lax.rem(lane, rows)
    pos_lane = jnp.sum(jnp.where(q_row == q_lane, jnp.broadcast_to(pos_col, (rows, LANES)), 0.0), axis=0, keepdims=True)
    q_lane = q_lane[:1]
    q_seq = jnp.where(q_lane < half, half * me + q_lane, half * (2 * n - 2 - me) + q_lane)
    q_first = q_seq - pos_lane.astype(jnp.int32)
    k_row = iota((keys, LANES), 0)
    k_dev = k_row // rows
    k_in = lax.rem(k_row, rows)
    k_seq = jnp.where(k_in < half, half * k_dev + k_in, half * (2 * n - 2 - k_dev) + k_in)
    bias_v[...] = jnp.where((k_seq >= q_first) & (k_seq <= q_seq), 0.0, MASKED)

    get_x.wait()
    get_wkr.wait()
    kr = mm(x_v[...], wkr_v[...])
    get_wdkv.wait()
    kv = mm(x_v[...], wdkv_v[...])
    get_gkv.wait()
    lat[me, :rows, :] = rms_norm(kv, gkv_v[...].astype(jnp.float32))
    kr = rope_lanes(jnp.concatenate([kr] * (LANES // rope), axis=1))
    packed = jnp.zeros((PACK_ROWS, LANES), jnp.bfloat16)
    slot = iota((PACK_ROWS, LANES), 1) // rope
    for s in range(rows // PACK_ROWS):
        packed = jnp.where(slot == s, kr[s * PACK_ROWS:(s + 1) * PACK_ROWS], packed)
    lat[me, rows:, :LANES] = packed
    lat[me, rows:, LANES:] = jnp.zeros((PACK_ROWS, kv_rank - LANES), jnp.bfloat16)

    pl.semaphore_wait(barrier, n // 2)

    def send(block, peer, index):
        cp = pltpu.make_async_remote_copy(src_ref=lat.at[block], dst_ref=lat.at[block], send_sem=send_sem.at[index],
                                          recv_sem=recv_sem.at[block], device_id={"ctx": peer}, device_id_type=MESH)
        cp.start()
        return cp

    sends = [send(me, peer, k) for k, peer in enumerate(others)]
    sends.append(send(me, partner, len(sends)))

    get_gq.wait()
    get_wdq.wait()
    cq_v[...] = rms_norm(mm(x_v[...], wdq_v[...]), gq_v[...].astype(jnp.float32))
    get_wuq.wait()
    low = lane < nope
    zero = jnp.zeros((rows, LANES), jnp.bfloat16)
    for c in range(pairs // 4):
        q = mm(cq_v[...], wuq_v[:, c * 4 * LANES:(c + 1) * 4 * LANES]).astype(jnp.bfloat16)
        for i in range(4):
            t = q[:, i * LANES:(i + 1) * LANES]
            qcat[c * 4 + i, :rows, :LANES] = jnp.where(low, t, zero)
            qcat[c * 4 + i, rows:, :LANES] = jnp.where(low, zero, t)
    get_wqr.wait()
    per = LANES // rope
    for c in range(pairs * 2 // per // 2):
        q = mm(cq_v[...], wqr_v[:, c * 2 * LANES:(c + 1) * 2 * LANES])
        for i in range(2):
            t = rope_lanes(q[:, i * LANES:(i + 1) * LANES])
            for s in range(per):
                head = (c * 2 + i) * per + s
                at = head % 2 * rows
                qcat[head // 2, at:at + rows, LANES:] = jnp.where(lane // rope == s, t, zero)

    def arrived(block):
        pltpu.make_async_remote_copy(src_ref=lat.at[block], dst_ref=lat.at[block], send_sem=send_sem.at[0],
                                     recv_sem=recv_sem.at[block], device_id={"ctx": partner}, device_id_type=MESH).wait_recv()

    for block in others:
        arrived(block)
        sends.append(send(block, partner, len(sends)))
    arrived(partner)
    for k in range(1, n // 2):
        arrived(lax.rem(partner + 2 * k, n))

    c_all = lat[:, :rows, :].reshape(keys, kv_rank)
    packs = lat[:, rows:, :LANES]
    pslot = iota((n, PACK_ROWS, LANES), 2) // rope
    spread = jnp.stack([jnp.where(pslot == s, packs, jnp.zeros_like(packs)) for s in range(rows // PACK_ROWS)], axis=1)
    same = lax.rem(iota((LANES, LANES), 0), rope) == lax.rem(iota((LANES, LANES), 1), rope)
    kr_v[...] = mm(spread.reshape(keys, LANES), jnp.where(same, 1.0, 0.0).astype(jnp.bfloat16)).astype(jnp.bfloat16)
    get_wuk.wait()
    for c in range(pairs // 2):
        k = mm(c_all, wuk_v[:, c * 2 * LANES:(c + 1) * 2 * LANES]).astype(jnp.bfloat16)
        kcat[2 * c] = k[:, :LANES]
        kcat[2 * c + 1] = k[:, LANES:]
    get_wuv.wait()
    for c in range(pairs // 2):
        cols = slice(c * 2 * LANES, (c + 1) * 2 * LANES)
        vt[cols, :] = mm(wuv_v[:, cols], c_all, TT).astype(jnp.bfloat16)

    factor = (nope + rope) ** -0.5 * math.log2(math.e)

    def attend(p, carry):
        k = jnp.concatenate([kcat[p], kr_v[...]], axis=1)
        t = mm(k, qcat[p], NT) * factor + bias_v[...]
        m = jnp.max(t, axis=0, keepdims=True)
        e = jnp.exp2(t - m)
        total = jnp.sum(e, axis=0, keepdims=True)
        cols = pl.ds(pl.multiple_of(p * LANES, LANES), LANES)
        o = (mm(vt[cols, :], e.astype(jnp.bfloat16)) * (1.0 / total)).T
        o_v[:, cols] = jnp.where(low, o[:rows], o[rows:]).astype(jnp.bfloat16)
        return carry

    lax.fori_loop(0, pairs, attend, 0, unroll=2)

    puts = []
    for c, get in enumerate(get_wout):
        cols = slice(c * out_chunk, (c + 1) * out_chunk)
        get.wait()
        y_v[:, cols] = mm(o_v[...], wout_v[:, cols]).astype(jnp.bfloat16)
        put = pltpu.make_async_copy(y_v.at[:, cols], y_h.at[:, cols], y_sem.at[c])
        put.start()
        puts.append(put)
    for cp in sends:
        cp.wait_send()
    for put in puts:
        put.wait()


def solution(mesh):
    n = mesh.shape["ctx"]
    row_spec = P(("dp", "ctx"), None)
    id_spec = P(("dp", "ctx"))

    def per_device(x, pos, seg, w_dq, w_uq, w_qr, w_dkv, w_kr, w_uk, w_uv, w_out, gain_q, gain_kv):
        rows, width = x.shape
        pairs = w_uq.shape[1] // LANES
        keys = n * rows
        kv_rank = w_dkv.shape[1]
        bf, f32 = jnp.bfloat16, jnp.float32
        args = (x, pos.reshape(1, rows), w_dq, w_uq, w_qr, w_dkv, w_kr, w_uk, w_uv, w_out,
                gain_q.reshape(1, -1), gain_kv.reshape(1, -1))
        out_chunks = 5
        scratch = [pltpu.VMEM(a.shape, a.dtype) for a in args]
        scratch += [
            pltpu.VMEM((n, rows + PACK_ROWS, kv_rank), bf),
            pltpu.VMEM((rows, w_dq.shape[1]), bf),
            pltpu.VMEM((pairs, 2 * rows, 2 * LANES), bf),
            pltpu.VMEM((pairs, keys, LANES), bf),
            pltpu.VMEM((keys, LANES), bf),
            pltpu.VMEM((w_uv.shape[1], keys), bf),
            pltpu.VMEM((keys, LANES), f32),
            pltpu.VMEM((rows, w_uv.shape[1]), bf),
            pltpu.VMEM((rows, width), bf),
            pltpu.SemaphoreType.DMA((len(args) - 1 + out_chunks,)),
            pltpu.SemaphoreType.DMA((out_chunks,)),
            pltpu.SemaphoreType.DMA((n - 1,)),
            pltpu.SemaphoreType.DMA((n,)),
        ]
        return pl.pallas_call(
            functools.partial(layer_kernel, n),
            out_shape=jax.ShapeDtypeStruct(x.shape, bf),
            in_specs=[pl.BlockSpec(memory_space=pl.ANY)] * len(args),
            out_specs=pl.BlockSpec(memory_space=pl.ANY),
            scratch_shapes=scratch,
            compiler_params=pltpu.CompilerParams(collective_id=0, has_side_effects=True, vmem_limit_bytes=60 << 20),
        )(*args)

    return jax.shard_map(per_device, mesh=mesh, in_specs=(row_spec, id_spec, id_spec) + (P(),) * 10, out_specs=row_spec, check_vma=False)
```

```python
import functools
import math

import jax
import jax.numpy as jnp
import numpy as np
from jax import lax
from jax.experimental import pallas as pl
from jax.experimental.pallas import tpu as pltpu
from jax.sharding import PartitionSpec as P

NORM_EPS = 1e-6
MASKED = -1e30
LANES = 128
PACK_ROWS = 16
GROUP = 2
OUT_CHUNKS = 5
MESH = pl.DeviceIdType.MESH
NT = (((1,), (1,)), ((), ()))
TT = (((0,), (1,)), ((), ()))


def mm(a, b, dims=(((1,), (0,)), ((), ()))):
    return lax.dot_general(a, b, dims, preferred_element_type=jnp.float32)


def rms_norm(vals, gain):
    mean_sq = jnp.mean(vals * vals, axis=-1, keepdims=True)
    return (vals * lax.rsqrt(mean_sq + NORM_EPS) * gain).astype(jnp.bfloat16)


def iota(shape, dim):
    return lax.broadcasted_iota(jnp.int32, shape, dim)


def layer_kernel(n, x_h, pos_h, wdq_h, wuq_h, wqr_h, wdkv_h, wkr_h, wuk_h, wuv_h, wout_h, gq_h, gkv_h, y_v,
                 x_v, pos_v, wdq_v, wuq_v, wqr_v, wdkv_v, wkr_v, wuk_v, wuv_v, wout_v, gq_v, gkv_v,
                 lat, cq_v, qcat, kcat, kr_v, vt, bias_v, o_v, s_v, m_v, p_v, l_v, in_sem, send_sem, recv_sem):
    rows, width = x_v.shape
    kv_rank = wdkv_v.shape[1]
    rope = wkr_v.shape[0]
    half_rope = rope // 2
    pairs = kcat.shape[0]
    nope = LANES // 2
    keys = n * rows
    half = rows // 2
    out_chunk = width // OUT_CHUNKS

    me = lax.axis_index("ctx")
    partner = me + 1 - 2 * lax.rem(me, 2)
    others = [lax.rem(me + 2 * k, n) for k in range(1, n // 2)]

    copies = []

    def fetch(src, dst):
        cp = pltpu.make_async_copy(src, dst, in_sem.at[len(copies)])
        cp.start()
        copies.append(cp)
        return cp

    get_pos = fetch(pos_h, pos_v)
    get_x = fetch(x_h, x_v)
    get_wkr = fetch(wkr_h, wkr_v)
    get_wdkv = fetch(wdkv_h, wdkv_v)
    get_gkv = fetch(gkv_h, gkv_v)
    get_gq = fetch(gq_h, gq_v)
    get_wdq = fetch(wdq_h, wdq_v)
    get_wuq = fetch(wuq_h, wuq_v)
    get_wqr = fetch(wqr_h, wqr_v)
    get_wuk = fetch(wuk_h, wuk_v)
    get_wuv = fetch(wuv_h, wuv_v)
    get_wout = [fetch(wout_h.at[:, pl.ds(c * out_chunk, out_chunk)], wout_v.at[:, pl.ds(c * out_chunk, out_chunk)])
                for c in range(OUT_CHUNKS)]

    barrier = pltpu.get_barrier_semaphore()
    for peer in [partner] + others:
        pl.semaphore_signal(barrier, inc=1, device_id={"ctx": peer}, device_id_type=MESH)

    get_pos.wait()
    pos_row = pos_v[...].astype(jnp.float32)
    diag = iota((rows, rows), 0) == iota((rows, rows), 1)
    pos_col = jnp.sum(jnp.where(diag, jnp.broadcast_to(pos_row, (rows, rows)), 0.0), axis=1, keepdims=True)
    lane = iota((rows, LANES), 1)
    freq_id = lax.rem(lane, half_rope)
    inv_freq = jnp.zeros((rows, LANES), jnp.float32)
    for f in range(half_rope):
        inv_freq = jnp.where(freq_id == f, float(np.float32(10000.0 ** (-2.0 * f / rope))), inv_freq)
    angles = pos_col * inv_freq
    first = lax.rem(lane, rope) < half_rope
    cos_tab = jnp.cos(angles)
    sin_tab = jnp.sin(angles)
    sin_tab = jnp.where(first, -sin_tab, sin_tab)

    def rope_lanes(a):
        other = jnp.where(first, pltpu.roll(a, LANES - half_rope, 1), pltpu.roll(a, half_rope, 1))
        return (a * cos_tab + other * sin_tab).astype(jnp.bfloat16)

    q_row = iota((rows, LANES), 0)
    q_lane = lax.rem(lane, rows)
    pos_lane = jnp.sum(jnp.where(q_row == q_lane, jnp.broadcast_to(pos_col, (rows, LANES)), 0.0), axis=0, keepdims=True)
    q_lane = q_lane[:1]
    q_seq = jnp.where(q_lane < half, half * me + q_lane, half * (2 * n - 2 - me) + q_lane)
    q_first = q_seq - pos_lane.astype(jnp.int32)
    k_row = iota((keys, LANES), 0)
    k_dev = k_row // rows
    k_in = lax.rem(k_row, rows)
    k_seq = jnp.where(k_in < half, half * k_dev + k_in, half * (2 * n - 2 - k_dev) + k_in)
    bias_v[...] = jnp.where((k_seq >= q_first) & (k_seq <= q_seq), 0.0, MASKED)

    get_x.wait()
    get_wkr.wait()
    kr = mm(x_v[...], wkr_v[...], NT)
    get_wdkv.wait()
    kv = mm(x_v[...], wdkv_v[...])
    get_gkv.wait()
    lat[me, :rows, :] = rms_norm(kv, gkv_v[...].astype(jnp.float32).reshape(1, -1))
    kr = rope_lanes(jnp.concatenate([kr] * (LANES // rope), axis=1))
    packed = jnp.zeros((PACK_ROWS, LANES), jnp.bfloat16)
    slot = iota((PACK_ROWS, LANES), 1) // rope
    for s in range(rows // PACK_ROWS):
        packed = jnp.where(slot == s, kr[s * PACK_ROWS:(s + 1) * PACK_ROWS], packed)
    lat[me, rows:, :LANES] = packed
    lat[me, rows:, LANES:] = jnp.zeros((PACK_ROWS, kv_rank - LANES), jnp.bfloat16)

    pl.semaphore_wait(barrier, n // 2)

    def send(block, peer, index):
        cp = pltpu.make_async_remote_copy(src_ref=lat.at[block], dst_ref=lat.at[block], send_sem=send_sem.at[index],
                                          recv_sem=recv_sem.at[block], device_id={"ctx": peer}, device_id_type=MESH)
        cp.start()
        return cp

    sends = [send(me, peer, k) for k, peer in enumerate(others)]
    sends.append(send(me, partner, len(sends)))

    get_gq.wait()
    get_wdq.wait()
    cq_v[...] = rms_norm(mm(x_v[...], wdq_v[...]), gq_v[...].astype(jnp.float32).reshape(1, -1))
    get_wuq.wait()
    low = lane < nope
    zero = jnp.zeros((rows, LANES), jnp.bfloat16)
    for c in range(pairs // 4):
        q = mm(cq_v[...], wuq_v[:, c * 4 * LANES:(c + 1) * 4 * LANES]).astype(jnp.bfloat16)
        for i in range(4):
            t = q[:, i * LANES:(i + 1) * LANES]
            qcat[c * 4 + i, :rows, :LANES] = jnp.where(low, t, zero)
            qcat[c * 4 + i, rows:, :LANES] = jnp.where(low, zero, t)
    get_wqr.wait()
    per = LANES // rope
    for c in range(pairs * 2 // per // 2):
        q = mm(cq_v[...], wqr_v[:, c * 2 * LANES:(c + 1) * 2 * LANES])
        for i in range(2):
            t = rope_lanes(q[:, i * LANES:(i + 1) * LANES])
            for s in range(per):
                head = (c * 2 + i) * per + s
                at = head % 2 * rows
                qcat[head // 2, at:at + rows, LANES:] = jnp.where(lane // rope == s, t, zero)

    def arrived(block):
        pltpu.make_async_remote_copy(src_ref=lat.at[block], dst_ref=lat.at[block], send_sem=send_sem.at[0],
                                     recv_sem=recv_sem.at[block], device_id={"ctx": partner}, device_id_type=MESH).wait_recv()

    for block in others:
        arrived(block)
        sends.append(send(block, partner, len(sends)))
    arrived(partner)
    for k in range(1, n // 2):
        arrived(lax.rem(partner + 2 * k, n))

    c_all = lat[:, :rows, :].reshape(keys, kv_rank)
    packs = lat[:, rows:, :LANES]
    pslot = iota((n, PACK_ROWS, LANES), 2) // rope
    spread = jnp.stack([jnp.where(pslot == s, packs, jnp.zeros_like(packs)) for s in range(rows // PACK_ROWS)], axis=1)
    same = lax.rem(iota((LANES, LANES), 0), rope) == lax.rem(iota((LANES, LANES), 1), rope)
    kr_v[...] = mm(spread.reshape(keys, LANES), jnp.where(same, 1.0, 0.0).astype(jnp.bfloat16)).astype(jnp.bfloat16)
    get_wuk.wait()
    for c in range(pairs // 2):
        k = mm(c_all, wuk_v[:, c * 2 * LANES:(c + 1) * 2 * LANES]).astype(jnp.bfloat16)
        kcat[2 * c] = k[:, :LANES]
        kcat[2 * c + 1] = k[:, LANES:]
    get_wuv.wait()
    for c in range(pairs // 2):
        cols = slice(c * 2 * LANES, (c + 1) * 2 * LANES)
        vt[cols, :] = mm(wuv_v[:, cols], c_all, TT).astype(jnp.bfloat16)

    factor = (nope + rope) ** -0.5 * math.log2(math.e)
    steps = pairs // GROUP

    def scores(g):
        for i in range(GROUP):
            k = jnp.concatenate([kcat[g * GROUP + i], kr_v[...]], axis=1)
            t = mm(k, qcat[g * GROUP + i], NT) * factor + bias_v[...]
            s_v[g % 2, i] = t
            m_v[g % 2, i] = jnp.max(t, axis=0, keepdims=True)

    def weights(g):
        for i in range(GROUP):
            e = jnp.exp2(s_v[g % 2, i] - m_v[g % 2, i])
            p_v[g % 2, i] = e.astype(jnp.bfloat16)
            l_v[g % 2, i] = 1.0 / jnp.sum(e, axis=0, keepdims=True)

    def values(g):
        for i in range(GROUP):
            cols = slice((g * GROUP + i) * LANES, (g * GROUP + i + 1) * LANES)
            o = (mm(vt[cols, :], p_v[g % 2, i]) * l_v[g % 2, i]).T
            o_v[:, cols] = jnp.where(low, o[:rows], o[rows:]).astype(jnp.bfloat16)

    for g in range(steps + 2):
        if g >= 2:
            values(g - 2)
        if 1 <= g <= steps:
            weights(g - 1)
        if g < steps:
            scores(g)

    for get in get_wout:
        get.wait()
    for c in range(len(get_wout)):
        cols = slice(c * out_chunk, (c + 1) * out_chunk)
        y_v[:, cols] = mm(o_v[...], wout_v[:, cols]).astype(jnp.bfloat16)
    for cp in sends:
        cp.wait_send()


def solution(mesh):
    n = mesh.shape["ctx"]
    row_spec = P(("dp", "ctx"), None)
    id_spec = P(("dp", "ctx"))

    def per_device(x, pos, seg, w_dq, w_uq, w_qr, w_dkv, w_kr, w_uk, w_uv, w_out, gain_q, gain_kv):
        rows, width = x.shape
        pairs = w_uq.shape[1] // LANES
        keys = n * rows
        kv_rank = w_dkv.shape[1]
        bf, f32 = jnp.bfloat16, jnp.float32
        args = (x, pos.reshape(1, rows), w_dq, w_uq, w_qr, w_dkv, w_kr.T, w_uk, w_uv, w_out,
                gain_q, gain_kv)
        scratch = [pltpu.VMEM(a.shape, a.dtype) for a in args]
        scratch += [
            pltpu.VMEM((n, rows + PACK_ROWS, kv_rank), bf),
            pltpu.VMEM((rows, w_dq.shape[1]), bf),
            pltpu.VMEM((pairs, 2 * rows, 2 * LANES), bf),
            pltpu.VMEM((pairs, keys, LANES), bf),
            pltpu.VMEM((keys, LANES), bf),
            pltpu.VMEM((w_uv.shape[1], keys), bf),
            pltpu.VMEM((keys, LANES), f32),
            pltpu.VMEM((rows, w_uv.shape[1]), bf),
            pltpu.VMEM((2, GROUP, keys, LANES), f32),
            pltpu.VMEM((2, GROUP, 1, LANES), f32),
            pltpu.VMEM((2, GROUP, keys, LANES), bf),
            pltpu.VMEM((2, GROUP, 1, LANES), f32),
            pltpu.SemaphoreType.DMA((len(args) - 1 + OUT_CHUNKS,)),
            pltpu.SemaphoreType.DMA((n - 1,)),
            pltpu.SemaphoreType.DMA((n,)),
        ]
        return pl.pallas_call(
            functools.partial(layer_kernel, n),
            out_shape=jax.ShapeDtypeStruct(x.shape, bf),
            in_specs=[pl.BlockSpec(memory_space=pltpu.HBM)] * len(args),
            out_specs=pl.BlockSpec(memory_space=pltpu.VMEM),
            scratch_shapes=scratch,
            compiler_params=pltpu.CompilerParams(collective_id=0, has_side_effects=True, vmem_limit_bytes=62000000),
        )(*args)

    return jax.shard_map(per_device, mesh=mesh, in_specs=(row_spec, id_spec, id_spec) + (P(),) * 10, out_specs=row_spec, check_vma=False)
```

```python
import functools
import math

import jax
import jax.numpy as jnp
import numpy as np
from jax import lax
from jax.experimental import pallas as pl
from jax.experimental.pallas import tpu as pltpu
from jax.sharding import PartitionSpec as P

NORM_EPS = 1e-6
MASKED = -1e30
LANES = 128
PACK_ROWS = 16
GROUP = 2
OUT_CHUNKS = 5
MESH = pl.DeviceIdType.MESH
NT = (((1,), (1,)), ((), ()))
TT = (((0,), (1,)), ((), ()))


def mm(a, b, dims=(((1,), (0,)), ((), ()))):
    return lax.dot_general(a, b, dims, preferred_element_type=jnp.float32)


def rms_norm(vals, gain):
    mean_sq = jnp.mean(vals * vals, axis=-1, keepdims=True)
    return (vals * lax.rsqrt(mean_sq + NORM_EPS) * gain).astype(jnp.bfloat16)


def iota(shape, dim):
    return lax.broadcasted_iota(jnp.int32, shape, dim)


def layer_kernel(n, x_h, pos_h, wdq_h, wuq_h, wqr_h, wdkv_h, wkr_h, wuk_h, wuv_h, wout_h, gq_h, gkv_h, y_v,
                 x_v, pos_v, wdq_v, wuq_v, wqr_v, wdkv_v, wkr_v, wuk_v, wuv_v, wout_v, gq_v, gkv_v,
                 lat, cq_v, qcat, kcat, kr_v, vt, bias_v, o_v, s_v, m_v, p_v, l_v, in_sem, send_sem, recv_sem):
    rows, width = x_v.shape
    kv_rank = wdkv_v.shape[1]
    rope = wkr_v.shape[0]
    half_rope = rope // 2
    pairs = kcat.shape[0]
    nope = LANES // 2
    keys = n * rows
    half = rows // 2
    out_chunk = width // OUT_CHUNKS

    me = lax.axis_index("ctx")
    partner = me + 1 - 2 * lax.rem(me, 2)
    others = [lax.rem(me + 2 * k, n) for k in range(1, n // 2)]

    fetches = []

    def fetch(src, dst):
        fetches.append(pltpu.make_async_copy(src, dst, in_sem.at[len(fetches)]))
        return fetches[-1]

    def start(*copies):
        for cp in copies:
            cp.start()

    get_pos = fetch(pos_h, pos_v)
    get_x = fetch(x_h, x_v)
    get_wkr = fetch(wkr_h, wkr_v)
    get_wdkv = fetch(wdkv_h, wdkv_v)
    get_gkv = fetch(gkv_h, gkv_v)
    get_gq = fetch(gq_h, gq_v)
    get_wdq = fetch(wdq_h, wdq_v)
    get_wuq = fetch(wuq_h, wuq_v)
    get_wqr = fetch(wqr_h, wqr_v)
    get_wuk = fetch(wuk_h, wuk_v)
    get_wuv = fetch(wuv_h, wuv_v)
    get_wout = [fetch(wout_h.at[:, pl.ds(c * out_chunk, out_chunk)], wout_v.at[:, pl.ds(c * out_chunk, out_chunk)])
                for c in range(OUT_CHUNKS)]
    start(get_pos, get_x, get_wkr, get_wdkv, get_gkv, get_gq, get_wdq)

    barrier = pltpu.get_barrier_semaphore()
    for peer in [partner] + others:
        pl.semaphore_signal(barrier, inc=1, device_id={"ctx": peer}, device_id_type=MESH)

    get_pos.wait()
    pos_row = pos_v[...].astype(jnp.float32)
    diag = iota((rows, rows), 0) == iota((rows, rows), 1)
    pos_col = jnp.sum(jnp.where(diag, jnp.broadcast_to(pos_row, (rows, rows)), 0.0), axis=1, keepdims=True)
    lane = iota((rows, LANES), 1)
    freq_id = lax.rem(lane, half_rope)
    inv_freq = jnp.zeros((rows, LANES), jnp.float32)
    for f in range(half_rope):
        inv_freq = jnp.where(freq_id == f, float(np.float32(10000.0 ** (-2.0 * f / rope))), inv_freq)
    angles = pos_col * inv_freq
    first = lax.rem(lane, rope) < half_rope
    cos_tab = jnp.cos(angles)
    sin_tab = jnp.sin(angles)
    sin_tab = jnp.where(first, -sin_tab, sin_tab)

    def rope_lanes(a):
        other = jnp.where(first, pltpu.roll(a, LANES - half_rope, 1), pltpu.roll(a, half_rope, 1))
        return (a * cos_tab + other * sin_tab).astype(jnp.bfloat16)

    q_row = iota((rows, LANES), 0)
    q_lane = lax.rem(lane, rows)
    pos_lane = jnp.sum(jnp.where(q_row == q_lane, jnp.broadcast_to(pos_col, (rows, LANES)), 0.0), axis=0, keepdims=True)
    q_lane = q_lane[:1]
    q_seq = jnp.where(q_lane < half, half * me + q_lane, half * (2 * n - 2 - me) + q_lane)
    q_first = q_seq - pos_lane.astype(jnp.int32)
    k_row = iota((keys, LANES), 0)
    k_dev = k_row // rows
    k_in = lax.rem(k_row, rows)
    k_seq = jnp.where(k_in < half, half * k_dev + k_in, half * (2 * n - 2 - k_dev) + k_in)
    bias_v[...] = jnp.where((k_seq >= q_first) & (k_seq <= q_seq), 0.0, MASKED)

    get_x.wait()
    get_wkr.wait()
    kr = mm(x_v[...], wkr_v[...], NT)
    get_wdkv.wait()
    start(get_wuq, get_wqr, get_wuk, get_wuv)
    kv = mm(x_v[...], wdkv_v[...])
    get_gkv.wait()
    lat[me, :rows, :] = rms_norm(kv, gkv_v[...].astype(jnp.float32).reshape(1, -1))
    kr = rope_lanes(jnp.concatenate([kr] * (LANES // rope), axis=1))
    packed = jnp.zeros((PACK_ROWS, LANES), jnp.bfloat16)
    slot = iota((PACK_ROWS, LANES), 1) // rope
    for s in range(rows // PACK_ROWS):
        packed = jnp.where(slot == s, kr[s * PACK_ROWS:(s + 1) * PACK_ROWS], packed)
    lat[me, rows:, :LANES] = packed
    lat[me, rows:, LANES:] = jnp.zeros((PACK_ROWS, kv_rank - LANES), jnp.bfloat16)

    pl.semaphore_wait(barrier, n // 2)

    def send(block, peer, index):
        cp = pltpu.make_async_remote_copy(src_ref=lat.at[block], dst_ref=lat.at[block], send_sem=send_sem.at[index],
                                          recv_sem=recv_sem.at[block], device_id={"ctx": peer}, device_id_type=MESH)
        cp.start()
        return cp

    sends = [send(me, peer, k) for k, peer in enumerate(others)]
    sends.append(send(me, partner, len(sends)))

    get_gq.wait()
    get_wdq.wait()
    start(*get_wout)
    cq_v[...] = rms_norm(mm(x_v[...], wdq_v[...]), gq_v[...].astype(jnp.float32).reshape(1, -1))
    get_wuq.wait()
    low = lane < nope
    zero = jnp.zeros((rows, LANES), jnp.bfloat16)
    for c in range(pairs // 4):
        q = mm(cq_v[...], wuq_v[:, c * 4 * LANES:(c + 1) * 4 * LANES]).astype(jnp.bfloat16)
        for i in range(4):
            t = q[:, i * LANES:(i + 1) * LANES]
            qcat[c * 4 + i, :rows, :LANES] = jnp.where(low, t, zero)
            qcat[c * 4 + i, rows:, :LANES] = jnp.where(low, zero, t)
    get_wqr.wait()
    per = LANES // rope
    for c in range(pairs * 2 // per // 2):
        q = mm(cq_v[...], wqr_v[:, c * 2 * LANES:(c + 1) * 2 * LANES])
        for i in range(2):
            t = rope_lanes(q[:, i * LANES:(i + 1) * LANES])
            for s in range(per):
                head = (c * 2 + i) * per + s
                at = head % 2 * rows
                qcat[head // 2, at:at + rows, LANES:] = jnp.where(lane // rope == s, t, zero)

    def arrived(block):
        pltpu.make_async_remote_copy(src_ref=lat.at[block], dst_ref=lat.at[block], send_sem=send_sem.at[0],
                                     recv_sem=recv_sem.at[block], device_id={"ctx": partner}, device_id_type=MESH).wait_recv()

    for block in others:
        arrived(block)
        sends.append(send(block, partner, len(sends)))
    arrived(partner)
    for k in range(1, n // 2):
        arrived(lax.rem(partner + 2 * k, n))

    c_all = lat[:, :rows, :].reshape(keys, kv_rank)
    packs = lat[:, rows:, :LANES]
    pslot = iota((n, PACK_ROWS, LANES), 2) // rope
    spread = jnp.stack([jnp.where(pslot == s, packs, jnp.zeros_like(packs)) for s in range(rows // PACK_ROWS)], axis=1)
    same = lax.rem(iota((LANES, LANES), 0), rope) == lax.rem(iota((LANES, LANES), 1), rope)
    kr_v[...] = mm(spread.reshape(keys, LANES), jnp.where(same, 1.0, 0.0).astype(jnp.bfloat16)).astype(jnp.bfloat16)
    get_wuk.wait()
    for c in range(pairs // 2):
        k = mm(c_all, wuk_v[:, c * 2 * LANES:(c + 1) * 2 * LANES]).astype(jnp.bfloat16)
        kcat[2 * c] = k[:, :LANES]
        kcat[2 * c + 1] = k[:, LANES:]
    get_wuv.wait()
    for c in range(pairs // 2):
        cols = slice(c * 2 * LANES, (c + 1) * 2 * LANES)
        vt[cols, :] = mm(wuv_v[:, cols], c_all, TT).astype(jnp.bfloat16)

    factor = (nope + rope) ** -0.5 * math.log2(math.e)
    steps = pairs // GROUP

    def scores(g):
        for i in range(GROUP):
            k = jnp.concatenate([kcat[g * GROUP + i], kr_v[...]], axis=1)
            t = mm(k, qcat[g * GROUP + i], NT) * factor + bias_v[...]
            s_v[g % 2, i] = t
            m_v[g % 2, i] = jnp.max(t, axis=0, keepdims=True)

    def weights(g):
        for i in range(GROUP):
            e = jnp.exp2(s_v[g % 2, i] - m_v[g % 2, i])
            p_v[g % 2, i] = e.astype(jnp.bfloat16)
            l_v[g % 2, i] = 1.0 / jnp.sum(e, axis=0, keepdims=True)

    def values(g):
        for i in range(GROUP):
            cols = slice((g * GROUP + i) * LANES, (g * GROUP + i + 1) * LANES)
            o = (mm(vt[cols, :], p_v[g % 2, i]) * l_v[g % 2, i]).T
            o_v[:, cols] = jnp.where(low, o[:rows], o[rows:]).astype(jnp.bfloat16)

    for g in range(steps + 2):
        if g >= 2:
            values(g - 2)
        if 1 <= g <= steps:
            weights(g - 1)
        if g < steps:
            scores(g)

    for get in get_wout:
        get.wait()
    for c in range(len(get_wout)):
        cols = slice(c * out_chunk, (c + 1) * out_chunk)
        y_v[:, cols] = mm(o_v[...], wout_v[:, cols]).astype(jnp.bfloat16)
    for cp in sends:
        cp.wait_send()


def solution(mesh):
    n = mesh.shape["ctx"]
    row_spec = P(("dp", "ctx"), None)
    id_spec = P(("dp", "ctx"))

    def per_device(x, pos, seg, w_dq, w_uq, w_qr, w_dkv, w_kr, w_uk, w_uv, w_out, gain_q, gain_kv):
        rows, width = x.shape
        pairs = w_uq.shape[1] // LANES
        keys = n * rows
        kv_rank = w_dkv.shape[1]
        bf, f32 = jnp.bfloat16, jnp.float32
        args = (x, pos.reshape(1, rows), w_dq, w_uq, w_qr, w_dkv, w_kr.T, w_uk, w_uv, w_out,
                gain_q, gain_kv)
        scratch = [pltpu.VMEM(a.shape, a.dtype) for a in args]
        scratch += [
            pltpu.VMEM((n, rows + PACK_ROWS, kv_rank), bf),
            pltpu.VMEM((rows, w_dq.shape[1]), bf),
            pltpu.VMEM((pairs, 2 * rows, 2 * LANES), bf),
            pltpu.VMEM((pairs, keys, LANES), bf),
            pltpu.VMEM((keys, LANES), bf),
            pltpu.VMEM((w_uv.shape[1], keys), bf),
            pltpu.VMEM((keys, LANES), f32),
            pltpu.VMEM((rows, w_uv.shape[1]), bf),
            pltpu.VMEM((2, GROUP, keys, LANES), f32),
            pltpu.VMEM((2, GROUP, 1, LANES), f32),
            pltpu.VMEM((2, GROUP, keys, LANES), bf),
            pltpu.VMEM((2, GROUP, 1, LANES), f32),
            pltpu.SemaphoreType.DMA((len(args) - 1 + OUT_CHUNKS,)),
            pltpu.SemaphoreType.DMA((n - 1,)),
            pltpu.SemaphoreType.DMA((n,)),
        ]
        return pl.pallas_call(
            functools.partial(layer_kernel, n),
            out_shape=jax.ShapeDtypeStruct(x.shape, bf),
            in_specs=[pl.BlockSpec(memory_space=pltpu.HBM)] * len(args),
            out_specs=pl.BlockSpec(memory_space=pltpu.VMEM),
            scratch_shapes=scratch,
            compiler_params=pltpu.CompilerParams(collective_id=0, has_side_effects=True, vmem_limit_bytes=62000000),
        )(*args)

    return jax.shard_map(per_device, mesh=mesh, in_specs=(row_spec, id_spec, id_spec) + (P(),) * 10, out_specs=row_spec, check_vma=False)
```

```python
import functools
import math

import jax
import jax.numpy as jnp
import numpy as np
from jax import lax
from jax.experimental import pallas as pl
from jax.experimental.pallas import tpu as pltpu
from jax.sharding import PartitionSpec as P

NORM_EPS = 1e-6
MASKED = -1e30
LANES = 128
PACK_ROWS = 16
GROUP = 2
OUT_CHUNKS = 5
MESH = pl.DeviceIdType.MESH
NT = (((1,), (1,)), ((), ()))
TT = (((0,), (1,)), ((), ()))


def mm(a, b, dims=(((1,), (0,)), ((), ()))):
    return lax.dot_general(a, b, dims, preferred_element_type=jnp.float32)


def rms_norm(vals, gain):
    mean_sq = jnp.mean(vals * vals, axis=-1, keepdims=True)
    return (vals * lax.rsqrt(mean_sq + NORM_EPS) * gain).astype(jnp.bfloat16)


def iota(shape, dim):
    return lax.broadcasted_iota(jnp.int32, shape, dim)


def layer_kernel(n, x_h, pos_h, wdq_h, wuq_h, wqr_h, wdkv_h, wkr_h, wuk_h, wuv_h, wout_h, gq_h, gkv_h, y_v,
                 x_v, pos_v, wdq_v, wuq_v, wqr_v, wdkv_v, wkr_v, wuk_v, wuv_v, wout_v, gq_v, gkv_v,
                 lat, cq_v, qcat, kcat, kr_v, vt, bias_v, o_v, s_v, m_v, p_v, l_v, in_sem, send_sem, recv_sem):
    rows, width = x_v.shape
    kv_rank = wdkv_v.shape[1]
    rope = wkr_v.shape[0]
    half_rope = rope // 2
    pairs = kcat.shape[0]
    nope = LANES // 2
    keys = n * rows
    half = rows // 2
    out_chunk = width // OUT_CHUNKS

    me = lax.axis_index("ctx")
    peers = [lax.rem(me + k, n) for k in range(1, n)]

    fetches = []

    def fetch(src, dst):
        fetches.append(pltpu.make_async_copy(src, dst, in_sem.at[len(fetches)]))
        return fetches[-1]

    def start(*copies):
        for cp in copies:
            cp.start()

    get_pos = fetch(pos_h, pos_v)
    get_x = fetch(x_h, x_v)
    get_wkr = fetch(wkr_h, wkr_v)
    get_wdkv = fetch(wdkv_h, wdkv_v)
    get_gkv = fetch(gkv_h, gkv_v)
    get_gq = fetch(gq_h, gq_v)
    get_wdq = fetch(wdq_h, wdq_v)
    get_wuq = fetch(wuq_h, wuq_v)
    get_wqr = fetch(wqr_h, wqr_v)
    get_wuk = fetch(wuk_h, wuk_v)
    get_wuv = fetch(wuv_h, wuv_v)
    get_wout = [fetch(wout_h.at[:, pl.ds(c * out_chunk, out_chunk)], wout_v.at[:, pl.ds(c * out_chunk, out_chunk)])
                for c in range(OUT_CHUNKS)]
    start(get_pos, get_x, get_wkr, get_wdkv, get_gkv, get_gq, get_wdq)

    barrier = pltpu.get_barrier_semaphore()
    for peer in peers:
        pl.semaphore_signal(barrier, inc=1, device_id={"ctx": peer}, device_id_type=MESH)

    get_pos.wait()
    pos_row = pos_v[...].astype(jnp.float32)
    diag = iota((rows, rows), 0) == iota((rows, rows), 1)
    pos_col = jnp.sum(jnp.where(diag, jnp.broadcast_to(pos_row, (rows, rows)), 0.0), axis=1, keepdims=True)
    lane = iota((rows, LANES), 1)
    freq_id = lax.rem(lane, half_rope)
    inv_freq = jnp.zeros((rows, LANES), jnp.float32)
    for f in range(half_rope):
        inv_freq = jnp.where(freq_id == f, float(np.float32(10000.0 ** (-2.0 * f / rope))), inv_freq)
    angles = pos_col * inv_freq
    first = lax.rem(lane, rope) < half_rope
    cos_tab = jnp.cos(angles)
    sin_tab = jnp.sin(angles)
    sin_tab = jnp.where(first, -sin_tab, sin_tab)

    def rope_lanes(a):
        other = jnp.where(first, pltpu.roll(a, LANES - half_rope, 1), pltpu.roll(a, half_rope, 1))
        return (a * cos_tab + other * sin_tab).astype(jnp.bfloat16)

    q_row = iota((rows, LANES), 0)
    q_lane = lax.rem(lane, rows)
    pos_lane = jnp.sum(jnp.where(q_row == q_lane, jnp.broadcast_to(pos_col, (rows, LANES)), 0.0), axis=0, keepdims=True)
    q_lane = q_lane[:1]
    q_seq = jnp.where(q_lane < half, half * me + q_lane, half * (2 * n - 2 - me) + q_lane)
    q_first = q_seq - pos_lane.astype(jnp.int32)
    k_row = iota((keys, LANES), 0)
    k_dev = k_row // rows
    k_in = lax.rem(k_row, rows)
    k_seq = jnp.where(k_in < half, half * k_dev + k_in, half * (2 * n - 2 - k_dev) + k_in)
    bias_v[...] = jnp.where((k_seq >= q_first) & (k_seq <= q_seq), 0.0, MASKED)

    get_x.wait()
    get_wkr.wait()
    kr = mm(x_v[...], wkr_v[...], NT)
    get_wdkv.wait()
    start(get_wuq, get_wqr, get_wuk, get_wuv)
    kv = mm(x_v[...], wdkv_v[...])
    get_gkv.wait()
    lat[me, :rows, :] = rms_norm(kv, gkv_v[...].astype(jnp.float32).reshape(1, -1))
    kr = rope_lanes(jnp.concatenate([kr] * (LANES // rope), axis=1))
    packed = jnp.zeros((PACK_ROWS, LANES), jnp.bfloat16)
    slot = iota((PACK_ROWS, LANES), 1) // rope
    for s in range(rows // PACK_ROWS):
        packed = jnp.where(slot == s, kr[s * PACK_ROWS:(s + 1) * PACK_ROWS], packed)
    lat[me, rows:, :LANES] = packed
    lat[me, rows:, LANES:] = jnp.zeros((PACK_ROWS, kv_rank - LANES), jnp.bfloat16)

    pl.semaphore_wait(barrier, n - 1)

    def send(block, peer, index):
        cp = pltpu.make_async_remote_copy(src_ref=lat.at[block], dst_ref=lat.at[block], send_sem=send_sem.at[index],
                                          recv_sem=recv_sem.at[block], device_id={"ctx": peer}, device_id_type=MESH)
        cp.start()
        return cp

    order = sorted(range(n - 1), key=lambda k: -min(k + 1, n - 1 - k))
    sends = [send(me, peers[k], k) for k in order]

    get_gq.wait()
    get_wdq.wait()
    start(*get_wout)
    cq_v[...] = rms_norm(mm(x_v[...], wdq_v[...]), gq_v[...].astype(jnp.float32).reshape(1, -1))
    get_wuq.wait()
    low = lane < nope
    zero = jnp.zeros((rows, LANES), jnp.bfloat16)
    for c in range(pairs // 4):
        q = mm(cq_v[...], wuq_v[:, c * 4 * LANES:(c + 1) * 4 * LANES]).astype(jnp.bfloat16)
        for i in range(4):
            t = q[:, i * LANES:(i + 1) * LANES]
            qcat[c * 4 + i, :rows, :LANES] = jnp.where(low, t, zero)
            qcat[c * 4 + i, rows:, :LANES] = jnp.where(low, zero, t)
    get_wqr.wait()
    per = LANES // rope
    for c in range(pairs * 2 // per // 2):
        q = mm(cq_v[...], wqr_v[:, c * 2 * LANES:(c + 1) * 2 * LANES])
        for i in range(2):
            t = rope_lanes(q[:, i * LANES:(i + 1) * LANES])
            for s in range(per):
                head = (c * 2 + i) * per + s
                at = head % 2 * rows
                qcat[head // 2, at:at + rows, LANES:] = jnp.where(lane // rope == s, t, zero)

    for block in peers:
        pltpu.make_async_remote_copy(src_ref=lat.at[block], dst_ref=lat.at[block], send_sem=send_sem.at[0],
                                     recv_sem=recv_sem.at[block], device_id={"ctx": block}, device_id_type=MESH).wait_recv()

    c_all = lat[:, :rows, :].reshape(keys, kv_rank)
    packs = lat[:, rows:, :LANES]
    pslot = iota((n, PACK_ROWS, LANES), 2) // rope
    spread = jnp.stack([jnp.where(pslot == s, packs, jnp.zeros_like(packs)) for s in range(rows // PACK_ROWS)], axis=1)
    same = lax.rem(iota((LANES, LANES), 0), rope) == lax.rem(iota((LANES, LANES), 1), rope)
    kr_v[...] = mm(spread.reshape(keys, LANES), jnp.where(same, 1.0, 0.0).astype(jnp.bfloat16)).astype(jnp.bfloat16)
    get_wuk.wait()
    for c in range(pairs // 2):
        k = mm(c_all, wuk_v[:, c * 2 * LANES:(c + 1) * 2 * LANES]).astype(jnp.bfloat16)
        kcat[2 * c] = k[:, :LANES]
        kcat[2 * c + 1] = k[:, LANES:]
    get_wuv.wait()
    for c in range(pairs // 2):
        cols = slice(c * 2 * LANES, (c + 1) * 2 * LANES)
        vt[cols, :] = mm(wuv_v[:, cols], c_all, TT).astype(jnp.bfloat16)

    factor = (nope + rope) ** -0.5 * math.log2(math.e)
    steps = pairs // GROUP

    def scores(g):
        for i in range(GROUP):
            k = jnp.concatenate([kcat[g * GROUP + i], kr_v[...]], axis=1)
            t = mm(k, qcat[g * GROUP + i], NT) * factor + bias_v[...]
            s_v[g % 2, i] = t
            m_v[g % 2, i] = jnp.max(t, axis=0, keepdims=True)

    def weights(g):
        for i in range(GROUP):
            e = jnp.exp2(s_v[g % 2, i] - m_v[g % 2, i])
            p_v[g % 2, i] = e.astype(jnp.bfloat16)
            l_v[g % 2, i] = 1.0 / jnp.sum(e, axis=0, keepdims=True)

    def values(g):
        for i in range(GROUP):
            cols = slice((g * GROUP + i) * LANES, (g * GROUP + i + 1) * LANES)
            o = (mm(vt[cols, :], p_v[g % 2, i]) * l_v[g % 2, i]).T
            o_v[:, cols] = jnp.where(low, o[:rows], o[rows:]).astype(jnp.bfloat16)

    for g in range(steps + 2):
        if g >= 2:
            values(g - 2)
        if 1 <= g <= steps:
            weights(g - 1)
        if g < steps:
            scores(g)

    for get in get_wout:
        get.wait()
    for c in range(len(get_wout)):
        cols = slice(c * out_chunk, (c + 1) * out_chunk)
        y_v[:, cols] = mm(o_v[...], wout_v[:, cols]).astype(jnp.bfloat16)
    for cp in sends:
        cp.wait_send()


def solution(mesh):
    n = mesh.shape["ctx"]
    row_spec = P(("dp", "ctx"), None)
    id_spec = P(("dp", "ctx"))

    def per_device(x, pos, seg, w_dq, w_uq, w_qr, w_dkv, w_kr, w_uk, w_uv, w_out, gain_q, gain_kv):
        rows, width = x.shape
        pairs = w_uq.shape[1] // LANES
        keys = n * rows
        kv_rank = w_dkv.shape[1]
        bf, f32 = jnp.bfloat16, jnp.float32
        args = (x, pos.reshape(1, rows), w_dq, w_uq, w_qr, w_dkv, w_kr.T, w_uk, w_uv, w_out,
                gain_q, gain_kv)
        scratch = [pltpu.VMEM(a.shape, a.dtype) for a in args]
        scratch += [
            pltpu.VMEM((n, rows + PACK_ROWS, kv_rank), bf),
            pltpu.VMEM((rows, w_dq.shape[1]), bf),
            pltpu.VMEM((pairs, 2 * rows, 2 * LANES), bf),
            pltpu.VMEM((pairs, keys, LANES), bf),
            pltpu.VMEM((keys, LANES), bf),
            pltpu.VMEM((w_uv.shape[1], keys), bf),
            pltpu.VMEM((keys, LANES), f32),
            pltpu.VMEM((rows, w_uv.shape[1]), bf),
            pltpu.VMEM((2, GROUP, keys, LANES), f32),
            pltpu.VMEM((2, GROUP, 1, LANES), f32),
            pltpu.VMEM((2, GROUP, keys, LANES), bf),
            pltpu.VMEM((2, GROUP, 1, LANES), f32),
            pltpu.SemaphoreType.DMA((len(args) - 1 + OUT_CHUNKS,)),
            pltpu.SemaphoreType.DMA((n - 1,)),
            pltpu.SemaphoreType.DMA((n,)),
        ]
        return pl.pallas_call(
            functools.partial(layer_kernel, n),
            out_shape=jax.ShapeDtypeStruct(x.shape, bf),
            in_specs=[pl.BlockSpec(memory_space=pltpu.HBM)] * len(args),
            out_specs=pl.BlockSpec(memory_space=pltpu.VMEM),
            scratch_shapes=scratch,
            compiler_params=pltpu.CompilerParams(collective_id=0, has_side_effects=True, vmem_limit_bytes=62000000),
        )(*args)

    return jax.shard_map(per_device, mesh=mesh, in_specs=(row_spec, id_spec, id_spec) + (P(),) * 10, out_specs=row_spec, check_vma=False)
```

```python
import functools
import math

import jax
import jax.numpy as jnp
import numpy as np
from jax import lax
from jax.experimental import pallas as pl
from jax.experimental.pallas import tpu as pltpu
from jax.sharding import PartitionSpec as P

NORM_EPS = 1e-6
MASKED = -1e30
LANES = 128
PACK_ROWS = 16
GROUP = 2
OUT_CHUNKS = 5
MESH = pl.DeviceIdType.MESH
NT = (((1,), (1,)), ((), ()))
TT = (((0,), (1,)), ((), ()))


def mm(a, b, dims=(((1,), (0,)), ((), ()))):
    return lax.dot_general(a, b, dims, preferred_element_type=jnp.float32)


def rms_norm(vals, gain):
    mean_sq = jnp.mean(vals * vals, axis=-1, keepdims=True)
    return (vals * lax.rsqrt(mean_sq + NORM_EPS) * gain).astype(jnp.bfloat16)


def iota(shape, dim):
    return lax.broadcasted_iota(jnp.int32, shape, dim)


def layer_kernel(n, x_h, pos_h, wdq_h, wuq_h, wqr_h, wdkv_h, wkr_h, wuk_h, wuv_h, wout_h, gq_h, gkv_h, y_v,
                 x_v, pos_v, wdq_v, wuq_v, wqr_v, wdkv_v, wkr_v, wuk_v, wuv_v, wout_v, gq_v, gkv_v,
                 lat, cq_v, qcat, kcat, kr_v, vt, bias_v, o_v, s_v, m_v, p_v, l_v, in_sem, send_sem, recv_sem):
    rows, width = x_v.shape
    kv_rank = wdkv_v.shape[1]
    rope = wkr_v.shape[0]
    half_rope = rope // 2
    pairs = kcat.shape[0]
    nope = LANES // 2
    keys = n * rows
    half = rows // 2
    out_chunk = width // OUT_CHUNKS

    me = lax.axis_index("ctx")
    peers = [lax.rem(me + k, n) for k in range(1, n)]

    fetches = []

    def fetch(src, dst):
        fetches.append(pltpu.make_async_copy(src, dst, in_sem.at[len(fetches)]))
        return fetches[-1]

    def start(*copies):
        for cp in copies:
            cp.start()

    get_pos = fetch(pos_h, pos_v)
    get_x = fetch(x_h, x_v)
    get_wkr = fetch(wkr_h, wkr_v)
    get_wdkv = fetch(wdkv_h, wdkv_v)
    get_gkv = fetch(gkv_h, gkv_v)
    get_gq = fetch(gq_h, gq_v)
    get_wdq = fetch(wdq_h, wdq_v)
    get_wuq = fetch(wuq_h, wuq_v)
    get_wqr = fetch(wqr_h, wqr_v)
    get_wuk = fetch(wuk_h, wuk_v)
    get_wuv = fetch(wuv_h, wuv_v)
    get_wout = [fetch(wout_h.at[:, pl.ds(c * out_chunk, out_chunk)], wout_v.at[:, pl.ds(c * out_chunk, out_chunk)])
                for c in range(OUT_CHUNKS)]
    start(get_pos, get_x, get_wkr, get_wdkv, get_gkv, get_gq, get_wdq)

    barrier = pltpu.get_barrier_semaphore()
    for peer in peers:
        pl.semaphore_signal(barrier, inc=1, device_id={"ctx": peer}, device_id_type=MESH)

    get_pos.wait()
    pos_row = pos_v[...].astype(jnp.float32)
    diag = iota((rows, rows), 0) == iota((rows, rows), 1)
    pos_col = jnp.sum(jnp.where(diag, jnp.broadcast_to(pos_row, (rows, rows)), 0.0), axis=1, keepdims=True)
    lane = iota((rows, LANES), 1)
    freq_id = lax.rem(lane, half_rope)
    inv_freq = jnp.zeros((rows, LANES), jnp.float32)
    for f in range(half_rope):
        inv_freq = jnp.where(freq_id == f, float(np.float32(10000.0 ** (-2.0 * f / rope))), inv_freq)
    angles = pos_col * inv_freq
    first = lax.rem(lane, rope) < half_rope
    cos_tab = jnp.cos(angles)
    sin_tab = jnp.sin(angles)
    sin_tab = jnp.where(first, -sin_tab, sin_tab)

    def rope_lanes(a):
        other = jnp.where(first, pltpu.roll(a, LANES - half_rope, 1), pltpu.roll(a, half_rope, 1))
        return (a * cos_tab + other * sin_tab).astype(jnp.bfloat16)

    q_row = iota((rows, LANES), 0)
    q_lane = lax.rem(lane, rows)
    pos_lane = jnp.sum(jnp.where(q_row == q_lane, jnp.broadcast_to(pos_col, (rows, LANES)), 0.0), axis=0, keepdims=True)
    q_lane = q_lane[:1]
    q_seq = jnp.where(q_lane < half, half * me + q_lane, half * (2 * n - 2 - me) + q_lane)
    q_first = q_seq - pos_lane.astype(jnp.int32)
    k_row = iota((keys, LANES), 0)
    k_dev = k_row // rows
    k_in = lax.rem(k_row, rows)
    k_seq = jnp.where(k_in < half, half * k_dev + k_in, half * (2 * n - 2 - k_dev) + k_in)
    bias_v[...] = jnp.where((k_seq >= q_first) & (k_seq <= q_seq), 0.0, MASKED)

    get_x.wait()
    get_wkr.wait()
    kr = mm(x_v[...], wkr_v[...], NT)
    get_wdkv.wait()
    start(get_wuq, get_wqr, get_wuk, get_wuv)
    kv = mm(x_v[...], wdkv_v[...])
    get_gkv.wait()
    lat[me, :rows, :] = rms_norm(kv, gkv_v[...].astype(jnp.float32).reshape(1, -1))
    kr = rope_lanes(jnp.concatenate([kr] * (LANES // rope), axis=1))
    packed = jnp.zeros((PACK_ROWS, LANES), jnp.bfloat16)
    slot = iota((PACK_ROWS, LANES), 1) // rope
    for s in range(rows // PACK_ROWS):
        packed = jnp.where(slot == s, kr[s * PACK_ROWS:(s + 1) * PACK_ROWS], packed)
    lat[me, rows:, :LANES] = packed
    lat[me, rows:, LANES:] = jnp.zeros((PACK_ROWS, kv_rank - LANES), jnp.bfloat16)

    pl.semaphore_wait(barrier, n - 1)

    def send(block, peer, index):
        cp = pltpu.make_async_remote_copy(src_ref=lat.at[block], dst_ref=lat.at[block], send_sem=send_sem.at[index],
                                          recv_sem=recv_sem.at[block], device_id={"ctx": peer}, device_id_type=MESH)
        cp.start()
        return cp

    order = sorted(range(n - 1), key=lambda k: -min(k + 1, n - 1 - k))
    sends = [send(me, peers[k], k) for k in order]

    get_gq.wait()
    get_wdq.wait()
    start(*get_wout)
    cq_v[...] = rms_norm(mm(x_v[...], wdq_v[...]), gq_v[...].astype(jnp.float32).reshape(1, -1))
    get_wuq.wait()
    low = lane < nope
    zero = jnp.zeros((rows, LANES), jnp.bfloat16)
    for c in range(pairs // 4):
        q = mm(cq_v[...], wuq_v[:, c * 4 * LANES:(c + 1) * 4 * LANES]).astype(jnp.bfloat16)
        for i in range(4):
            t = q[:, i * LANES:(i + 1) * LANES]
            qcat[c * 4 + i, :rows, :LANES] = jnp.where(low, t, zero)
            qcat[c * 4 + i, rows:, :LANES] = jnp.where(low, zero, t)
    get_wqr.wait()
    per = LANES // rope
    for c in range(pairs * 2 // per // 2):
        q = mm(cq_v[...], wqr_v[:, c * 2 * LANES:(c + 1) * 2 * LANES])
        for i in range(2):
            t = rope_lanes(q[:, i * LANES:(i + 1) * LANES])
            for s in range(per):
                head = (c * 2 + i) * per + s
                at = head % 2 * rows
                qcat[head // 2, at:at + rows, LANES:] = jnp.where(lane // rope == s, t, zero)

    for block in peers:
        pltpu.make_async_remote_copy(src_ref=lat.at[block], dst_ref=lat.at[block], send_sem=send_sem.at[0],
                                     recv_sem=recv_sem.at[block], device_id={"ctx": block}, device_id_type=MESH).wait_recv()

    c_all = lat[:, :rows, :].reshape(keys, kv_rank)
    packs = lat[:, rows:, :LANES]
    pslot = iota((n, PACK_ROWS, LANES), 2) // rope
    spread = jnp.stack([jnp.where(pslot == s, packs, jnp.zeros_like(packs)) for s in range(rows // PACK_ROWS)], axis=1)
    same = lax.rem(iota((LANES, LANES), 0), rope) == lax.rem(iota((LANES, LANES), 1), rope)
    kr_v[...] = mm(spread.reshape(keys, LANES), jnp.where(same, 1.0, 0.0).astype(jnp.bfloat16)).astype(jnp.bfloat16)
    get_wuk.wait()
    for c in range(pairs // 2):
        k = mm(c_all, wuk_v[:, c * 2 * LANES:(c + 1) * 2 * LANES]).astype(jnp.bfloat16)
        kcat[2 * c] = k[:, :LANES]
        kcat[2 * c + 1] = k[:, LANES:]
    get_wuv.wait()
    for c in range(pairs // 2):
        cols = slice(c * 2 * LANES, (c + 1) * 2 * LANES)
        vt[cols, :] = mm(wuv_v[:, cols], c_all, TT).astype(jnp.bfloat16)

    factor = (nope + rope) ** -0.5 * math.log2(math.e)
    steps = pairs // GROUP

    def scores(g):
        for i in range(GROUP):
            k = jnp.concatenate([kcat[g * GROUP + i], kr_v[...]], axis=1)
            t = mm(k, qcat[g * GROUP + i], NT) * factor + bias_v[...]
            s_v[g % 2, i] = t
            m_v[g % 2, i] = jnp.max(t, axis=0, keepdims=True)

    def weights(g):
        for i in range(GROUP):
            e = jnp.exp2(s_v[g % 2, i] - m_v[g % 2, i])
            p_v[g % 2, i] = e.astype(jnp.bfloat16)
            l_v[g % 2, i] = 1.0 / jnp.sum(e, axis=0, keepdims=True)

    def values(g):
        for i in range(GROUP):
            cols = slice((g * GROUP + i) * LANES, (g * GROUP + i + 1) * LANES)
            o = (mm(vt[cols, :], p_v[g % 2, i]) * l_v[g % 2, i]).T
            o_v[:, cols] = jnp.where(low, o[:rows], o[rows:]).astype(jnp.bfloat16)

    for g in range(steps + 2):
        if g >= 2:
            values(g - 2)
        if 1 <= g <= steps:
            weights(g - 1)
        if g < steps:
            scores(g)

    for get in get_wout:
        get.wait()
    for c in range(len(get_wout)):
        cols = slice(c * out_chunk, (c + 1) * out_chunk)
        y_v[:, cols] = mm(o_v[...], wout_v[:, cols]).astype(jnp.bfloat16)
    for cp in sends:
        cp.wait_send()


def solution(mesh):
    n = mesh.shape["ctx"]
    row_spec = P(("dp", "ctx"), None)
    id_spec = P(("dp", "ctx"))

    def per_device(x, pos, seg, w_dq, w_uq, w_qr, w_dkv, w_kr, w_uk, w_uv, w_out, gain_q, gain_kv):
        rows, width = x.shape
        pairs = w_uq.shape[1] // LANES
        keys = n * rows
        kv_rank = w_dkv.shape[1]
        bf, f32 = jnp.bfloat16, jnp.float32
        args = (x, pos.reshape(1, rows), w_dq, w_uq, w_qr, w_dkv, w_kr.T, w_uk, w_uv, w_out,
                gain_q, gain_kv)
        scratch = [pltpu.VMEM(a.shape, a.dtype) for a in args]
        scratch += [
            pltpu.VMEM((n, rows + PACK_ROWS, kv_rank), bf),
            pltpu.VMEM((rows, w_dq.shape[1]), bf),
            pltpu.VMEM((pairs, 2 * rows, 2 * LANES), bf),
            pltpu.VMEM((pairs, keys, LANES), bf),
            pltpu.VMEM((keys, LANES), bf),
            pltpu.VMEM((w_uv.shape[1], keys), bf),
            pltpu.VMEM((keys, LANES), f32),
            pltpu.VMEM((rows, w_uv.shape[1]), bf),
            pltpu.VMEM((2, GROUP, keys, LANES), f32),
            pltpu.VMEM((2, GROUP, 1, LANES), f32),
            pltpu.VMEM((2, GROUP, keys, LANES), bf),
            pltpu.VMEM((2, GROUP, 1, LANES), f32),
            pltpu.SemaphoreType.DMA((len(args) - 1 + OUT_CHUNKS,)),
            pltpu.SemaphoreType.DMA((n - 1,)),
            pltpu.SemaphoreType.DMA((n,)),
        ]
        return pl.pallas_call(
            functools.partial(layer_kernel, n),
            out_shape=pltpu.VMEM(x.shape, bf),
            in_specs=[pl.BlockSpec(memory_space=pltpu.HBM)] * len(args),
            out_specs=pl.BlockSpec(memory_space=pltpu.VMEM),
            scratch_shapes=scratch,
            compiler_params=pltpu.CompilerParams(collective_id=0, has_side_effects=True, vmem_limit_bytes=62000000),
        )(*args)

    return jax.shard_map(per_device, mesh=mesh, in_specs=(row_spec, id_spec, id_spec) + (P(),) * 10, out_specs=row_spec, check_vma=False)
```

```python
import functools
import math

import jax
import jax.numpy as jnp
import numpy as np
from jax import lax
from jax.experimental import pallas as pl
from jax.experimental.pallas import tpu as pltpu
from jax.sharding import PartitionSpec as P

NORM_EPS = 1e-6
MASKED = -1e30
LANES = 128
PACK_ROWS = 16
GROUP = 2
OUT_CHUNKS = 5
MESH = pl.DeviceIdType.MESH
NT = (((1,), (1,)), ((), ()))


def mm(a, b, dims=(((1,), (0,)), ((), ()))):
    return lax.dot_general(a, b, dims, preferred_element_type=jnp.float32)


def rms_norm(vals, gain):
    mean_sq = jnp.mean(vals * vals, axis=-1, keepdims=True)
    return (vals * lax.rsqrt(mean_sq + NORM_EPS) * gain).astype(jnp.bfloat16)


def iota(shape, dim):
    return lax.broadcasted_iota(jnp.int32, shape, dim)


def layer_kernel(n, x_h, pos_h, wdq_h, wuq_h, wqr_h, wdkv_h, wkr_h, wuk_h, wuv_h, wout_h, gq_h, gkv_h, y_v,
                 x_v, pos_v, wdq_v, wuq_v, wqr_v, wdkv_v, wkr_v, wuk_v, wuv_v, wout_v, gq_v, gkv_v,
                 lat, cq_v, qcat, kt_v, krt_v, v_v, bias_v, o_v, s_v, p_v, l_v, in_sem, send_sem, recv_sem):
    rows, width = x_v.shape
    kv_rank = wdkv_v.shape[1]
    rope = wkr_v.shape[0]
    half_rope = rope // 2
    pairs = kt_v.shape[0]
    nope = LANES // 2
    half = rows // 2
    chips = n // 2
    keys = chips * rows
    short = half + PACK_ROWS
    out_chunk = width // OUT_CHUNKS

    me = lax.axis_index("ctx")
    my_chip = me // 2
    peers = [lax.rem(me + k, n) for k in range(1, n)]

    barrier = pltpu.get_barrier_semaphore()
    for peer in peers:
        pl.semaphore_signal(barrier, inc=1, device_id={"ctx": peer}, device_id_type=MESH)

    fetches = []

    def fetch(src, dst):
        fetches.append(pltpu.make_async_copy(src, dst, in_sem.at[len(fetches)]))
        return fetches[-1]

    def start(*copies):
        for cp in copies:
            cp.start()

    get_pos = fetch(pos_h, pos_v)
    get_x = fetch(x_h, x_v)
    get_wkr = fetch(wkr_h, wkr_v)
    get_wdkv = fetch(wdkv_h, wdkv_v)
    get_gkv = fetch(gkv_h, gkv_v)
    get_gq = fetch(gq_h, gq_v)
    get_wdq = fetch(wdq_h, wdq_v)
    get_wuq = fetch(wuq_h, wuq_v)
    get_wqr = fetch(wqr_h, wqr_v)
    get_wuk = fetch(wuk_h, wuk_v)
    get_wuv = fetch(wuv_h, wuv_v)
    get_wout = [fetch(wout_h.at[:, pl.ds(c * out_chunk, out_chunk)], wout_v.at[:, pl.ds(c * out_chunk, out_chunk)])
                for c in range(OUT_CHUNKS)]
    start(get_pos, get_x, get_wkr, get_wdkv, get_gkv, get_gq, get_wdq)

    get_pos.wait()
    pos_row = pos_v[...].astype(jnp.float32)

    def pos_of(count, index):
        spot = iota((count, rows), 1) == index(iota((count, rows), 0))
        return jnp.sum(jnp.where(spot, jnp.broadcast_to(pos_row, (count, rows)), 0.0), axis=1, keepdims=True)

    lane = iota((rows, LANES), 1)
    freq_id = lax.rem(lane[:1], half_rope)
    inv_freq = jnp.zeros((1, LANES), jnp.float32)
    for f in range(half_rope):
        inv_freq = jnp.where(freq_id == f, float(np.float32(10000.0 ** (-2.0 * f / rope))), inv_freq)
    angles = pos_of(rows, lambda r: r) * inv_freq
    first = lax.rem(lane, rope) < half_rope
    cos_tab = jnp.cos(angles)
    sin_tab = jnp.sin(angles)
    sin_tab = jnp.where(first, -sin_tab, sin_tab)

    def rope_lanes(a):
        other = jnp.where(first, pltpu.roll(a, LANES - half_rope, 1), pltpu.roll(a, half_rope, 1))
        return (a * cos_tab + other * sin_tab).astype(jnp.bfloat16)

    count = 2 * rows
    q_pos = pos_of(count, lambda r: lax.rem(r, half) + jnp.where(r >= rows, half, 0)).astype(jnp.int32)
    q_row = iota((count, 1), 0)
    q_seq = jnp.where(q_row < rows, half * me, half * (2 * n - 1 - me)) + lax.rem(q_row, half)
    q_first = q_seq - q_pos
    col = iota((1, keys), 1)
    slot = col // rows
    swapped = slot + 1 - 2 * lax.rem(slot, 2)
    inner = lax.rem(col, rows)

    def key_seq(slot, late):
        dev = 2 * lax.rem(my_chip + slot, chips) + inner // half
        return half * jnp.where(late, 2 * n - 1 - dev, dev) + lax.rem(inner, half)

    def visible(seq, lo, hi):
        return jnp.where((seq >= lo) & (seq <= hi), 0.0, MASKED)

    bias_v[:count] = visible(key_seq(slot, False), q_first, q_seq)
    bias_v[count:] = visible(key_seq(swapped, True), q_first[rows:], q_seq[rows:])

    for peer in peers:
        @pl.when(peer < me)
        def _():
            lat[peer, short:, :] = jnp.zeros((half, kv_rank), jnp.bfloat16)

    get_x.wait()
    get_wkr.wait()
    kr = mm(x_v[...], wkr_v[...], NT)
    get_wdkv.wait()
    start(get_wuq, get_wqr, get_wuk, get_wuv)
    kv = mm(x_v[...], wdkv_v[...])
    get_gkv.wait()
    c_kv = rms_norm(kv, gkv_v[...].astype(jnp.float32).reshape(1, -1))
    lat[me, :half, :] = c_kv[:half]
    lat[me, short:, :] = c_kv[half:]
    kr = rope_lanes(jnp.concatenate([kr] * (LANES // rope), axis=1))
    packed = jnp.zeros((PACK_ROWS, LANES), jnp.bfloat16)
    part = iota((PACK_ROWS, LANES), 1) // rope
    for s in range(rows // PACK_ROWS):
        packed = jnp.where(part == s, kr[s * PACK_ROWS:(s + 1) * PACK_ROWS], packed)
    lat[me, half:short, :LANES] = packed
    lat[me, half:short, LANES:] = jnp.zeros((PACK_ROWS, kv_rank - LANES), jnp.bfloat16)

    pl.semaphore_wait(barrier, n - 1)

    def push(block, peer, index, count):
        at = lat.at[block, pl.ds(0, count)]
        return pltpu.make_async_remote_copy(src_ref=at, dst_ref=at, send_sem=send_sem.at[index],
                                            recv_sem=recv_sem.at[block], device_id={"ctx": peer}, device_id_type=MESH)

    def send(k):
        @pl.when(peers[k] < me)
        def _():
            push(me, peers[k], k, short + half).start()

        @pl.when(peers[k] > me)
        def _():
            push(me, peers[k], k, short).start()

    def sent(k):
        @pl.when(peers[k] < me)
        def _():
            push(me, peers[k], k, short + half).wait_send()

        @pl.when(peers[k] > me)
        def _():
            push(me, peers[k], k, short).wait_send()

    def arrived(block):
        @pl.when(block > me)
        def _():
            push(block, me, 0, short + half).wait_recv()

        @pl.when(block < me)
        def _():
            push(block, me, 0, short).wait_recv()

    for k in sorted(range(n - 1), key=lambda k: -min(k + 1, n - 1 - k)):
        send(k)

    get_gq.wait()
    get_wdq.wait()
    start(*get_wout)
    cq_v[...] = rms_norm(mm(x_v[...], wdq_v[...]), gq_v[...].astype(jnp.float32).reshape(1, -1))
    low = lane < nope
    zero = jnp.zeros((rows, LANES), jnp.bfloat16)

    def put_query(head, cols, t):
        at = head % 2 * half
        qcat[head // 2, at:at + half, cols] = t[:half]
        qcat[head // 2, rows + at:rows + at + half, cols] = t[half:]

    get_wuq.wait()
    for c in range(pairs // 4):
        q = mm(cq_v[...], wuq_v[:, c * 4 * LANES:(c + 1) * 4 * LANES]).astype(jnp.bfloat16)
        for i in range(4):
            t = q[:, i * LANES:(i + 1) * LANES]
            put_query(2 * (c * 4 + i), slice(0, LANES), jnp.where(low, t, zero))
            put_query(2 * (c * 4 + i) + 1, slice(0, LANES), jnp.where(low, zero, t))
    get_wqr.wait()
    per = LANES // rope
    for c in range(pairs // per):
        q = mm(cq_v[...], wqr_v[:, c * 2 * LANES:(c + 1) * 2 * LANES])
        for i in range(2):
            t = rope_lanes(q[:, i * LANES:(i + 1) * LANES])
            for s in range(per):
                put_query((c * 2 + i) * per + s, slice(LANES, 2 * LANES), jnp.where(lane // rope == s, t, zero))

    same = lax.rem(iota((LANES, LANES), 0), rope) == lax.rem(iota((LANES, LANES), 1), rope)
    same = jnp.where(same, 1.0, 0.0).astype(jnp.bfloat16)

    def up_project(t):
        chip = lax.rem(my_chip + t, chips)
        block = lat[pl.ds(2 * chip, 2)]
        pieces = [block[:, :half].reshape(rows, kv_rank), block[:, short:].reshape(rows, kv_rank)]
        groups = half // PACK_ROWS
        spread = [[jnp.where(part == p * groups + s, block[d, half:short, :LANES], jnp.zeros((PACK_ROWS, LANES), jnp.bfloat16))
                   for d in range(2) for s in range(groups)] for p in range(2)]
        first_piece = t % 2
        order = [first_piece, 1 - first_piece]
        c_chip = jnp.concatenate([pieces[p] for p in order], axis=0)
        krt = mm(same, jnp.concatenate(spread[order[0]] + spread[order[1]], axis=0), NT).astype(jnp.bfloat16)
        spots = [(order[i], (t - t % 2 + i) * rows, i * rows) for i in range(2)]
        for p, at, src in spots:
            krt_v[p, :, at:at + rows] = krt[:, src:src + rows]
        for c in range(pairs // 2):
            cols = slice(c * 2 * LANES, (c + 1) * 2 * LANES)
            k = mm(c_chip, wuk_v[:, cols]).astype(jnp.bfloat16)
            v = mm(c_chip, wuv_v[:, cols]).astype(jnp.bfloat16)
            for p, at, src in spots:
                v_v[p, at:at + rows, cols] = v[src:src + rows]
            for i in range(2):
                kt = k[:, i * LANES:(i + 1) * LANES].T
                for p, at, src in spots:
                    kt_v[2 * c + i, p, :, at:at + rows] = kt[:, src:src + rows]

    get_wuk.wait()
    get_wuv.wait()
    for t in sorted(range(chips), key=lambda t: min(t, chips - t)):
        for d in range(2):
            if t > 0:
                arrived(2 * lax.rem(my_chip + t, chips) + d)
        if t == 0:
            arrived(me + 1 - 2 * lax.rem(me, 2))
        up_project(t)

    factor = (nope + rope) ** -0.5 * math.log2(math.e)
    steps = pairs // GROUP

    def scores(g):
        for i in range(GROUP):
            p = g * GROUP + i
            early = jnp.concatenate([kt_v[p, 0], krt_v[0]], axis=0)
            late = jnp.concatenate([kt_v[p, 1], krt_v[1]], axis=0)
            s_v[g % 2, i, :count] = mm(qcat[p], early) * factor + bias_v[:count]
            s_v[g % 2, i, count:] = mm(qcat[p, rows:], late) * factor + bias_v[count:]

    def halves(a, op):
        return op(a[:, :LANES], a[:, LANES:])

    def weights(g):
        for i in range(GROUP):
            a, b, c = s_v[g % 2, i, :rows], s_v[g % 2, i, rows:count], s_v[g % 2, i, count:]
            m_a = jnp.max(halves(a, jnp.maximum), axis=1, keepdims=True)
            m_b = jnp.max(jnp.maximum(halves(b, jnp.maximum), halves(c, jnp.maximum)), axis=1, keepdims=True)
            a, b, c = jnp.exp2(a - m_a), jnp.exp2(b - m_b), jnp.exp2(c - m_b)
            p_v[g % 2, i, :rows] = a.astype(jnp.bfloat16)
            p_v[g % 2, i, rows:count] = b.astype(jnp.bfloat16)
            p_v[g % 2, i, count:] = c.astype(jnp.bfloat16)
            l_a = jnp.sum(halves(a, jnp.add), axis=1, keepdims=True)
            l_b = jnp.sum(halves(b, jnp.add) + halves(c, jnp.add), axis=1, keepdims=True)
            l_v[g % 2, i, :rows] = jnp.broadcast_to(1.0 / l_a, (rows, LANES))
            l_v[g % 2, i, rows:] = jnp.broadcast_to(1.0 / l_b, (rows, LANES))

    def values(g):
        for i in range(GROUP):
            cols = slice((g * GROUP + i) * LANES, (g * GROUP + i + 1) * LANES)
            o = mm(p_v[g % 2, i, :count], v_v[0, :, cols])
            o_a = o[:rows] * l_v[g % 2, i, :rows]
            o_b = (o[rows:] + mm(p_v[g % 2, i, count:], v_v[1, :, cols])) * l_v[g % 2, i, rows:]
            o_v[:half, cols] = jnp.where(low[:half], o_a[:half], o_a[half:]).astype(jnp.bfloat16)
            o_v[half:, cols] = jnp.where(low[:half], o_b[:half], o_b[half:]).astype(jnp.bfloat16)

    for g in range(steps + 2):
        if g >= 2:
            values(g - 2)
        if 1 <= g <= steps:
            weights(g - 1)
        if g < steps:
            scores(g)

    for get in get_wout:
        get.wait()
    for c in range(OUT_CHUNKS):
        cols = slice(c * out_chunk, (c + 1) * out_chunk)
        y_v[:, cols] = mm(o_v[...], wout_v[:, cols]).astype(jnp.bfloat16)
    for k in range(n - 1):
        sent(k)


def solution(mesh):
    n = mesh.shape["ctx"]
    row_spec = P(("dp", "ctx"), None)
    id_spec = P(("dp", "ctx"))

    def per_device(x, pos, seg, w_dq, w_uq, w_qr, w_dkv, w_kr, w_uk, w_uv, w_out, gain_q, gain_kv):
        rows, width = x.shape
        pairs = w_uq.shape[1] // LANES
        keys = n * rows
        kv_rank = w_dkv.shape[1]
        bf, f32 = jnp.bfloat16, jnp.float32
        args = (x, pos.reshape(1, rows), w_dq, w_uq, w_qr, w_dkv, w_kr.T, w_uk, w_uv, w_out,
                gain_q, gain_kv)
        scratch = [pltpu.VMEM(a.shape, a.dtype) for a in args]
        scratch += [
            pltpu.VMEM((n, rows + PACK_ROWS, kv_rank), bf),
            pltpu.VMEM((rows, w_dq.shape[1]), bf),
            pltpu.VMEM((pairs, 2 * rows, 2 * LANES), bf),
            pltpu.VMEM((pairs, 2, LANES, keys // 2), bf),
            pltpu.VMEM((2, LANES, keys // 2), bf),
            pltpu.VMEM((2, keys // 2, w_uv.shape[1]), bf),
            pltpu.VMEM((3 * rows, keys // 2), f32),
            pltpu.VMEM((rows, w_uv.shape[1]), bf),
            pltpu.VMEM((2, GROUP, 3 * rows, keys // 2), f32),
            pltpu.VMEM((2, GROUP, 3 * rows, keys // 2), bf),
            pltpu.VMEM((2, GROUP, 2 * rows, LANES), f32),
            pltpu.SemaphoreType.DMA((len(args) - 1 + OUT_CHUNKS,)),
            pltpu.SemaphoreType.DMA((n - 1,)),
            pltpu.SemaphoreType.DMA((n,)),
        ]
        return pl.pallas_call(
            functools.partial(layer_kernel, n),
            out_shape=pltpu.VMEM(x.shape, bf),
            in_specs=[pl.BlockSpec(memory_space=pltpu.HBM)] * len(args),
            out_specs=pl.BlockSpec(memory_space=pltpu.VMEM),
            scratch_shapes=scratch,
            compiler_params=pltpu.CompilerParams(collective_id=0, has_side_effects=True, vmem_limit_bytes=62000000),
        )(*args)

    return jax.shard_map(per_device, mesh=mesh, in_specs=(row_spec, id_spec, id_spec) + (P(),) * 10, out_specs=row_spec, check_vma=False)
```

```python
import functools
import math

import jax
import jax.numpy as jnp
import numpy as np
from jax import lax
from jax.experimental import pallas as pl
from jax.experimental.pallas import tpu as pltpu
from jax.sharding import PartitionSpec as P

NORM_EPS = 1e-6
MASKED = -1e30
LANES = 128
PACK_ROWS = 16
GROUP = 2
OUT_CHUNKS = 5
KV_CUTS = (0, 3, 6, 8, 10)
MESH = pl.DeviceIdType.MESH
NT = (((1,), (1,)), ((), ()))


def mm(a, b, dims=(((1,), (0,)), ((), ()))):
    return lax.dot_general(a, b, dims, preferred_element_type=jnp.float32)


def rms_norm(vals, gain):
    mean_sq = jnp.mean(vals * vals, axis=-1, keepdims=True)
    return (vals * lax.rsqrt(mean_sq + NORM_EPS) * gain).astype(jnp.bfloat16)


def iota(shape, dim):
    return lax.broadcasted_iota(jnp.int32, shape, dim)


def layer_kernel(n, x_h, pos_h, wdq_h, wuq_h, wqr_h, wdkv_h, wkr_h, wuk_h, wuv_h, wout_h, gq_h, gkv_h, y_v,
                 x_v, pos_v, wdq_v, wuq_v, wqr_v, wdkv_v, wkr_v, wuk_v, wuv_v, wout_v, gq_v, gkv_v,
                 lat, kv_v, cq_v, qcat, kt_v, krt_v, v_v, bias_v, o_v, s_v, p_v, l_v, in_sem, send_sem, recv_sem):
    rows, width = x_v.shape
    kv_rank = wdkv_v.shape[1]
    rope = wkr_v.shape[0]
    half_rope = rope // 2
    pairs = kt_v.shape[0]
    nope = LANES // 2
    half = rows // 2
    chips = n // 2
    keys = chips * rows
    short = half + PACK_ROWS
    out_chunk = width // OUT_CHUNKS

    me = lax.axis_index("ctx")
    my_chip = me // 2
    peers = [jnp.where(me > k, k, k + 1) for k in range(n - 1)]

    def chip_at(slot):
        return jnp.where(slot == 0, my_chip, jnp.where(slot > my_chip, slot, slot - 1))


    fetches = []

    def fetch(src, dst):
        fetches.append(pltpu.make_async_copy(src, dst, in_sem.at[len(fetches)]))
        return fetches[-1]

    def start(*copies):
        for cp in copies:
            cp.start()

    get_pos = fetch(pos_h, pos_v)
    get_x = fetch(x_h, x_v)
    get_wkr = fetch(wkr_h, wkr_v)
    depth = 2 * LANES
    cuts = [width // depth * c // 10 * depth for c in KV_CUTS]
    get_wdkv = [fetch(wdkv_h.at[pl.ds(lo, hi - lo)], wdkv_v.at[pl.ds(lo, hi - lo)]) for lo, hi in zip(cuts[::2], cuts[2::2])]
    get_gkv = fetch(gkv_h, gkv_v)
    get_gq = fetch(gq_h, gq_v)
    get_wdq = fetch(wdq_h, wdq_v)
    get_wuq = fetch(wuq_h, wuq_v)
    get_wqr = fetch(wqr_h, wqr_v)
    get_wuk = fetch(wuk_h, wuk_v)
    get_wuv = fetch(wuv_h, wuv_v)
    get_wout = [fetch(wout_h.at[:, pl.ds(c * out_chunk, out_chunk)], wout_v.at[:, pl.ds(c * out_chunk, out_chunk)])
                for c in range(OUT_CHUNKS)]
    start(get_pos, get_x, get_wkr, get_gkv, *get_wdkv)

    barrier = pltpu.get_barrier_semaphore()
    for peer in peers:
        pl.semaphore_signal(barrier, inc=1, device_id={"ctx": peer}, device_id_type=MESH)

    get_pos.wait()
    start(get_gq, get_wdq)
    pos_row = pos_v[...].astype(jnp.float32)

    def pos_of(count, index):
        spot = iota((count, rows), 1) == index(iota((count, rows), 0))
        return jnp.sum(jnp.where(spot, jnp.broadcast_to(pos_row, (count, rows)), 0.0), axis=1, keepdims=True)

    lane = iota((rows, LANES), 1)
    freq_id = lax.rem(lane[:1], half_rope)
    inv_freq = jnp.zeros((1, LANES), jnp.float32)
    for f in range(half_rope):
        inv_freq = jnp.where(freq_id == f, float(np.float32(10000.0 ** (-2.0 * f / rope))), inv_freq)
    angles = pos_of(rows, lambda r: r) * inv_freq
    first = lax.rem(lane, rope) < half_rope
    cos_tab = jnp.cos(angles)
    sin_tab = jnp.sin(angles)
    sin_tab = jnp.where(first, -sin_tab, sin_tab)

    def rope_lanes(a):
        other = jnp.where(first, pltpu.roll(a, LANES - half_rope, 1), pltpu.roll(a, half_rope, 1))
        return (a * cos_tab + other * sin_tab).astype(jnp.bfloat16)

    count = 2 * rows
    q_pos = pos_of(count, lambda r: lax.rem(r, half) + jnp.where(r >= rows, half, 0)).astype(jnp.int32)
    q_row = iota((count, 1), 0)
    q_seq = jnp.where(q_row < rows, half * me, half * (2 * n - 1 - me)) + lax.rem(q_row, half)
    q_first = q_seq - q_pos
    col = iota((1, keys), 1)
    slot = col // rows
    swapped = slot + 1 - 2 * lax.rem(slot, 2)
    inner = lax.rem(col, rows)

    def key_seq(slot, late):
        dev = 2 * chip_at(slot) + inner // half
        return half * jnp.where(late, 2 * n - 1 - dev, dev) + lax.rem(inner, half)

    def visible(seq, lo, hi):
        return jnp.where((seq >= lo) & (seq <= hi), 0.0, MASKED)

    bias_v[:count] = visible(key_seq(slot, False), q_first, q_seq)
    bias_v[count:] = visible(key_seq(swapped, True), q_first[rows:], q_seq[rows:])

    get_x.wait()
    get_wkr.wait()
    kr = mm(x_v[...], wkr_v[...], NT)
    for c, get in enumerate(get_wdkv):
        get.wait()
        for i in range(2 * c, 2 * c + 2):
            kv_v[i] = mm(x_v[:, cuts[i]:cuts[i + 1]], wdkv_v[cuts[i]:cuts[i + 1]])
    kv = sum(kv_v[i] for i in range(len(cuts) - 1))
    start(get_wuq, get_wqr, get_wuk, get_wuv)
    get_gkv.wait()
    c_kv = rms_norm(kv, gkv_v[...].astype(jnp.float32).reshape(1, -1))
    lat[me, :half, :] = c_kv[:half]
    lat[me, short:, :] = c_kv[half:]
    kr = rope_lanes(jnp.concatenate([kr] * (LANES // rope), axis=1))
    packed = jnp.zeros((PACK_ROWS, LANES), jnp.bfloat16)
    part = iota((PACK_ROWS, LANES), 1) // rope
    for s in range(rows // PACK_ROWS):
        packed = jnp.where(part == s, kr[s * PACK_ROWS:(s + 1) * PACK_ROWS], packed)
    lat[me, half:short, :LANES] = packed
    lat[me, half:short, LANES:] = jnp.zeros((PACK_ROWS, kv_rank - LANES), jnp.bfloat16)

    pl.semaphore_wait(barrier, n - 1)

    def push(block, peer, index):
        return pltpu.make_async_remote_copy(src_ref=lat.at[block], dst_ref=lat.at[block], send_sem=send_sem.at[index],
                                            recv_sem=recv_sem.at[block], device_id={"ctx": peer}, device_id_type=MESH)

    sends = [push(me, peer, k) for k, peer in enumerate(peers)]
    start(*sends)

    get_gq.wait()
    get_wdq.wait()
    start(*get_wout)
    cq_v[...] = rms_norm(mm(x_v[...], wdq_v[...]), gq_v[...].astype(jnp.float32).reshape(1, -1))
    low = lane < nope
    zero = jnp.zeros((rows, LANES), jnp.bfloat16)

    def put_query(head, cols, t):
        at = head % 2 * half
        qcat[head // 2, at:at + half, cols] = t[:half]
        qcat[head // 2, rows + at:rows + at + half, cols] = t[half:]

    get_wuq.wait()
    for c in range(pairs // 4):
        q = mm(cq_v[...], wuq_v[:, c * 4 * LANES:(c + 1) * 4 * LANES]).astype(jnp.bfloat16)
        for i in range(4):
            t = q[:, i * LANES:(i + 1) * LANES]
            put_query(2 * (c * 4 + i), slice(0, LANES), jnp.where(low, t, zero))
            put_query(2 * (c * 4 + i) + 1, slice(0, LANES), jnp.where(low, zero, t))
    get_wqr.wait()
    per = LANES // rope
    for c in range(pairs // per):
        q = mm(cq_v[...], wqr_v[:, c * 2 * LANES:(c + 1) * 2 * LANES])
        for i in range(2):
            t = rope_lanes(q[:, i * LANES:(i + 1) * LANES])
            for s in range(per):
                put_query((c * 2 + i) * per + s, slice(LANES, 2 * LANES), jnp.where(lane // rope == s, t, zero))

    same = lax.rem(iota((LANES, LANES), 0), rope) == lax.rem(iota((LANES, LANES), 1), rope)
    same = jnp.where(same, 1.0, 0.0).astype(jnp.bfloat16)

    def up_project(t):
        chip = chip_at(t)
        block = lat[pl.ds(2 * chip, 2)]
        pieces = [block[:, :half].reshape(rows, kv_rank), block[:, short:].reshape(rows, kv_rank)]
        groups = half // PACK_ROWS
        spread = [[jnp.where(part == p * groups + s, block[d, half:short, :LANES], jnp.zeros((PACK_ROWS, LANES), jnp.bfloat16))
                   for d in range(2) for s in range(groups)] for p in range(2)]
        first_piece = t % 2
        order = [first_piece, 1 - first_piece]
        c_chip = jnp.concatenate([pieces[p] for p in order], axis=0)
        krt = mm(same, jnp.concatenate(spread[order[0]] + spread[order[1]], axis=0), NT).astype(jnp.bfloat16)
        spots = [(order[i], (t - t % 2 + i) * rows, i * rows) for i in range(2)]
        for p, at, src in spots:
            krt_v[p, :, at:at + rows] = krt[:, src:src + rows]
        for c in range(pairs // 2):
            cols = slice(c * 2 * LANES, (c + 1) * 2 * LANES)
            k = mm(c_chip, wuk_v[:, cols]).astype(jnp.bfloat16)
            for i in range(2):
                kt = k[:, i * LANES:(i + 1) * LANES].T
                for p, at, src in spots:
                    kt_v[2 * c + i, p, :, at:at + rows] = kt[:, src:src + rows]
        for c in range(pairs // 2):
            cols = slice(c * 2 * LANES, (c + 1) * 2 * LANES)
            v = mm(c_chip, wuv_v[:, cols]).astype(jnp.bfloat16)
            for p, at, src in spots:
                v_v[p, at:at + rows, cols] = v[src:src + rows]

    get_wuk.wait()
    get_wuv.wait()
    for t in range(chips):
        chip = chip_at(t)
        for block in [2 * chip, 2 * chip + 1] if t else [me + 1 - 2 * lax.rem(me, 2)]:
            push(block, me, 0).wait_recv()
        up_project(t)

    factor = (nope + rope) ** -0.5 * math.log2(math.e)
    steps = pairs // GROUP

    def scores(g):
        for i in range(GROUP):
            p = g * GROUP + i
            early = jnp.concatenate([kt_v[p, 0], krt_v[0]], axis=0)
            late = jnp.concatenate([kt_v[p, 1], krt_v[1]], axis=0)
            s_v[g % 2, i, :count] = mm(qcat[p], early) * factor + bias_v[:count]
            s_v[g % 2, i, count:] = mm(qcat[p, rows:], late) * factor + bias_v[count:]

    def halves(a, op):
        return op(a[:, :LANES], a[:, LANES:])

    def weights(g):
        for i in range(GROUP):
            a, b, c = s_v[g % 2, i, :rows], s_v[g % 2, i, rows:count], s_v[g % 2, i, count:]
            m_a = jnp.max(halves(a, jnp.maximum), axis=1, keepdims=True)
            m_b = jnp.max(jnp.maximum(halves(b, jnp.maximum), halves(c, jnp.maximum)), axis=1, keepdims=True)
            a, b, c = jnp.exp2(a - m_a), jnp.exp2(b - m_b), jnp.exp2(c - m_b)
            p_v[g % 2, i, :rows] = a.astype(jnp.bfloat16)
            p_v[g % 2, i, rows:count] = b.astype(jnp.bfloat16)
            p_v[g % 2, i, count:] = c.astype(jnp.bfloat16)
            l_a = jnp.sum(halves(a, jnp.add), axis=1, keepdims=True)
            l_b = jnp.sum(halves(b, jnp.add) + halves(c, jnp.add), axis=1, keepdims=True)
            l_v[g % 2, i, :rows] = jnp.broadcast_to(1.0 / l_a, (rows, LANES))
            l_v[g % 2, i, rows:] = jnp.broadcast_to(1.0 / l_b, (rows, LANES))

    def values(g):
        for i in range(GROUP):
            cols = slice((g * GROUP + i) * LANES, (g * GROUP + i + 1) * LANES)
            o = mm(p_v[g % 2, i, :count], v_v[0, :, cols])
            o_a = o[:rows] * l_v[g % 2, i, :rows]
            o_b = (o[rows:] + mm(p_v[g % 2, i, count:], v_v[1, :, cols])) * l_v[g % 2, i, rows:]
            o_v[:half, cols] = jnp.where(low[:half], o_a[:half], o_a[half:]).astype(jnp.bfloat16)
            o_v[half:, cols] = jnp.where(low[:half], o_b[:half], o_b[half:]).astype(jnp.bfloat16)

    for g in range(steps + 2):
        if g >= 2:
            values(g - 2)
        if 1 <= g <= steps:
            weights(g - 1)
        if g < steps:
            scores(g)

    for get in get_wout:
        get.wait()
    for c in range(OUT_CHUNKS):
        cols = slice(c * out_chunk, (c + 1) * out_chunk)
        y_v[:, cols] = mm(o_v[...], wout_v[:, cols]).astype(jnp.bfloat16)
    for cp in sends:
        cp.wait_send()


def solution(mesh):
    n = mesh.shape["ctx"]
    row_spec = P(("dp", "ctx"), None)
    id_spec = P(("dp", "ctx"))

    def per_device(x, pos, seg, w_dq, w_uq, w_qr, w_dkv, w_kr, w_uk, w_uv, w_out, gain_q, gain_kv):
        rows, width = x.shape
        pairs = w_uq.shape[1] // LANES
        keys = n * rows
        kv_rank = w_dkv.shape[1]
        bf, f32 = jnp.bfloat16, jnp.float32
        args = (x, pos.reshape(1, rows), w_dq, w_uq, w_qr, w_dkv, w_kr.T, w_uk, w_uv, w_out,
                gain_q, gain_kv)
        scratch = [pltpu.VMEM(a.shape, a.dtype) for a in args]
        scratch += [
            pltpu.VMEM((n, rows + PACK_ROWS, kv_rank), bf),
            pltpu.VMEM((len(KV_CUTS) - 1, rows, kv_rank), f32),
            pltpu.VMEM((rows, w_dq.shape[1]), bf),
            pltpu.VMEM((pairs, 2 * rows, 2 * LANES), bf),
            pltpu.VMEM((pairs, 2, LANES, keys // 2), bf),
            pltpu.VMEM((2, LANES, keys // 2), bf),
            pltpu.VMEM((2, keys // 2, w_uv.shape[1]), bf),
            pltpu.VMEM((3 * rows, keys // 2), f32),
            pltpu.VMEM((rows, w_uv.shape[1]), bf),
            pltpu.VMEM((2, GROUP, 3 * rows, keys // 2), f32),
            pltpu.VMEM((2, GROUP, 3 * rows, keys // 2), bf),
            pltpu.VMEM((2, GROUP, 2 * rows, LANES), f32),
            pltpu.SemaphoreType.DMA((len(args) - 2 + len(KV_CUTS) // 2 + OUT_CHUNKS,)),
            pltpu.SemaphoreType.DMA((n - 1,)),
            pltpu.SemaphoreType.DMA((n,)),
        ]
        return pl.pallas_call(
            functools.partial(layer_kernel, n),
            out_shape=pltpu.VMEM(x.shape, bf),
            in_specs=[pl.BlockSpec(memory_space=pltpu.HBM)] * len(args),
            out_specs=pl.BlockSpec(memory_space=pltpu.VMEM),
            scratch_shapes=scratch,
            compiler_params=pltpu.CompilerParams(collective_id=0, has_side_effects=True, vmem_limit_bytes=62000000),
        )(*args)

    return jax.shard_map(per_device, mesh=mesh, in_specs=(row_spec, id_spec, id_spec) + (P(),) * 10, out_specs=row_spec, check_vma=False)
```

```python
import functools
import math

import jax
import jax.numpy as jnp
import numpy as np
from jax import lax
from jax.experimental import pallas as pl
from jax.experimental.pallas import tpu as pltpu
from jax.sharding import PartitionSpec as P

NORM_EPS = 1e-6
MASKED = -1e30
LANES = 128
PACK_ROWS = 16
PACKS = 2
GROUP = 2
KV_CUTS = (0, 5, 10)
MESH = pl.DeviceIdType.MESH
NT = (((1,), (1,)), ((), ()))


def mm(a, b, dims=(((1,), (0,)), ((), ()))):
    return lax.dot_general(a, b, dims, preferred_element_type=jnp.float32)


def rms_norm(vals, gain):
    mean_sq = jnp.mean(vals * vals, axis=-1, keepdims=True)
    return (vals * lax.rsqrt(mean_sq + NORM_EPS) * gain).astype(jnp.bfloat16)


def iota(shape, dim):
    return lax.broadcasted_iota(jnp.int32, shape, dim)


def layer_kernel(n, x_h, pos_h, wdq_h, wuq_h, wqr_h, wdkv_h, wkr_h, wuk_h, wuv_h, wout_h, gq_h, gkv_h, y_v,
                 x_v, pos_v, wdq_v, wuq_v, wqr_v, wdkv_v, wkr_v, wuk_v, wuv_v, wout_v, gq_v, gkv_v,
                 lat, kv_v, cq_v, qcat, kt_v, krt_v, v_v, bias_v, o_v, s_v, p_v, l_v, in_sem, send_sem, recv_sem):
    rows, width = x_v.shape
    kv_rank = wdkv_v.shape[1]
    rope = wkr_v.shape[0]
    half_rope = rope // 2
    pairs = kt_v.shape[0]
    nope = LANES // 2
    half = rows // 2
    chips = n // 2
    keys = chips * rows
    pack_rows = PACK_ROWS // PACKS
    panels, _, panel = wout_v.shape

    me = lax.axis_index("ctx")
    my_chip = me // 2
    partner = me + 1 - 2 * lax.rem(me, 2)
    odd = lax.rem(me, 2) == 1

    def chip_at(slot):
        return jnp.where(slot == 0, my_chip, jnp.where(slot > my_chip, slot, slot - 1))


    fetches = []

    def fetch(src, dst):
        fetches.append(pltpu.make_async_copy(src, dst, in_sem.at[len(fetches)]))
        return fetches[-1]

    def start(*copies):
        for cp in copies:
            cp.start()

    get_pos = fetch(pos_h, pos_v)
    get_x = fetch(x_h, x_v)
    get_wkr = fetch(wkr_h, wkr_v)
    depth = 2 * LANES
    cuts = [width // depth * c // 10 * depth for c in KV_CUTS]
    get_wdkv = [fetch(wdkv_h.at[pl.ds(lo, hi - lo)], wdkv_v.at[pl.ds(lo, hi - lo)]) for lo, hi in zip(cuts, cuts[1:])]
    get_gkv = fetch(gkv_h, gkv_v)
    get_gq = fetch(gq_h, gq_v)
    get_wdq = fetch(wdq_h, wdq_v)
    get_wuq = fetch(wuq_h, wuq_v)
    get_wqr = fetch(wqr_h, wqr_v)
    get_wuk = fetch(wuk_h, wuk_v)
    get_wuv = fetch(wuv_h, wuv_v)
    get_wout = [fetch(wout_h.at[:, pl.ds(c * panel, panel)], wout_v.at[c]) for c in range(panels)]
    start(get_pos, get_x, get_wkr, get_gkv, *get_wdkv)

    barrier = pltpu.get_barrier_semaphore()
    pl.semaphore_signal(barrier, inc=1, device_id={"ctx": partner}, device_id_type=MESH)

    @pl.when(odd)
    def _():
        for t in range(1, chips):
            for d in range(2):
                pl.semaphore_signal(barrier, inc=1, device_id={"ctx": 2 * chip_at(t) + d}, device_id_type=MESH)

    get_pos.wait()
    get_x.wait()
    get_wkr.wait()
    start(get_gq, get_wdq)
    pos_row = pos_v[...].astype(jnp.float32)

    def pos_of(count, index):
        spot = iota((count, rows), 1) == index(iota((count, rows), 0))
        return jnp.sum(jnp.where(spot, jnp.broadcast_to(pos_row, (count, rows)), 0.0), axis=1, keepdims=True)

    lane = iota((rows, LANES), 1)
    freq_id = lax.rem(lane[:1], half_rope)
    inv_freq = jnp.zeros((1, LANES), jnp.float32)
    for f in range(half_rope):
        inv_freq = jnp.where(freq_id == f, float(np.float32(10000.0 ** (-2.0 * f / rope))), inv_freq)
    angles = pos_of(rows, lambda r: r) * inv_freq
    first = lax.rem(lane, rope) < half_rope
    cos_tab = jnp.cos(angles)
    sin_tab = jnp.sin(angles)
    sin_tab = jnp.where(first, -sin_tab, sin_tab)

    def rope_lanes(a):
        other = jnp.where(first, pltpu.roll(a, LANES - half_rope, 1), pltpu.roll(a, half_rope, 1))
        return (a * cos_tab + other * sin_tab).astype(jnp.bfloat16)

    count = 2 * rows
    q_pos = pos_of(count, lambda r: lax.rem(r, half) + jnp.where(r >= rows, half, 0)).astype(jnp.int32)
    q_row = iota((count, 1), 0)
    q_seq = jnp.where(q_row < rows, half * me, half * (2 * n - 1 - me)) + lax.rem(q_row, half)
    q_first = q_seq - q_pos
    col = iota((1, keys), 1)
    slot = col // rows
    swapped = slot + 1 - 2 * lax.rem(slot, 2)
    inner = lax.rem(col, rows)

    def key_seq(slot, late):
        dev = 2 * chip_at(slot) + inner // half
        return half * jnp.where(late, 2 * n - 1 - dev, dev) + lax.rem(inner, half)

    def visible(seq, lo, hi):
        return jnp.where((seq >= lo) & (seq <= hi), 0.0, MASKED)

    bias_v[:count] = visible(key_seq(slot, False), q_first, q_seq)
    bias_v[count:] = visible(key_seq(swapped, True), q_first[rows:], q_seq[rows:])

    kr = mm(x_v[...], wkr_v[...], NT)
    for get in get_wdkv:
        get.wait()
    for i in range(kv_rank // LANES):
        kv_v[:, i * LANES:(i + 1) * LANES] = mm(x_v[...], wdkv_v[:, i * LANES:(i + 1) * LANES])
    kv = kv_v[...]
    start(get_wuq, get_wqr, get_wuk, get_wuv)
    get_gkv.wait()
    c_kv = rms_norm(kv, gkv_v[...].astype(jnp.float32).reshape(1, -1))
    lat[me, :rows, :] = c_kv
    kr = rope_lanes(jnp.concatenate([kr] * (LANES // rope), axis=1))
    packed = jnp.zeros((PACK_ROWS, LANES), jnp.float32)
    kr = kr.astype(jnp.float32)
    part = iota((PACK_ROWS, LANES), 1) // rope
    for s in range(rows // PACK_ROWS):
        packed = jnp.where(part == s, kr[s * PACK_ROWS:(s + 1) * PACK_ROWS], packed)
    for i in range(PACKS):
        lat[me, rows:, i * LANES:(i + 1) * LANES] = packed[i * pack_rows:(i + 1) * pack_rows].astype(jnp.bfloat16)

    pl.semaphore_wait(barrier, chips)

    def push(block, peer, index):
        return pltpu.make_async_remote_copy(src_ref=lat.at[block], dst_ref=lat.at[block], send_sem=send_sem.at[index],
                                            recv_sem=recv_sem.at[block], device_id={"ctx": peer}, device_id_type=MESH)

    sends = [push(me, 2 * chip_at(t) + 1, t) for t in range(1, chips)] + [push(me, partner, 0)]
    start(*sends)

    def forward(t):
        return [push(2 * chip_at(t) + d, partner, chips + 2 * (t - 1) + d) for d in range(2)]

    def relay(t):
        for d, cp in enumerate(forward(t)):
            push(2 * chip_at(t) + d, me, 0).wait_recv()
            cp.start()

    get_gq.wait()
    get_wdq.wait()
    start(*get_wout)
    cq_v[...] = rms_norm(mm(x_v[...], wdq_v[...]), gq_v[...].astype(jnp.float32).reshape(1, -1))
    low = lane < nope
    zero = jnp.zeros((rows, LANES), jnp.bfloat16)

    def put_query(head, cols, t):
        at = head % 2 * half
        qcat[head // 2, at:at + half, cols] = t[:half]
        qcat[head // 2, rows + at:rows + at + half, cols] = t[half:]

    get_wuq.wait()
    for c in range(pairs // 4):
        q = mm(cq_v[...], wuq_v[:, c * 4 * LANES:(c + 1) * 4 * LANES]).astype(jnp.bfloat16)
        for i in range(4):
            t = q[:, i * LANES:(i + 1) * LANES]
            put_query(2 * (c * 4 + i), slice(0, LANES), jnp.where(low, t, zero))
            put_query(2 * (c * 4 + i) + 1, slice(0, LANES), jnp.where(low, zero, t))
    get_wqr.wait()
    per = LANES // rope
    for c in range(pairs // per):
        q = mm(cq_v[...], wqr_v[:, c * 2 * LANES:(c + 1) * 2 * LANES])
        for i in range(2):
            t = rope_lanes(q[:, i * LANES:(i + 1) * LANES])
            for s in range(per):
                put_query((c * 2 + i) * per + s, slice(LANES, 2 * LANES), jnp.where(lane // rope == s, t, zero))

    same = lax.rem(iota((LANES, LANES), 0), rope) == lax.rem(iota((LANES, LANES), 1), rope)
    same = jnp.where(same, 1.0, 0.0).astype(jnp.bfloat16)

    def up_project(t):
        chip = chip_at(t)
        block = lat[pl.ds(2 * chip, 2), :rows]
        pieces = [block[:, :half].reshape(rows, kv_rank), block[:, half:rows].reshape(rows, kv_rank)]
        groups = half // PACK_ROWS
        tails = [lat[2 * chip + d, rows:].astype(jnp.float32) for d in range(2)]
        packs = [jnp.concatenate([a[:, i * LANES:(i + 1) * LANES] for i in range(PACKS)], axis=0) for a in tails]
        spread = [[jnp.where(part == p * groups + s, packs[d], 0.0).astype(jnp.bfloat16)
                   for d in range(2) for s in range(groups)] for p in range(2)]
        first_piece = t % 2
        order = [first_piece, 1 - first_piece]
        c_chip = jnp.concatenate([pieces[p] for p in order], axis=0)
        krt = mm(same, jnp.concatenate(spread[order[0]] + spread[order[1]], axis=0), NT).astype(jnp.bfloat16)
        spots = [(order[i], (t - t % 2 + i) * rows, i * rows) for i in range(2)]
        for p, at, src in spots:
            krt_v[p, :, at:at + rows] = krt[:, src:src + rows]
        for c in range(pairs // 2):
            cols = slice(c * 2 * LANES, (c + 1) * 2 * LANES)
            k = mm(c_chip, wuk_v[:, cols]).astype(jnp.bfloat16)
            for i in range(2):
                kt = k[:, i * LANES:(i + 1) * LANES].T
                for p, at, src in spots:
                    kt_v[2 * c + i, p, :, at:at + rows] = kt[:, src:src + rows]
        for c in range(pairs // 2):
            cols = slice(c * 2 * LANES, (c + 1) * 2 * LANES)
            v = mm(c_chip, wuv_v[:, cols]).astype(jnp.bfloat16)
            for i in range(2):
                for p, at, src in spots:
                    v_v[2 * c + i, p, at:at + rows] = v[src:src + rows, i * LANES:(i + 1) * LANES]

    get_wuk.wait()
    get_wuv.wait()
    for t in range(chips):
        for first_slot, last_slot in [(1, 2)] * (t == 0) + [(2, chips)] * (t == 2):
            @pl.when(odd)
            def _():
                for u in range(first_slot, last_slot):
                    relay(u)
        if t == 0:
            push(partner, me, 0).wait_recv()
        else:
            @pl.when(jnp.logical_not(odd))
            def _():
                for d in range(2):
                    push(2 * chip_at(t) + d, me, 0).wait_recv()
        up_project(t)

    factor = (nope + rope) ** -0.5 * math.log2(math.e)
    steps = pairs // GROUP

    def scores(g):
        for i in range(GROUP):
            p = g * GROUP + i
            early = jnp.concatenate([kt_v[p, 0], krt_v[0]], axis=0)
            late = jnp.concatenate([kt_v[p, 1], krt_v[1]], axis=0)
            s_v[g % 2, i, :count] = mm(qcat[p], early) * factor + bias_v[:count]
            s_v[g % 2, i, count:] = mm(qcat[p, rows:], late) * factor + bias_v[count:]

    def halves(a, op):
        return op(a[:, :LANES], a[:, LANES:])

    def weights(g):
        for i in range(GROUP):
            a, b, c = s_v[g % 2, i, :rows], s_v[g % 2, i, rows:count], s_v[g % 2, i, count:]
            m_a = jnp.max(halves(a, jnp.maximum), axis=1, keepdims=True)
            m_b = jnp.max(jnp.maximum(halves(b, jnp.maximum), halves(c, jnp.maximum)), axis=1, keepdims=True)
            a, b, c = jnp.exp2(a - m_a), jnp.exp2(b - m_b), jnp.exp2(c - m_b)
            p_v[g % 2, i, :rows] = a.astype(jnp.bfloat16)
            p_v[g % 2, i, rows:count] = b.astype(jnp.bfloat16)
            p_v[g % 2, i, count:] = c.astype(jnp.bfloat16)
            l_a = jnp.sum(halves(a, jnp.add), axis=1, keepdims=True)
            l_b = jnp.sum(halves(b, jnp.add) + halves(c, jnp.add), axis=1, keepdims=True)
            l_v[g % 2, i, :rows] = jnp.broadcast_to(1.0 / l_a, (rows, LANES))
            l_v[g % 2, i, rows:] = jnp.broadcast_to(1.0 / l_b, (rows, LANES))

    def values(g):
        for i in range(GROUP):
            cols = slice((g * GROUP + i) * LANES, (g * GROUP + i + 1) * LANES)
            o = mm(p_v[g % 2, i, :count], v_v[g * GROUP + i, 0])
            o_a = o[:rows] * l_v[g % 2, i, :rows]
            o_b = (o[rows:] + mm(p_v[g % 2, i, count:], v_v[g * GROUP + i, 1])) * l_v[g % 2, i, rows:]
            o_v[:half, cols] = jnp.where(low[:half], o_a[:half], o_a[half:]).astype(jnp.bfloat16)
            o_v[half:, cols] = jnp.where(low[:half], o_b[:half], o_b[half:]).astype(jnp.bfloat16)

    for g in range(steps + 2):
        if g >= 2:
            values(g - 2)
        if 1 <= g <= steps:
            weights(g - 1)
        if g < steps:
            scores(g)

    for get in get_wout:
        get.wait()
    for c in range(panels):
        y_v[:, c * panel:(c + 1) * panel] = mm(o_v[...], wout_v[c]).astype(jnp.bfloat16)
    for cp in sends:
        cp.wait_send()

    @pl.when(odd)
    def _():
        for t in range(1, chips):
            for cp in forward(t):
                cp.wait_send()


def solution(mesh):
    n = mesh.shape["ctx"]
    row_spec = P(("dp", "ctx"), None)
    id_spec = P(("dp", "ctx"))

    def per_device(x, pos, seg, w_dq, w_uq, w_qr, w_dkv, w_kr, w_uk, w_uv, w_out, gain_q, gain_kv):
        rows, width = x.shape
        pairs = w_uq.shape[1] // LANES
        keys = n * rows
        kv_rank = w_dkv.shape[1]
        bf, f32 = jnp.bfloat16, jnp.float32
        args = (x, pos.reshape(1, rows), w_dq, w_uq, w_qr, w_dkv, w_kr.T, w_uk, w_uv, w_out,
                gain_q, gain_kv)
        panels = w_out.shape[1] // (2 * LANES)
        scratch = [pltpu.VMEM((panels, w_out.shape[0], 2 * LANES) if a is w_out else a.shape, a.dtype) for a in args]
        scratch += [
            pltpu.VMEM((n, rows + PACK_ROWS // PACKS, kv_rank), bf),
            pltpu.VMEM((rows, kv_rank), f32),
            pltpu.VMEM((rows, w_dq.shape[1]), bf),
            pltpu.VMEM((pairs, 2 * rows, 2 * LANES), bf),
            pltpu.VMEM((pairs, 2, LANES, keys // 2), bf),
            pltpu.VMEM((2, LANES, keys // 2), bf),
            pltpu.VMEM((pairs, 2, keys // 2, LANES), bf),
            pltpu.VMEM((3 * rows, keys // 2), f32),
            pltpu.VMEM((rows, w_uv.shape[1]), bf),
            pltpu.VMEM((2, GROUP, 3 * rows, keys // 2), f32),
            pltpu.VMEM((2, GROUP, 3 * rows, keys // 2), bf),
            pltpu.VMEM((2, GROUP, 2 * rows, LANES), f32),
            pltpu.SemaphoreType.DMA((len(args) - 2 + len(KV_CUTS) - 1 + panels,)),
            pltpu.SemaphoreType.DMA((n // 2 + n - 2,)),
            pltpu.SemaphoreType.DMA((n,)),
        ]
        return pl.pallas_call(
            functools.partial(layer_kernel, n),
            out_shape=pltpu.VMEM(x.shape, bf),
            in_specs=[pl.BlockSpec(memory_space=pltpu.HBM)] * len(args),
            out_specs=pl.BlockSpec(memory_space=pltpu.VMEM),
            scratch_shapes=scratch,
            compiler_params=pltpu.CompilerParams(collective_id=0, has_side_effects=True, vmem_limit_bytes=62000000),
        )(*args)

    return jax.shard_map(per_device, mesh=mesh, in_specs=(row_spec, id_spec, id_spec) + (P(),) * 10, out_specs=row_spec, check_vma=False)
```

```python
import functools
import math

import jax
import jax.numpy as jnp
import numpy as np
from jax import lax
from jax.experimental import pallas as pl
from jax.experimental.pallas import tpu as pltpu
from jax.sharding import PartitionSpec as P

NORM_EPS = 1e-6
MASKED = -1e30
LANES = 128
PACK_ROWS = 16
PACKS = 2
GROUP = 4
KV_CUTS = (0, 2, 4, 6, 8, 10)
MESH = pl.DeviceIdType.MESH
NT = (((1,), (1,)), ((), ()))


def mm(a, b, dims=(((1,), (0,)), ((), ()))):
    return lax.dot_general(a, b, dims, preferred_element_type=jnp.float32)


def rms_norm(vals, gain):
    mean_sq = jnp.mean(vals * vals, axis=-1, keepdims=True)
    return (vals * lax.rsqrt(mean_sq + NORM_EPS) * gain).astype(jnp.bfloat16)


def iota(shape, dim):
    return lax.broadcasted_iota(jnp.int32, shape, dim)


def layer_kernel(n, x_h, pos_h, wdq_h, wuq_h, wqr_h, wdkv_h, wkr_h, wuk_h, wuv_h, wout_h, gq_h, gkv_h, y_v,
                 x_v, pos_v, wdq_v, wuq_v, wqr_v, wdkv_v, wkr_v, wuk_v, wuv_v, wout_v, gq_v, gkv_v,
                 lat, kv_v, cq_v, qcat, kt_v, krt_v, v_v, bias_v, o_v, s_v, p_v, l_v, y_sum, in_sem, send_sem, recv_sem):
    rows, width = x_v.shape
    kv_rank = wdkv_v.shape[1]
    rope = wkr_v.shape[0]
    half_rope = rope // 2
    pairs = kt_v.shape[0]
    nope = LANES // 2
    half = rows // 2
    chips = n // 2
    keys = chips * rows
    pack_rows = PACK_ROWS // PACKS
    steps = pairs // GROUP
    deep = GROUP * LANES
    panel = 2 * LANES

    me = lax.axis_index("ctx")
    my_chip = me // 2
    partner = me + 1 - 2 * lax.rem(me, 2)
    odd = lax.rem(me, 2) == 1

    def chip_at(slot):
        return jnp.where(slot == 0, my_chip, jnp.where(slot > my_chip, slot, slot - 1))


    fetches = []

    def fetch(src, dst):
        fetches.append(pltpu.make_async_copy(src, dst, in_sem.at[len(fetches)]))
        return fetches[-1]

    def start(*copies):
        for cp in copies:
            cp.start()

    get_pos = fetch(pos_h, pos_v)
    get_x = fetch(x_h, x_v)
    get_wkr = fetch(wkr_h, wkr_v)
    depth = 2 * LANES
    cuts = [width // depth * c // 10 * depth for c in KV_CUTS]
    get_wdkv = [fetch(wdkv_h.at[pl.ds(lo, hi - lo)], wdkv_v.at[pl.ds(lo, hi - lo)]) for lo, hi in zip(cuts, cuts[1:])]
    get_gkv = fetch(gkv_h, gkv_v)
    get_gq = fetch(gq_h, gq_v)
    get_wdq = fetch(wdq_h, wdq_v)
    get_wuq = fetch(wuq_h, wuq_v)
    get_wqr = fetch(wqr_h, wqr_v)
    get_wuk = fetch(wuk_h, wuk_v)
    get_wuv = fetch(wuv_h, wuv_v)
    get_wout = [fetch(wout_h.at[pl.ds(g * deep, deep)], wout_v.at[pl.ds(g * deep, deep)]) for g in range(steps)]
    start(get_pos, get_x, get_wkr, get_gkv, *get_wdkv, get_gq, get_wdq, get_wuq, get_wqr, get_wuk, get_wuv, *get_wout)

    barrier = pltpu.get_barrier_semaphore()
    pl.semaphore_signal(barrier, inc=1, device_id={"ctx": partner}, device_id_type=MESH)

    @pl.when(odd)
    def _():
        for t in range(1, chips):
            for d in range(2):
                pl.semaphore_signal(barrier, inc=1, device_id={"ctx": 2 * chip_at(t) + d}, device_id_type=MESH)

    get_pos.wait()
    get_x.wait()
    get_wkr.wait()
    pos_row = pos_v[...].astype(jnp.float32)

    def pos_of(count, index):
        spot = iota((count, rows), 1) == index(iota((count, rows), 0))
        return jnp.sum(jnp.where(spot, jnp.broadcast_to(pos_row, (count, rows)), 0.0), axis=1, keepdims=True)

    lane = iota((rows, LANES), 1)
    freq_id = lax.rem(lane[:1], half_rope)
    inv_freq = jnp.zeros((1, LANES), jnp.float32)
    for f in range(half_rope):
        inv_freq = jnp.where(freq_id == f, float(np.float32(10000.0 ** (-2.0 * f / rope))), inv_freq)
    angles = pos_of(rows, lambda r: r) * inv_freq
    first = lax.rem(lane, rope) < half_rope
    cos_tab = jnp.cos(angles)
    sin_tab = jnp.sin(angles)
    sin_tab = jnp.where(first, -sin_tab, sin_tab)

    def rope_lanes(a):
        other = jnp.where(first, pltpu.roll(a, LANES - half_rope, 1), pltpu.roll(a, half_rope, 1))
        return (a * cos_tab + other * sin_tab).astype(jnp.bfloat16)

    count = 2 * rows
    q_pos = pos_of(count, lambda r: lax.rem(r, half) + jnp.where(r >= rows, half, 0)).astype(jnp.int32)
    q_row = iota((count, 1), 0)
    q_seq = jnp.where(q_row < rows, half * me, half * (2 * n - 1 - me)) + lax.rem(q_row, half)
    q_first = q_seq - q_pos
    col = iota((1, keys), 1)
    slot = col // rows
    swapped = slot + 1 - 2 * lax.rem(slot, 2)
    inner = lax.rem(col, rows)

    def key_seq(slot, late):
        dev = 2 * chip_at(slot) + inner // half
        return half * jnp.where(late, 2 * n - 1 - dev, dev) + lax.rem(inner, half)

    def visible(seq, lo, hi):
        return jnp.where((seq >= lo) & (seq <= hi), 0.0, MASKED)

    bias_v[:count] = visible(key_seq(slot, False), q_first, q_seq)
    bias_v[count:] = visible(key_seq(swapped, True), q_first[rows:], q_seq[rows:])

    kr = mm(x_v[...], wkr_v[...], NT)
    for get in get_wdkv:
        get.wait()
    for i in range(kv_rank // LANES):
        kv_v[:, i * LANES:(i + 1) * LANES] = mm(x_v[...], wdkv_v[:, i * LANES:(i + 1) * LANES])
    kv = kv_v[...]
    get_gkv.wait()
    c_kv = rms_norm(kv, gkv_v[...].astype(jnp.float32).reshape(1, -1))
    lat[me, :rows, :] = c_kv
    kr = rope_lanes(jnp.concatenate([kr] * (LANES // rope), axis=1))
    packed = jnp.zeros((PACK_ROWS, LANES), jnp.float32)
    kr = kr.astype(jnp.float32)
    part = iota((PACK_ROWS, LANES), 1) // rope
    for s in range(rows // PACK_ROWS):
        packed = jnp.where(part == s, kr[s * PACK_ROWS:(s + 1) * PACK_ROWS], packed)
    for i in range(PACKS):
        lat[me, rows:, i * LANES:(i + 1) * LANES] = packed[i * pack_rows:(i + 1) * pack_rows].astype(jnp.bfloat16)

    pl.semaphore_wait(barrier, chips)

    def push(block, peer, index):
        return pltpu.make_async_remote_copy(src_ref=lat.at[block], dst_ref=lat.at[block], send_sem=send_sem.at[index],
                                            recv_sem=recv_sem.at[block], device_id={"ctx": peer}, device_id_type=MESH)

    sends = [push(me, 2 * chip_at(t) + 1, t) for t in range(1, chips)] + [push(me, partner, 0)]
    start(*sends)

    def forward(t):
        return [push(2 * chip_at(t) + d, partner, chips + 2 * (t - 1) + d) for d in range(2)]

    def relay(t):
        for d, cp in enumerate(forward(t)):
            push(2 * chip_at(t) + d, me, 0).wait_recv()
            cp.start()

    get_gq.wait()
    get_wdq.wait()
    cq_v[...] = rms_norm(mm(x_v[...], wdq_v[...]), gq_v[...].astype(jnp.float32).reshape(1, -1))
    low = lane < nope
    zero = jnp.zeros((rows, LANES), jnp.bfloat16)

    def put_query(head, cols, t):
        at = head % 2 * half
        qcat[head // 2, at:at + half, cols] = t[:half]
        qcat[head // 2, rows + at:rows + at + half, cols] = t[half:]

    get_wuq.wait()
    for c in range(pairs // 4):
        q = mm(cq_v[...], wuq_v[:, c * 4 * LANES:(c + 1) * 4 * LANES]).astype(jnp.bfloat16)
        for i in range(4):
            t = q[:, i * LANES:(i + 1) * LANES]
            put_query(2 * (c * 4 + i), slice(0, LANES), jnp.where(low, t, zero))
            put_query(2 * (c * 4 + i) + 1, slice(0, LANES), jnp.where(low, zero, t))
    get_wqr.wait()
    per = LANES // rope
    for c in range(pairs // per):
        q = mm(cq_v[...], wqr_v[:, c * 2 * LANES:(c + 1) * 2 * LANES])
        for i in range(2):
            t = rope_lanes(q[:, i * LANES:(i + 1) * LANES])
            for s in range(per):
                put_query((c * 2 + i) * per + s, slice(LANES, 2 * LANES), jnp.where(lane // rope == s, t, zero))

    same = lax.rem(iota((LANES, LANES), 0), rope) == lax.rem(iota((LANES, LANES), 1), rope)
    same = jnp.where(same, 1.0, 0.0).astype(jnp.bfloat16)

    def up_project(slots):
        pieces, packs = [], []
        groups = half // PACK_ROWS
        for t in slots:
            chip = chip_at(t)
            block = lat[pl.ds(2 * chip, 2), :rows]
            tails = [lat[2 * chip + d, rows:].astype(jnp.float32) for d in range(2)]
            tails = [jnp.concatenate([a[:, i * LANES:(i + 1) * LANES] for i in range(PACKS)], axis=0) for a in tails]
            for p in [t % 2, 1 - t % 2]:
                pieces.append(block[:, p * half:(p + 1) * half].reshape(rows, kv_rank))
                packs += [jnp.where(part == p * groups + s, tails[d], 0.0).astype(jnp.bfloat16) for d in range(2) for s in range(groups)]
        c_all = jnp.concatenate(pieces, axis=0)
        krt = mm(same, jnp.concatenate(packs, axis=0), NT).astype(jnp.bfloat16)
        spots = [((t + i) % 2, (t - t % 2 + i) * rows, (2 * j + i) * rows) for j, t in enumerate(slots) for i in range(2)]
        for p, at, src in spots:
            krt_v[p, :, at:at + rows] = krt[:, src:src + rows]
        for c in range(pairs // 2):
            cols = slice(c * 2 * LANES, (c + 1) * 2 * LANES)
            k = mm(c_all, wuk_v[:, cols]).astype(jnp.bfloat16)
            for i in range(2):
                kt = k[:, i * LANES:(i + 1) * LANES].T
                for p, at, src in spots:
                    kt_v[2 * c + i, p, :, at:at + rows] = kt[:, src:src + rows]
        for c in range(pairs // 2):
            cols = slice(c * 2 * LANES, (c + 1) * 2 * LANES)
            v = mm(c_all, wuv_v[:, cols]).astype(jnp.bfloat16)
            for i in range(2):
                for p, at, src in spots:
                    v_v[2 * c + i, p, at:at + rows] = v[src:src + rows, i * LANES:(i + 1) * LANES]

    get_wuk.wait()
    get_wuv.wait()
    push(partner, me, 0).wait_recv()
    for t in range(0, chips, 2):
        slots = [u for u in (t, t + 1) if u > 0]

        @pl.when(odd)
        def _():
            for u in slots:
                relay(u)

        @pl.when(jnp.logical_not(odd))
        def _():
            for u in slots:
                for d in range(2):
                    push(2 * chip_at(u) + d, me, 0).wait_recv()

        if t + 2 >= chips:
            for get in get_wout:
                get.wait()
        up_project([t, t + 1])

    factor = (nope + rope) ** -0.5 * math.log2(math.e)

    def scores(g):
        for i in range(GROUP):
            p = g * GROUP + i
            early = jnp.concatenate([kt_v[p, 0], krt_v[0]], axis=0)
            late = jnp.concatenate([kt_v[p, 1], krt_v[1]], axis=0)
            s_v[g % 2, i, :count] = mm(qcat[p], early) * factor + bias_v[:count]
            s_v[g % 2, i, count:] = mm(qcat[p, rows:], late) * factor + bias_v[count:]

    def halves(a, op):
        return op(a[:, :LANES], a[:, LANES:])

    def weights(g):
        for i in range(GROUP):
            a, b, c = s_v[g % 2, i, :rows], s_v[g % 2, i, rows:count], s_v[g % 2, i, count:]
            m_a = jnp.max(halves(a, jnp.maximum), axis=1, keepdims=True)
            m_b = jnp.max(jnp.maximum(halves(b, jnp.maximum), halves(c, jnp.maximum)), axis=1, keepdims=True)
            a, b, c = jnp.exp2(a - m_a), jnp.exp2(b - m_b), jnp.exp2(c - m_b)
            p_v[g % 2, i, :rows] = a.astype(jnp.bfloat16)
            p_v[g % 2, i, rows:count] = b.astype(jnp.bfloat16)
            p_v[g % 2, i, count:] = c.astype(jnp.bfloat16)
            l_a = jnp.sum(halves(a, jnp.add), axis=1, keepdims=True)
            l_b = jnp.sum(halves(b, jnp.add) + halves(c, jnp.add), axis=1, keepdims=True)
            l_v[g % 2, i, :rows] = jnp.broadcast_to(1.0 / l_a, (rows, LANES))
            l_v[g % 2, i, rows:] = jnp.broadcast_to(1.0 / l_b, (rows, LANES))

    def values(g):
        for i in range(GROUP):
            cols = slice((g * GROUP + i) * LANES, (g * GROUP + i + 1) * LANES)
            o = mm(p_v[g % 2, i, :count], v_v[g * GROUP + i, 0])
            o_a = o[:rows] * l_v[g % 2, i, :rows]
            o_b = (o[rows:] + mm(p_v[g % 2, i, count:], v_v[g * GROUP + i, 1])) * l_v[g % 2, i, rows:]
            o_v[:half, cols] = jnp.where(low[:half], o_a[:half], o_a[half:]).astype(jnp.bfloat16)
            o_v[half:, cols] = jnp.where(low[:half], o_b[:half], o_b[half:]).astype(jnp.bfloat16)

    def project(g):
        for c in range(width // panel):
            cols = slice(c * panel, (c + 1) * panel)
            y = mm(o_v[:, g * deep:(g + 1) * deep], wout_v[g * deep:(g + 1) * deep, cols])
            if g > 0:
                y += y_sum[:, cols]
            if g + 1 < steps:
                y_sum[:, cols] = y
            else:
                y_v[:, cols] = y.astype(jnp.bfloat16)

    for g in range(steps + 3):
        if g >= 3:
            project(g - 3)
        if 2 <= g < steps + 2:
            values(g - 2)
        if 1 <= g <= steps:
            weights(g - 1)
        if g < steps:
            scores(g)
    for cp in sends:
        cp.wait_send()

    @pl.when(odd)
    def _():
        for t in range(1, chips):
            for cp in forward(t):
                cp.wait_send()


def solution(mesh):
    n = mesh.shape["ctx"]
    row_spec = P(("dp", "ctx"), None)
    id_spec = P(("dp", "ctx"))

    def per_device(x, pos, seg, w_dq, w_uq, w_qr, w_dkv, w_kr, w_uk, w_uv, w_out, gain_q, gain_kv):
        rows, width = x.shape
        pairs = w_uq.shape[1] // LANES
        keys = n * rows
        kv_rank = w_dkv.shape[1]
        bf, f32 = jnp.bfloat16, jnp.float32
        args = (x, pos.reshape(1, rows), w_dq, w_uq, w_qr, w_dkv, w_kr.T, w_uk, w_uv, w_out,
                gain_q, gain_kv)
        scratch = [pltpu.VMEM(a.shape, a.dtype) for a in args]
        scratch += [
            pltpu.VMEM((n, rows + PACK_ROWS // PACKS, kv_rank), bf),
            pltpu.VMEM((rows, kv_rank), f32),
            pltpu.VMEM((rows, w_dq.shape[1]), bf),
            pltpu.VMEM((pairs, 2 * rows, 2 * LANES), bf),
            pltpu.VMEM((pairs, 2, LANES, keys // 2), bf),
            pltpu.VMEM((2, LANES, keys // 2), bf),
            pltpu.VMEM((pairs, 2, keys // 2, LANES), bf),
            pltpu.VMEM((3 * rows, keys // 2), f32),
            pltpu.VMEM((rows, w_uv.shape[1]), bf),
            pltpu.VMEM((2, GROUP, 3 * rows, keys // 2), f32),
            pltpu.VMEM((2, GROUP, 3 * rows, keys // 2), bf),
            pltpu.VMEM((2, GROUP, 2 * rows, LANES), f32),
            pltpu.VMEM((rows, width), f32),
            pltpu.SemaphoreType.DMA((len(args) - 2 + len(KV_CUTS) - 1 + pairs // GROUP,)),
            pltpu.SemaphoreType.DMA((n // 2 + n - 2,)),
            pltpu.SemaphoreType.DMA((n,)),
        ]
        return pl.pallas_call(
            functools.partial(layer_kernel, n),
            out_shape=pltpu.VMEM(x.shape, bf),
            in_specs=[pl.BlockSpec(memory_space=pltpu.HBM)] * len(args),
            out_specs=pl.BlockSpec(memory_space=pltpu.VMEM),
            scratch_shapes=scratch,
            compiler_params=pltpu.CompilerParams(collective_id=0, has_side_effects=True, vmem_limit_bytes=62000000),
        )(*args)

    return jax.shard_map(per_device, mesh=mesh, in_specs=(row_spec, id_spec, id_spec) + (P(),) * 10, out_specs=row_spec, check_vma=False)
```

```python
import functools
import math

import jax
import jax.numpy as jnp
import numpy as np
from jax import lax
from jax.experimental import pallas as pl
from jax.experimental.pallas import tpu as pltpu
from jax.sharding import PartitionSpec as P

NORM_EPS = 1e-6
MASKED = -1e30
LANES = 128
PACK_ROWS = 16
PACKS = 2
GROUP = 4
KV_CUTS = (0, 2, 4, 6, 8, 10)
MESH = pl.DeviceIdType.MESH
NT = (((1,), (1,)), ((), ()))


def mm(a, b, dims=(((1,), (0,)), ((), ()))):
    return lax.dot_general(a, b, dims, preferred_element_type=jnp.float32)


def rms_norm(vals, gain):
    mean_sq = jnp.mean(vals * vals, axis=-1, keepdims=True)
    return (vals * lax.rsqrt(mean_sq + NORM_EPS) * gain).astype(jnp.bfloat16)


def iota(shape, dim):
    return lax.broadcasted_iota(jnp.int32, shape, dim)


def layer_kernel(n, x_h, pos_h, wdq_h, wuq_h, wqr_h, wdkv_h, wkr_h, wuk_h, wuv_h, wout_h, gq_h, gkv_h, y_v,
                 x_v, pos_v, wdq_v, wuq_v, wqr_v, wdkv_v, wkr_v, wuk_v, wuv_v, wout_v, gq_v, gkv_v,
                 lat, kv_v, cq_v, qcat, kt_v, krt_v, v_v, bias_v, o_v, s_v, p_v, l_v, y_sum, in_sem, send_sem, recv_sem):
    rows, width = x_v.shape
    kv_rank = wdkv_v.shape[1]
    rope = wkr_v.shape[0]
    half_rope = rope // 2
    pairs = kt_v.shape[0]
    nope = LANES // 2
    half = rows // 2
    chips = n // 2
    keys = chips * rows
    pack_rows = PACK_ROWS // PACKS
    steps = pairs // GROUP
    deep = GROUP * LANES
    panel = 2 * LANES

    me = lax.axis_index("ctx")
    my_chip = me // 2
    partner = me + 1 - 2 * lax.rem(me, 2)
    odd = lax.rem(me, 2) == 1

    def chip_at(slot):
        return jnp.where(slot == 0, my_chip, jnp.where(slot > my_chip, slot, slot - 1))


    fetches = []

    def fetch(src, dst):
        fetches.append(pltpu.make_async_copy(src, dst, in_sem.at[len(fetches)]))
        return fetches[-1]

    def start(*copies):
        for cp in copies:
            cp.start()

    get_pos = fetch(pos_h, pos_v)
    get_x = fetch(x_h, x_v)
    get_wkr = fetch(wkr_h, wkr_v)
    depth = 2 * LANES
    cuts = [width // depth * c // 10 * depth for c in KV_CUTS]
    get_wdkv = [fetch(wdkv_h.at[pl.ds(lo, hi - lo)], wdkv_v.at[pl.ds(lo, hi - lo)]) for lo, hi in zip(cuts, cuts[1:])]
    get_gkv = fetch(gkv_h, gkv_v)
    get_gq = fetch(gq_h, gq_v)
    get_wdq = fetch(wdq_h, wdq_v)
    get_wuq = fetch(wuq_h, wuq_v)
    get_wqr = fetch(wqr_h, wqr_v)
    get_wuk = fetch(wuk_h, wuk_v)
    get_wuv = fetch(wuv_h, wuv_v)
    get_wout = [fetch(wout_h.at[pl.ds(g * deep, deep)], wout_v.at[pl.ds(g * deep, deep)]) for g in range(steps)]
    start(get_pos, get_x, get_wkr, get_gkv, *get_wdkv, get_gq, get_wdq, get_wuq, get_wqr, get_wuk, get_wuv, *get_wout)

    barrier = pltpu.get_barrier_semaphore()
    pl.semaphore_signal(barrier, inc=1, device_id={"ctx": partner}, device_id_type=MESH)

    @pl.when(odd)
    def _():
        for t in range(1, chips):
            for d in range(2):
                pl.semaphore_signal(barrier, inc=1, device_id={"ctx": 2 * chip_at(t) + d}, device_id_type=MESH)

    get_pos.wait()
    get_x.wait()
    get_wkr.wait()
    pos_row = pos_v[...].astype(jnp.float32)

    def pos_of(count, index):
        spot = iota((count, rows), 1) == index(iota((count, rows), 0))
        return jnp.sum(jnp.where(spot, jnp.broadcast_to(pos_row, (count, rows)), 0.0), axis=1, keepdims=True)

    lane = iota((rows, LANES), 1)
    freq_id = lax.rem(lane[:1], half_rope)
    inv_freq = jnp.zeros((1, LANES), jnp.float32)
    for f in range(half_rope):
        inv_freq = jnp.where(freq_id == f, float(np.float32(10000.0 ** (-2.0 * f / rope))), inv_freq)
    angles = pos_of(rows, lambda r: r) * inv_freq
    first = lax.rem(lane, rope) < half_rope
    cos_tab = jnp.cos(angles)
    sin_tab = jnp.sin(angles)
    sin_tab = jnp.where(first, -sin_tab, sin_tab)

    def rope_lanes(a):
        other = jnp.where(first, pltpu.roll(a, LANES - half_rope, 1), pltpu.roll(a, half_rope, 1))
        return (a * cos_tab + other * sin_tab).astype(jnp.bfloat16)

    count = 2 * rows
    q_pos = pos_of(count, lambda r: lax.rem(r, half) + jnp.where(r >= rows, half, 0)).astype(jnp.int32)
    q_row = iota((count, 1), 0)
    q_seq = jnp.where(q_row < rows, half * me, half * (2 * n - 1 - me)) + lax.rem(q_row, half)
    q_first = q_seq - q_pos
    col = iota((1, keys), 1)
    slot = col // rows
    swapped = slot + 1 - 2 * lax.rem(slot, 2)
    inner = lax.rem(col, rows)

    def key_seq(slot, late):
        dev = 2 * chip_at(slot) + inner // half
        return half * jnp.where(late, 2 * n - 1 - dev, dev) + lax.rem(inner, half)

    def visible(seq, lo, hi):
        return jnp.where((seq >= lo) & (seq <= hi), 0.0, MASKED)

    bias_v[:count] = visible(key_seq(slot, False), q_first, q_seq)
    bias_v[count:] = visible(key_seq(swapped, True), q_first[rows:], q_seq[rows:])

    kr = mm(x_v[...], wkr_v[...], NT)
    for get in get_wdkv:
        get.wait()
    for i in range(kv_rank // LANES):
        kv_v[:, i * LANES:(i + 1) * LANES] = mm(x_v[...], wdkv_v[:, i * LANES:(i + 1) * LANES])
    kv = kv_v[...]
    get_gkv.wait()
    c_kv = rms_norm(kv, gkv_v[...].astype(jnp.float32).reshape(1, -1))
    lat[me, :rows, :] = c_kv
    kr = rope_lanes(jnp.concatenate([kr] * (LANES // rope), axis=1))
    packed = jnp.zeros((PACK_ROWS, LANES), jnp.float32)
    kr = kr.astype(jnp.float32)
    part = iota((PACK_ROWS, LANES), 1) // rope
    for s in range(rows // PACK_ROWS):
        packed = jnp.where(part == s, kr[s * PACK_ROWS:(s + 1) * PACK_ROWS], packed)
    for i in range(PACKS):
        lat[me, rows:, i * LANES:(i + 1) * LANES] = packed[i * pack_rows:(i + 1) * pack_rows].astype(jnp.bfloat16)

    pl.semaphore_wait(barrier, chips)

    def push(block, peer, index):
        return pltpu.make_async_remote_copy(src_ref=lat.at[block], dst_ref=lat.at[block], send_sem=send_sem.at[index],
                                            recv_sem=recv_sem.at[block], device_id={"ctx": peer}, device_id_type=MESH)

    sends = [push(me, 2 * chip_at(t) + 1, t) for t in range(1, chips)] + [push(me, partner, 0)]
    start(*sends)

    def forward(t):
        return [push(2 * chip_at(t) + d, partner, chips + 2 * (t - 1) + d) for d in range(2)]

    def relay(t):
        for d, cp in enumerate(forward(t)):
            push(2 * chip_at(t) + d, me, 0).wait_recv()
            cp.start()

    get_gq.wait()
    get_wdq.wait()
    cq_v[...] = rms_norm(mm(x_v[...], wdq_v[...]), gq_v[...].astype(jnp.float32).reshape(1, -1))
    low = lane < nope
    zero = jnp.zeros((rows, LANES), jnp.bfloat16)

    def put_query(head, cols, t):
        at = head % 2 * half
        qcat[head // 2, at:at + half, cols] = t[:half]
        qcat[head // 2, rows + at:rows + at + half, cols] = t[half:]

    get_wuq.wait()
    for c in range(pairs // 4):
        q = mm(cq_v[...], wuq_v[:, c * 4 * LANES:(c + 1) * 4 * LANES]).astype(jnp.bfloat16)
        for i in range(4):
            t = q[:, i * LANES:(i + 1) * LANES]
            put_query(2 * (c * 4 + i), slice(0, LANES), jnp.where(low, t, zero))
            put_query(2 * (c * 4 + i) + 1, slice(0, LANES), jnp.where(low, zero, t))
    get_wqr.wait()
    per = LANES // rope
    for c in range(pairs // per):
        q = mm(cq_v[...], wqr_v[:, c * 2 * LANES:(c + 1) * 2 * LANES])
        for i in range(2):
            t = rope_lanes(q[:, i * LANES:(i + 1) * LANES])
            for s in range(per):
                put_query((c * 2 + i) * per + s, slice(LANES, 2 * LANES), jnp.where(lane // rope == s, t, zero))

    same = lax.rem(iota((LANES, LANES), 0), rope) == lax.rem(iota((LANES, LANES), 1), rope)
    same = jnp.where(same, 1.0, 0.0).astype(jnp.bfloat16)

    def up_project(slots):
        pieces, packs = [], []
        groups = half // PACK_ROWS
        for t in slots:
            chip = chip_at(t)
            block = lat[pl.ds(2 * chip, 2), :rows]
            tails = [lat[2 * chip + d, rows:].astype(jnp.float32) for d in range(2)]
            tails = [jnp.concatenate([a[:, i * LANES:(i + 1) * LANES] for i in range(PACKS)], axis=0) for a in tails]
            for p in [t % 2, 1 - t % 2]:
                pieces.append(block[:, p * half:(p + 1) * half].reshape(rows, kv_rank))
                packs += [jnp.where(part == p * groups + s, tails[d], 0.0).astype(jnp.bfloat16) for d in range(2) for s in range(groups)]
        c_all = jnp.concatenate(pieces, axis=0)
        krt = mm(same, jnp.concatenate(packs, axis=0), NT).astype(jnp.bfloat16)
        spots = [((t + i) % 2, (t - t % 2 + i) * rows, (2 * j + i) * rows) for j, t in enumerate(slots) for i in range(2)]
        for p, at, src in spots:
            krt_v[p, :, at:at + rows] = krt[:, src:src + rows]
        for c in range(pairs // 2):
            cols = slice(c * 2 * LANES, (c + 1) * 2 * LANES)
            k = mm(c_all, wuk_v[:, cols]).astype(jnp.bfloat16)
            for i in range(2):
                kt = k[:, i * LANES:(i + 1) * LANES].T
                for p, at, src in spots:
                    kt_v[2 * c + i, p, :, at:at + rows] = kt[:, src:src + rows]
        for c in range(pairs // 2):
            cols = slice(c * 2 * LANES, (c + 1) * 2 * LANES)
            v = mm(c_all, wuv_v[:, cols]).astype(jnp.bfloat16)
            for i in range(2):
                for p, at, src in spots:
                    v_v[2 * c + i, p, at:at + rows] = v[src:src + rows, i * LANES:(i + 1) * LANES]

    get_wuk.wait()
    get_wuv.wait()
    push(partner, me, 0).wait_recv()
    for t in range(0, chips, 2):
        slots = [u for u in (t, t + 1) if u > 0]

        @pl.when(odd)
        def _():
            for u in slots:
                relay(u)

        @pl.when(jnp.logical_not(odd))
        def _():
            for u in slots:
                for d in range(2):
                    push(2 * chip_at(u) + d, me, 0).wait_recv()

        up_project([t, t + 1])

    factor = (nope + rope) ** -0.5 * math.log2(math.e)

    def scores(g):
        for i in range(GROUP):
            p = g * GROUP + i
            early = jnp.concatenate([kt_v[p, 0], krt_v[0]], axis=0)
            late = jnp.concatenate([kt_v[p, 1], krt_v[1]], axis=0)
            s_v[g % 2, i, :count] = mm(qcat[p], early) * factor + bias_v[:count]
            s_v[g % 2, i, count:] = mm(qcat[p, rows:], late) * factor + bias_v[count:]

    def halves(a, op):
        return op(a[:, :LANES], a[:, LANES:])

    def weights(g):
        for i in range(GROUP):
            a, b, c = s_v[g % 2, i, :rows], s_v[g % 2, i, rows:count], s_v[g % 2, i, count:]
            m_a = jnp.max(halves(a, jnp.maximum), axis=1, keepdims=True)
            m_b = jnp.max(jnp.maximum(halves(b, jnp.maximum), halves(c, jnp.maximum)), axis=1, keepdims=True)
            a, b, c = jnp.exp2(a - m_a), jnp.exp2(b - m_b), jnp.exp2(c - m_b)
            p_v[g % 2, i, :rows] = a.astype(jnp.bfloat16)
            p_v[g % 2, i, rows:count] = b.astype(jnp.bfloat16)
            p_v[g % 2, i, count:] = c.astype(jnp.bfloat16)
            l_a = jnp.sum(halves(a, jnp.add), axis=1, keepdims=True)
            l_b = jnp.sum(halves(b, jnp.add) + halves(c, jnp.add), axis=1, keepdims=True)
            l_v[g % 2, i, :rows] = jnp.broadcast_to(1.0 / l_a, (rows, LANES))
            l_v[g % 2, i, rows:] = jnp.broadcast_to(1.0 / l_b, (rows, LANES))

    def values(g):
        for i in range(GROUP):
            cols = slice((g * GROUP + i) * LANES, (g * GROUP + i + 1) * LANES)
            o = mm(p_v[g % 2, i, :count], v_v[g * GROUP + i, 0])
            o_a = o[:rows] * l_v[g % 2, i, :rows]
            o_b = (o[rows:] + mm(p_v[g % 2, i, count:], v_v[g * GROUP + i, 1])) * l_v[g % 2, i, rows:]
            o_v[:half, cols] = jnp.where(low[:half], o_a[:half], o_a[half:]).astype(jnp.bfloat16)
            o_v[half:, cols] = jnp.where(low[:half], o_b[:half], o_b[half:]).astype(jnp.bfloat16)

    def project(g):
        for c in range(width // panel):
            cols = slice(c * panel, (c + 1) * panel)
            y = mm(o_v[:, g * deep:(g + 1) * deep], wout_v[g * deep:(g + 1) * deep, cols])
            if g > 0:
                y += y_sum[:, cols]
            if g + 1 < steps:
                y_sum[:, cols] = y
            else:
                y_v[:, cols] = y.astype(jnp.bfloat16)

    for g in range(steps + 3):
        if g == 3:
            for get in get_wout:
                get.wait()
        if g >= 3:
            project(g - 3)
        if 2 <= g < steps + 2:
            values(g - 2)
        if 1 <= g <= steps:
            weights(g - 1)
        if g < steps:
            scores(g)
    for cp in sends:
        cp.wait_send()

    @pl.when(odd)
    def _():
        for t in range(1, chips):
            for cp in forward(t):
                cp.wait_send()


def solution(mesh):
    n = mesh.shape["ctx"]
    row_spec = P(("dp", "ctx"), None)
    id_spec = P(("dp", "ctx"))

    def per_device(x, pos, seg, w_dq, w_uq, w_qr, w_dkv, w_kr, w_uk, w_uv, w_out, gain_q, gain_kv):
        rows, width = x.shape
        pairs = w_uq.shape[1] // LANES
        keys = n * rows
        kv_rank = w_dkv.shape[1]
        bf, f32 = jnp.bfloat16, jnp.float32
        args = (x, pos.reshape(1, rows), w_dq, w_uq, w_qr, w_dkv, w_kr.T, w_uk, w_uv, w_out,
                gain_q, gain_kv)
        scratch = [pltpu.VMEM(a.shape, a.dtype) for a in args]
        scratch += [
            pltpu.VMEM((n, rows + PACK_ROWS // PACKS, kv_rank), bf),
            pltpu.VMEM((rows, kv_rank), f32),
            pltpu.VMEM((rows, w_dq.shape[1]), bf),
            pltpu.VMEM((pairs, 2 * rows, 2 * LANES), bf),
            pltpu.VMEM((pairs, 2, LANES, keys // 2), bf),
            pltpu.VMEM((2, LANES, keys // 2), bf),
            pltpu.VMEM((pairs, 2, keys // 2, LANES), bf),
            pltpu.VMEM((3 * rows, keys // 2), f32),
            pltpu.VMEM((rows, w_uv.shape[1]), bf),
            pltpu.VMEM((2, GROUP, 3 * rows, keys // 2), f32),
            pltpu.VMEM((2, GROUP, 3 * rows, keys // 2), bf),
            pltpu.VMEM((2, GROUP, 2 * rows, LANES), f32),
            pltpu.VMEM((rows, width), f32),
            pltpu.SemaphoreType.DMA((len(args) - 2 + len(KV_CUTS) - 1 + pairs // GROUP,)),
            pltpu.SemaphoreType.DMA((n // 2 + n - 2,)),
            pltpu.SemaphoreType.DMA((n,)),
        ]
        return pl.pallas_call(
            functools.partial(layer_kernel, n),
            out_shape=pltpu.VMEM(x.shape, bf),
            in_specs=[pl.BlockSpec(memory_space=pltpu.HBM)] * len(args),
            out_specs=pl.BlockSpec(memory_space=pltpu.VMEM),
            scratch_shapes=scratch,
            compiler_params=pltpu.CompilerParams(collective_id=0, has_side_effects=True, vmem_limit_bytes=62000000),
        )(*args)

    return jax.shard_map(per_device, mesh=mesh, in_specs=(row_spec, id_spec, id_spec) + (P(),) * 10, out_specs=row_spec, check_vma=False)
```

```python
import functools
import math

import jax
import jax.numpy as jnp
import numpy as np
from jax import lax
from jax.experimental import pallas as pl
from jax.experimental.pallas import tpu as pltpu
from jax.sharding import PartitionSpec as P

NORM_EPS = 1e-6
MASKED = -1e30
LANES = 128
PACK_ROWS = 16
PACKS = 2
GROUP = 4
KV_CUTS = (0, 2, 4, 6, 8, 10)
MESH = pl.DeviceIdType.MESH
NT = (((1,), (1,)), ((), ()))


def mm(a, b, dims=(((1,), (0,)), ((), ()))):
    return lax.dot_general(a, b, dims, preferred_element_type=jnp.float32)


def rms_norm(vals, gain):
    mean_sq = jnp.mean(vals * vals, axis=-1, keepdims=True)
    return (vals * lax.rsqrt(mean_sq + NORM_EPS) * gain).astype(jnp.bfloat16)


def iota(shape, dim):
    return lax.broadcasted_iota(jnp.int32, shape, dim)


def layer_kernel(n, x_h, pos_h, wdq_h, wuq_h, wqr_h, wdkv_h, wkr_h, wuk_h, wuv_h, wout_h, gq_h, gkv_h, y_v,
                 x_v, pos_v, wdq_v, wuq_v, wqr_v, wdkv_v, wkr_v, wuk_v, wuv_v, wout_v, gq_v, gkv_v,
                 lat, kv_v, cq_v, qcat, kt_v, krt_v, v_v, bias_v, o_v, s_v, p_v, l_v, y_sum, in_sem, send_sem, recv_sem):
    rows, width = x_v.shape
    kv_rank = wdkv_v.shape[1]
    rope = wkr_v.shape[0]
    half_rope = rope // 2
    pairs = kt_v.shape[0]
    nope = LANES // 2
    half = rows // 2
    chips = n // 2
    keys = chips * rows
    pack_rows = PACK_ROWS // PACKS
    steps = pairs // GROUP
    deep = GROUP * LANES
    panel = 2 * LANES

    me = lax.axis_index("ctx")
    my_chip = me // 2
    partner = me + 1 - 2 * lax.rem(me, 2)
    odd = lax.rem(me, 2) == 1

    def chip_at(slot):
        return jnp.where(slot == 0, my_chip, jnp.where(slot > my_chip, slot, slot - 1))


    fetches = []

    def fetch(src, dst):
        fetches.append(pltpu.make_async_copy(src, dst, in_sem.at[len(fetches)]))
        return fetches[-1]

    def start(*copies):
        for cp in copies:
            cp.start()

    get_pos = fetch(pos_h, pos_v)
    get_x = fetch(x_h, x_v)
    get_wkr = fetch(wkr_h, wkr_v)
    depth = 2 * LANES
    cuts = [width // depth * c // 10 * depth for c in KV_CUTS]
    get_wdkv = [fetch(wdkv_h.at[pl.ds(lo, hi - lo)], wdkv_v.at[pl.ds(lo, hi - lo)]) for lo, hi in zip(cuts, cuts[1:])]
    get_gkv = fetch(gkv_h, gkv_v)
    get_gq = fetch(gq_h, gq_v)
    get_wdq = fetch(wdq_h, wdq_v)
    get_wuq = fetch(wuq_h, wuq_v)
    get_wqr = fetch(wqr_h, wqr_v)
    get_wuk = fetch(wuk_h, wuk_v)
    get_wuv = fetch(wuv_h, wuv_v)
    get_wout = [fetch(wout_h.at[pl.ds(g * deep, deep)], wout_v.at[pl.ds(g * deep, deep)]) for g in range(steps)]
    start(get_pos, get_x, get_wkr, get_gkv, *get_wdkv, get_gq, get_wdq, get_wuq, get_wqr, get_wuk, get_wuv, *get_wout)

    barrier = pltpu.get_barrier_semaphore()
    pl.semaphore_signal(barrier, inc=1, device_id={"ctx": partner}, device_id_type=MESH)

    @pl.when(odd)
    def _():
        for t in range(1, chips):
            for d in range(2):
                pl.semaphore_signal(barrier, inc=1, device_id={"ctx": 2 * chip_at(t) + d}, device_id_type=MESH)

    get_pos.wait()
    get_x.wait()
    get_wkr.wait()
    pos_row = pos_v[...].astype(jnp.float32)

    def pos_of(count, index):
        spot = iota((count, rows), 1) == index(iota((count, rows), 0))
        return jnp.sum(jnp.where(spot, jnp.broadcast_to(pos_row, (count, rows)), 0.0), axis=1, keepdims=True)

    lane = iota((rows, LANES), 1)
    freq_id = lax.rem(lane[:1], half_rope)
    inv_freq = jnp.zeros((1, LANES), jnp.float32)
    for f in range(half_rope):
        inv_freq = jnp.where(freq_id == f, float(np.float32(10000.0 ** (-2.0 * f / rope))), inv_freq)
    angles = pos_of(rows, lambda r: r) * inv_freq
    first = lax.rem(lane, rope) < half_rope
    cos_tab = jnp.cos(angles)
    sin_tab = jnp.sin(angles)
    sin_tab = jnp.where(first, -sin_tab, sin_tab)

    def rope_lanes(a):
        other = jnp.where(first, pltpu.roll(a, LANES - half_rope, 1), pltpu.roll(a, half_rope, 1))
        return (a * cos_tab + other * sin_tab).astype(jnp.bfloat16)

    count = 2 * rows
    q_pos = pos_of(count, lambda r: lax.rem(r, half) + jnp.where(r >= rows, half, 0)).astype(jnp.int32)
    q_row = iota((count, 1), 0)
    q_seq = jnp.where(q_row < rows, half * me, half * (2 * n - 1 - me)) + lax.rem(q_row, half)
    q_first = q_seq - q_pos
    col = iota((1, keys), 1)
    slot = col // rows
    swapped = slot + 1 - 2 * lax.rem(slot, 2)
    inner = lax.rem(col, rows)

    def key_seq(slot, late):
        dev = 2 * chip_at(slot) + inner // half
        return half * jnp.where(late, 2 * n - 1 - dev, dev) + lax.rem(inner, half)

    def visible(seq, lo, hi):
        return jnp.where((seq >= lo) & (seq <= hi), 0.0, MASKED)

    bias_v[:count] = visible(key_seq(slot, False), q_first, q_seq)
    bias_v[count:] = visible(key_seq(swapped, True), q_first[rows:], q_seq[rows:])

    kr = mm(x_v[...], wkr_v[...], NT)
    for get in get_wdkv:
        get.wait()
    for i in range(kv_rank // LANES):
        kv_v[:, i * LANES:(i + 1) * LANES] = mm(x_v[...], wdkv_v[:, i * LANES:(i + 1) * LANES])
    kv = kv_v[...]
    get_gkv.wait()
    c_kv = rms_norm(kv, gkv_v[...].astype(jnp.float32).reshape(1, -1))
    lat[me, :rows, :] = c_kv
    kr = rope_lanes(jnp.concatenate([kr] * (LANES // rope), axis=1))
    packed = jnp.zeros((PACK_ROWS, LANES), jnp.float32)
    kr = kr.astype(jnp.float32)
    part = iota((PACK_ROWS, LANES), 1) // rope
    for s in range(rows // PACK_ROWS):
        packed = jnp.where(part == s, kr[s * PACK_ROWS:(s + 1) * PACK_ROWS], packed)
    for i in range(PACKS):
        lat[me, rows:, i * LANES:(i + 1) * LANES] = packed[i * pack_rows:(i + 1) * pack_rows].astype(jnp.bfloat16)

    pl.semaphore_wait(barrier, chips)

    def push(block, peer, index):
        return pltpu.make_async_remote_copy(src_ref=lat.at[block], dst_ref=lat.at[block], send_sem=send_sem.at[index],
                                            recv_sem=recv_sem.at[block], device_id={"ctx": peer}, device_id_type=MESH)

    sends = [push(me, 2 * chip_at(t) + 1, t) for t in range(1, chips)] + [push(me, partner, 0)]
    start(*sends)

    def forward(t):
        return [push(2 * chip_at(t) + d, partner, chips + 2 * (t - 1) + d) for d in range(2)]

    def relay(t):
        for d, cp in enumerate(forward(t)):
            push(2 * chip_at(t) + d, me, 0).wait_recv()
            cp.start()

    get_gq.wait()
    get_wdq.wait()
    cq_v[...] = rms_norm(mm(x_v[...], wdq_v[...]), gq_v[...].astype(jnp.float32).reshape(1, -1))
    low = lane < nope
    zero = jnp.zeros((rows, LANES), jnp.bfloat16)

    def put_query(head, cols, t):
        at = head % 2 * half
        qcat[head // 2, at:at + half, cols] = t[:half]
        qcat[head // 2, rows + at:rows + at + half, cols] = t[half:]

    get_wuq.wait()
    for c in range(pairs // 4):
        q = mm(cq_v[...], wuq_v[:, c * 4 * LANES:(c + 1) * 4 * LANES]).astype(jnp.bfloat16)
        for i in range(4):
            t = q[:, i * LANES:(i + 1) * LANES]
            put_query(2 * (c * 4 + i), slice(0, LANES), jnp.where(low, t, zero))
            put_query(2 * (c * 4 + i) + 1, slice(0, LANES), jnp.where(low, zero, t))
    get_wqr.wait()
    per = LANES // rope
    for c in range(pairs // per):
        q = mm(cq_v[...], wqr_v[:, c * 2 * LANES:(c + 1) * 2 * LANES])
        for i in range(2):
            t = rope_lanes(q[:, i * LANES:(i + 1) * LANES])
            for s in range(per):
                put_query((c * 2 + i) * per + s, slice(LANES, LANES + rope), t[:, s * rope:(s + 1) * rope])

    same = iota((rope, LANES), 0) == lax.rem(iota((rope, LANES), 1), rope)
    same = jnp.where(same, 1.0, 0.0).astype(jnp.bfloat16)

    def up_project(slots):
        pieces, packs = [], []
        groups = half // PACK_ROWS
        for t in slots:
            chip = chip_at(t)
            block = lat[pl.ds(2 * chip, 2), :rows]
            tails = [lat[2 * chip + d, rows:].astype(jnp.float32) for d in range(2)]
            tails = [jnp.concatenate([a[:, i * LANES:(i + 1) * LANES] for i in range(PACKS)], axis=0) for a in tails]
            for p in [t % 2, 1 - t % 2]:
                pieces.append(block[:, p * half:(p + 1) * half].reshape(rows, kv_rank))
                packs += [jnp.where(part == p * groups + s, tails[d], 0.0).astype(jnp.bfloat16) for d in range(2) for s in range(groups)]
        c_all = jnp.concatenate(pieces, axis=0)
        krt = mm(same, jnp.concatenate(packs, axis=0), NT).astype(jnp.bfloat16)
        spots = [((t + i) % 2, (t - t % 2 + i) * rows, (2 * j + i) * rows) for j, t in enumerate(slots) for i in range(2)]
        for p, at, src in spots:
            krt_v[p, :, at:at + rows] = krt[:, src:src + rows]
        for c in range(pairs // 2):
            cols = slice(c * 2 * LANES, (c + 1) * 2 * LANES)
            k = mm(c_all, wuk_v[:, cols]).astype(jnp.bfloat16)
            for i in range(2):
                kt = k[:, i * LANES:(i + 1) * LANES].T
                for p, at, src in spots:
                    kt_v[2 * c + i, p, :, at:at + rows] = kt[:, src:src + rows]
        for c in range(pairs // 2):
            cols = slice(c * 2 * LANES, (c + 1) * 2 * LANES)
            v = mm(c_all, wuv_v[:, cols]).astype(jnp.bfloat16)
            for i in range(2):
                for p, at, src in spots:
                    v_v[2 * c + i, p, at:at + rows] = v[src:src + rows, i * LANES:(i + 1) * LANES]

    get_wuk.wait()
    get_wuv.wait()
    def receive(t):
        for d in range(2):
            push(2 * chip_at(t) + d, me, 0).wait_recv()

    even = jnp.logical_not(odd)
    push(partner, me, 0).wait_recv()
    pl.when(odd)(lambda: relay(1))
    pl.when(even)(lambda: receive(1))
    up_project([0, 1])

    @pl.when(odd)
    def _():
        for t in range(2, chips):
            relay(t)

    for t in range(2, chips):
        pl.when(even)(functools.partial(receive, t))
        up_project([t])

    factor = (nope + rope) ** -0.5 * math.log2(math.e)

    def scores(g):
        for i in range(GROUP):
            p = g * GROUP + i
            early = jnp.concatenate([kt_v[p, 0], krt_v[0]], axis=0)
            late = jnp.concatenate([kt_v[p, 1], krt_v[1]], axis=0)
            s_v[g % 2, i, :count] = mm(qcat[p], early) * factor + bias_v[:count]
            s_v[g % 2, i, count:] = mm(qcat[p, rows:], late) * factor + bias_v[count:]

    def halves(a, op):
        return op(a[:, :LANES], a[:, LANES:])

    def weights(g):
        for i in range(GROUP):
            a, b, c = s_v[g % 2, i, :rows], s_v[g % 2, i, rows:count], s_v[g % 2, i, count:]
            m_a = jnp.max(halves(a, jnp.maximum), axis=1, keepdims=True)
            m_b = jnp.max(jnp.maximum(halves(b, jnp.maximum), halves(c, jnp.maximum)), axis=1, keepdims=True)
            a, b, c = jnp.exp2(a - m_a), jnp.exp2(b - m_b), jnp.exp2(c - m_b)
            p_v[g % 2, i, :rows] = a.astype(jnp.bfloat16)
            p_v[g % 2, i, rows:count] = b.astype(jnp.bfloat16)
            p_v[g % 2, i, count:] = c.astype(jnp.bfloat16)
            l_a = jnp.sum(halves(a, jnp.add), axis=1, keepdims=True)
            l_b = jnp.sum(halves(b, jnp.add) + halves(c, jnp.add), axis=1, keepdims=True)
            l_v[g % 2, i, :rows] = jnp.broadcast_to(1.0 / l_a, (rows, LANES))
            l_v[g % 2, i, rows:] = jnp.broadcast_to(1.0 / l_b, (rows, LANES))

    def values(g):
        for i in range(GROUP):
            cols = slice((g * GROUP + i) * LANES, (g * GROUP + i + 1) * LANES)
            o = mm(p_v[g % 2, i, :count], v_v[g * GROUP + i, 0])
            o_a = o[:rows] * l_v[g % 2, i, :rows]
            o_b = (o[rows:] + mm(p_v[g % 2, i, count:], v_v[g * GROUP + i, 1])) * l_v[g % 2, i, rows:]
            o_v[:half, cols] = jnp.where(low[:half], o_a[:half], o_a[half:]).astype(jnp.bfloat16)
            o_v[half:, cols] = jnp.where(low[:half], o_b[:half], o_b[half:]).astype(jnp.bfloat16)

    def project(g):
        for c in range(width // panel):
            cols = slice(c * panel, (c + 1) * panel)
            y = mm(o_v[:, g * deep:(g + 1) * deep], wout_v[g * deep:(g + 1) * deep, cols])
            if g > 0:
                y += y_sum[:, cols]
            if g + 1 < steps:
                y_sum[:, cols] = y
            else:
                y_v[:, cols] = y.astype(jnp.bfloat16)

    for g in range(steps + 3):
        if g == 3:
            for get in get_wout:
                get.wait()
        if g >= 3:
            project(g - 3)
        if 2 <= g < steps + 2:
            values(g - 2)
        if 1 <= g <= steps:
            weights(g - 1)
        if g < steps:
            scores(g)
    for cp in sends:
        cp.wait_send()

    @pl.when(odd)
    def _():
        for t in range(1, chips):
            for cp in forward(t):
                cp.wait_send()


def solution(mesh):
    n = mesh.shape["ctx"]
    row_spec = P(("dp", "ctx"), None)
    id_spec = P(("dp", "ctx"))

    def per_device(x, pos, seg, w_dq, w_uq, w_qr, w_dkv, w_kr, w_uk, w_uv, w_out, gain_q, gain_kv):
        rows, width = x.shape
        pairs = w_uq.shape[1] // LANES
        keys = n * rows
        kv_rank = w_dkv.shape[1]
        rope = w_kr.shape[1]
        bf, f32 = jnp.bfloat16, jnp.float32
        args = (x, pos.reshape(1, rows), w_dq, w_uq, w_qr, w_dkv, w_kr.T, w_uk, w_uv, w_out,
                gain_q, gain_kv)
        scratch = [pltpu.VMEM(a.shape, a.dtype) for a in args]
        scratch += [
            pltpu.VMEM((n, rows + PACK_ROWS // PACKS, kv_rank), bf),
            pltpu.VMEM((rows, kv_rank), f32),
            pltpu.VMEM((rows, w_dq.shape[1]), bf),
            pltpu.VMEM((pairs, 2 * rows, LANES + rope), bf),
            pltpu.VMEM((pairs, 2, LANES, keys // 2), bf),
            pltpu.VMEM((2, rope, keys // 2), bf),
            pltpu.VMEM((pairs, 2, keys // 2, LANES), bf),
            pltpu.VMEM((3 * rows, keys // 2), f32),
            pltpu.VMEM((rows, w_uv.shape[1]), bf),
            pltpu.VMEM((2, GROUP, 3 * rows, keys // 2), f32),
            pltpu.VMEM((2, GROUP, 3 * rows, keys // 2), bf),
            pltpu.VMEM((2, GROUP, 2 * rows, LANES), f32),
            pltpu.VMEM((rows, width), f32),
            pltpu.SemaphoreType.DMA((len(args) - 2 + len(KV_CUTS) - 1 + pairs // GROUP,)),
            pltpu.SemaphoreType.DMA((n // 2 + n - 2,)),
            pltpu.SemaphoreType.DMA((n,)),
        ]
        return pl.pallas_call(
            functools.partial(layer_kernel, n),
            out_shape=pltpu.VMEM(x.shape, bf),
            in_specs=[pl.BlockSpec(memory_space=pltpu.HBM)] * len(args),
            out_specs=pl.BlockSpec(memory_space=pltpu.VMEM),
            scratch_shapes=scratch,
            compiler_params=pltpu.CompilerParams(collective_id=0, has_side_effects=True, vmem_limit_bytes=62000000),
        )(*args)

    return jax.shard_map(per_device, mesh=mesh, in_specs=(row_spec, id_spec, id_spec) + (P(),) * 10, out_specs=row_spec, check_vma=False)
```

```python
import functools
import math

import jax
import jax.numpy as jnp
import numpy as np
from jax import lax
from jax.experimental import pallas as pl
from jax.experimental.pallas import tpu as pltpu
from jax.sharding import PartitionSpec as P

NORM_EPS = 1e-6
MASKED = -1e30
LANES = 128
PACK_ROWS = 16
PACKS = 2
GROUP = 4
KV_CUTS = (0, 2, 4, 6, 8, 10)
MESH = pl.DeviceIdType.MESH
NT = (((1,), (1,)), ((), ()))


def mm(a, b, dims=(((1,), (0,)), ((), ()))):
    return lax.dot_general(a, b, dims, preferred_element_type=jnp.float32)


def rms_norm(vals, gain):
    mean_sq = jnp.mean(vals * vals, axis=-1, keepdims=True)
    return (vals * lax.rsqrt(mean_sq + NORM_EPS) * gain).astype(jnp.bfloat16)


def iota(shape, dim):
    return lax.broadcasted_iota(jnp.int32, shape, dim)


def layer_kernel(n, x_h, pos_h, wdq_h, wuq_h, wqr_h, wdkv_h, wkr_h, wuk_h, wuv_h, wout_h, gq_h, gkv_h, y_v,
                 x_v, pos_v, wdq_v, wuq_v, wqr_v, wdkv_v, wkr_v, wuk_v, wuv_v, wout_v, gq_v, gkv_v,
                 lat, kv_v, cq_v, qcat, kt_v, krt_v, v_v, bias_v, o_v, s_v, p_v, l_v, y_sum, fs_v, fp_v, fl_v, in_sem, send_sem, recv_sem):
    rows, width = x_v.shape
    kv_rank = wdkv_v.shape[1]
    rope = wkr_v.shape[0]
    half_rope = rope // 2
    pairs = kt_v.shape[0]
    nope = LANES // 2
    half = rows // 2
    chips = n // 2
    keys = chips * rows
    pack_rows = PACK_ROWS // PACKS
    steps = pairs // GROUP
    deep = GROUP * LANES
    panel = 2 * LANES

    me = lax.axis_index("ctx")
    my_chip = me // 2
    partner = me + 1 - 2 * lax.rem(me, 2)
    odd = lax.rem(me, 2) == 1

    def chip_at(slot):
        return jnp.where(slot == 0, my_chip, jnp.where(slot > my_chip, slot, slot - 1))


    fetches = []

    def fetch(src, dst):
        fetches.append(pltpu.make_async_copy(src, dst, in_sem.at[len(fetches)]))
        return fetches[-1]

    def start(*copies):
        for cp in copies:
            cp.start()

    get_pos = fetch(pos_h, pos_v)
    get_x = fetch(x_h, x_v)
    get_wkr = fetch(wkr_h, wkr_v)
    depth = 2 * LANES
    cuts = [width // depth * c // 10 * depth for c in KV_CUTS]
    get_wdkv = [fetch(wdkv_h.at[pl.ds(lo, hi - lo)], wdkv_v.at[pl.ds(lo, hi - lo)]) for lo, hi in zip(cuts, cuts[1:])]
    get_gkv = fetch(gkv_h, gkv_v)
    get_gq = fetch(gq_h, gq_v)
    get_wdq = fetch(wdq_h, wdq_v)
    get_wuq = fetch(wuq_h, wuq_v)
    get_wqr = fetch(wqr_h, wqr_v)
    get_wuk = fetch(wuk_h, wuk_v)
    get_wuv = fetch(wuv_h, wuv_v)
    get_wout = [fetch(wout_h.at[pl.ds(g * deep, deep)], wout_v.at[pl.ds(g * deep, deep)]) for g in range(steps)]
    start(get_pos, get_x, get_wkr, get_gkv, *get_wdkv, get_gq, get_wdq, get_wuq, get_wqr, get_wuk, get_wuv, *get_wout)

    barrier = pltpu.get_barrier_semaphore()
    pl.semaphore_signal(barrier, inc=1, device_id={"ctx": partner}, device_id_type=MESH)

    @pl.when(odd)
    def _():
        for t in range(1, chips):
            for d in range(2):
                pl.semaphore_signal(barrier, inc=1, device_id={"ctx": 2 * chip_at(t) + d}, device_id_type=MESH)

    get_pos.wait()
    get_x.wait()
    get_wkr.wait()
    pos_row = pos_v[...].astype(jnp.float32)

    def pos_of(count, index):
        spot = iota((count, rows), 1) == index(iota((count, rows), 0))
        return jnp.sum(jnp.where(spot, jnp.broadcast_to(pos_row, (count, rows)), 0.0), axis=1, keepdims=True)

    lane = iota((rows, LANES), 1)
    freq_id = lax.rem(lane[:1], half_rope)
    inv_freq = jnp.zeros((1, LANES), jnp.float32)
    for f in range(half_rope):
        inv_freq = jnp.where(freq_id == f, float(np.float32(10000.0 ** (-2.0 * f / rope))), inv_freq)
    angles = pos_of(rows, lambda r: r) * inv_freq
    first = lax.rem(lane, rope) < half_rope
    cos_tab = jnp.cos(angles)
    sin_tab = jnp.sin(angles)
    sin_tab = jnp.where(first, -sin_tab, sin_tab)

    def rope_lanes(a):
        other = jnp.where(first, pltpu.roll(a, LANES - half_rope, 1), pltpu.roll(a, half_rope, 1))
        return (a * cos_tab + other * sin_tab).astype(jnp.bfloat16)

    count = 2 * rows
    q_pos = pos_of(count, lambda r: lax.rem(r, half) + jnp.where(r >= rows, half, 0)).astype(jnp.int32)
    q_row = iota((count, 1), 0)
    q_seq = jnp.where(q_row < rows, half * me, half * (2 * n - 1 - me)) + lax.rem(q_row, half)
    q_first = q_seq - q_pos
    col = iota((1, keys), 1)
    slot = col // rows
    swapped = slot + 1 - 2 * lax.rem(slot, 2)
    inner = lax.rem(col, rows)

    def key_seq(slot, late):
        dev = 2 * chip_at(slot) + inner // half
        return half * jnp.where(late, 2 * n - 1 - dev, dev) + lax.rem(inner, half)

    def visible(seq, lo, hi):
        return jnp.where((seq >= lo) & (seq <= hi), 0.0, MASKED)

    bias_v[:count] = visible(key_seq(slot, False), q_first, q_seq)
    bias_v[count:] = visible(key_seq(swapped, True), q_first[rows:], q_seq[rows:])

    kr = mm(x_v[...], wkr_v[...], NT)
    for get in get_wdkv:
        get.wait()
    for i in range(2):
        at = slice(i * width // 2, (i + 1) * width // 2)
        kv_v[i] = mm(x_v[:, at], wdkv_v[at])
    turn = lax.rem(me, 2)
    kv = kv_v[turn] + kv_v[1 - turn]
    get_gkv.wait()
    c_kv = rms_norm(kv, gkv_v[...].astype(jnp.float32).reshape(1, -1))
    lat[me, :rows, :] = c_kv
    kr = rope_lanes(jnp.concatenate([kr] * (LANES // rope), axis=1))
    packed = jnp.zeros((PACK_ROWS, LANES), jnp.float32)
    kr = kr.astype(jnp.float32)
    part = iota((PACK_ROWS, LANES), 1) // rope
    for s in range(rows // PACK_ROWS):
        packed = jnp.where(part == s, kr[s * PACK_ROWS:(s + 1) * PACK_ROWS], packed)
    for i in range(PACKS):
        lat[me, rows:, i * LANES:(i + 1) * LANES] = packed[i * pack_rows:(i + 1) * pack_rows].astype(jnp.bfloat16)

    pl.semaphore_wait(barrier, chips)

    def push(block, peer, index):
        return pltpu.make_async_remote_copy(src_ref=lat.at[block], dst_ref=lat.at[block], send_sem=send_sem.at[index],
                                            recv_sem=recv_sem.at[block], device_id={"ctx": peer}, device_id_type=MESH)

    sends = [push(me, 2 * chip_at(t) + 1, t) for t in range(1, chips)] + [push(me, partner, 0)]
    start(*sends)

    def forward(t):
        return [push(2 * chip_at(t) + d, partner, chips + 2 * (t - 1) + d) for d in range(2)]

    def relay(t):
        for d, cp in enumerate(forward(t)):
            push(2 * chip_at(t) + d, me, 0).wait_recv()
            cp.start()

    get_gq.wait()
    get_wdq.wait()
    cq_v[...] = rms_norm(mm(x_v[...], wdq_v[...]), gq_v[...].astype(jnp.float32).reshape(1, -1))
    low = lane < nope
    zero = jnp.zeros((rows, LANES), jnp.bfloat16)

    def put_query(head, cols, t):
        at = head % 2 * half
        qcat[head // 2, at:at + half, cols] = t[:half]
        qcat[head // 2, rows + at:rows + at + half, cols] = t[half:]

    get_wuq.wait()
    for c in range(pairs // 4):
        q = mm(cq_v[...], wuq_v[:, c * 4 * LANES:(c + 1) * 4 * LANES]).astype(jnp.bfloat16)
        for i in range(4):
            t = q[:, i * LANES:(i + 1) * LANES]
            put_query(2 * (c * 4 + i), slice(0, LANES), jnp.where(low, t, zero))
            put_query(2 * (c * 4 + i) + 1, slice(0, LANES), jnp.where(low, zero, t))
    get_wqr.wait()
    per = LANES // rope
    for c in range(pairs // per):
        q = mm(cq_v[...], wqr_v[:, c * 2 * LANES:(c + 1) * 2 * LANES])
        for i in range(2):
            t = rope_lanes(q[:, i * LANES:(i + 1) * LANES])
            for s in range(per):
                put_query((c * 2 + i) * per + s, slice(LANES, LANES + rope), t[:, s * rope:(s + 1) * rope])

    same = iota((rope, LANES), 0) == lax.rem(iota((rope, LANES), 1), rope)
    same = jnp.where(same, 1.0, 0.0).astype(jnp.bfloat16)

    def up_project(slots):
        pieces, packs = [], []
        groups = half // PACK_ROWS
        for t in slots:
            chip = chip_at(t)
            block = lat[pl.ds(2 * chip, 2), :rows]
            tails = [lat[2 * chip + d, rows:].astype(jnp.float32) for d in range(2)]
            tails = [jnp.concatenate([a[:, i * LANES:(i + 1) * LANES] for i in range(PACKS)], axis=0) for a in tails]
            for p in [t % 2, 1 - t % 2]:
                pieces.append(block[:, p * half:(p + 1) * half].reshape(rows, kv_rank))
                packs += [jnp.where(part == p * groups + s, tails[d], 0.0).astype(jnp.bfloat16) for d in range(2) for s in range(groups)]
        c_all = jnp.concatenate(pieces, axis=0)
        krt = mm(same, jnp.concatenate(packs, axis=0), NT).astype(jnp.bfloat16)
        spots = [((t + i) % 2, (t - t % 2 + i) * rows, (2 * j + i) * rows) for j, t in enumerate(slots) for i in range(2)]
        for p, at, src in spots:
            krt_v[p, :, at:at + rows] = krt[:, src:src + rows]
        for c in range(pairs // 2):
            cols = slice(c * 2 * LANES, (c + 1) * 2 * LANES)
            k = mm(c_all, wuk_v[:, cols]).astype(jnp.bfloat16)
            for i in range(2):
                kt = k[:, i * LANES:(i + 1) * LANES].T
                for p, at, src in spots:
                    kt_v[2 * c + i, p, :, at:at + rows] = kt[:, src:src + rows]
        for c in range(pairs // 2):
            cols = slice(c * 2 * LANES, (c + 1) * 2 * LANES)
            v = mm(c_all, wuv_v[:, cols]).astype(jnp.bfloat16)
            for i in range(2):
                for p, at, src in spots:
                    v_v[2 * c + i, p, at:at + rows] = v[src:src + rows, i * LANES:(i + 1) * LANES]

    get_wuk.wait()
    get_wuv.wait()
    factor = (nope + rope) ** -0.5 * math.log2(math.e)

    def scores(g, part):
        for i in range(GROUP):
            p = g * GROUP + i
            top = rows if part == "second" else 0
            early = jnp.concatenate([kt_v[p, 0], krt_v[0]], axis=0)
            late = jnp.concatenate([kt_v[p, 1], krt_v[1]], axis=0)
            s_v[g % 2, i, top:count] = mm(qcat[p, top:], early) * factor + bias_v[top:count]
            s_v[g % 2, i, count:] = mm(qcat[p, rows:], late) * factor + bias_v[count:]

    def halves(a, op):
        return op(a[:, :LANES], a[:, LANES:])

    def weights(g, part):
        for i in range(GROUP):
            if part != "second":
                a = s_v[g % 2, i, :rows]
                m_a = jnp.max(halves(a, jnp.maximum), axis=1, keepdims=True)
                a = jnp.exp2(a - m_a)
                p_v[g % 2, i, :rows] = a.astype(jnp.bfloat16)
                l_a = jnp.sum(halves(a, jnp.add), axis=1, keepdims=True)
                l_v[g % 2, i, :rows] = jnp.broadcast_to(1.0 / l_a, (rows, LANES))
            b, c = s_v[g % 2, i, rows:count], s_v[g % 2, i, count:]
            m_b = jnp.max(jnp.maximum(halves(b, jnp.maximum), halves(c, jnp.maximum)), axis=1, keepdims=True)
            b, c = jnp.exp2(b - m_b), jnp.exp2(c - m_b)
            p_v[g % 2, i, rows:count] = b.astype(jnp.bfloat16)
            p_v[g % 2, i, count:] = c.astype(jnp.bfloat16)
            l_b = jnp.sum(halves(b, jnp.add) + halves(c, jnp.add), axis=1, keepdims=True)
            l_v[g % 2, i, rows:] = jnp.broadcast_to(1.0 / l_b, (rows, LANES))

    def values(g, part):
        for i in range(GROUP):
            cols = slice((g * GROUP + i) * LANES, (g * GROUP + i + 1) * LANES)
            o = mm(p_v[g % 2, i, rows if part == "second" else 0:count], v_v[g * GROUP + i, 0])
            o_b = (o[-rows:] + mm(p_v[g % 2, i, count:], v_v[g * GROUP + i, 1])) * l_v[g % 2, i, rows:]
            o_v[half:, cols] = jnp.where(low[:half], o_b[:half], o_b[half:]).astype(jnp.bfloat16)
            if part != "second":
                o_a = o[:rows] * l_v[g % 2, i, :rows]
                o_v[:half, cols] = jnp.where(low[:half], o_a[:half], o_a[half:]).astype(jnp.bfloat16)

    def project(g):
        for c in range(width // panel):
            cols = slice(c * panel, (c + 1) * panel)
            y = mm(o_v[:, g * deep:(g + 1) * deep], wout_v[g * deep:(g + 1) * deep, cols])
            if g > 0:
                y += y_sum[:, cols]
            if g + 1 < steps:
                y_sum[:, cols] = y
            else:
                y_v[:, cols] = y.astype(jnp.bfloat16)

    def first_queries():
        for p in range(pairs):
            own = jnp.concatenate([kt_v[p, 0, :, :LANES], krt_v[0, :, :LANES]], axis=0)
            fs_v[p] = mm(qcat[p, :rows], own) * factor + bias_v[:rows, :LANES]
        for p in range(pairs):
            a = fs_v[p]
            a = jnp.exp2(a - jnp.max(a, axis=1, keepdims=True))
            fp_v[p] = a.astype(jnp.bfloat16)
            fl_v[p] = jnp.broadcast_to(1.0 / jnp.sum(a, axis=1, keepdims=True), (rows, LANES))
        for p in range(pairs):
            o = mm(fp_v[p], v_v[p, 0, :LANES]) * fl_v[p]
            o_v[:half, p * LANES:(p + 1) * LANES] = jnp.where(low[:half], o[:half], o[half:]).astype(jnp.bfloat16)

    def receive(t):
        for d in range(2):
            push(2 * chip_at(t) + d, me, 0).wait_recv()

    even = jnp.logical_not(odd)
    push(partner, me, 0).wait_recv()
    pl.when(odd)(lambda: relay(1))
    pl.when(even)(lambda: receive(1))
    up_project([0, 1])
    pl.when(my_chip == 0)(first_queries)

    @pl.when(odd)
    def _():
        for t in range(2, chips):
            relay(t)

    for t in range(2, chips):
        pl.when(even)(functools.partial(receive, t))
        up_project([t])

    def finish(part):
        for g in range(steps + 3):
            if g == 3:
                for get in get_wout:
                    get.wait()
            if g >= 3:
                project(g - 3)
            if 2 <= g < steps + 2:
                values(g - 2, part)
            if 1 <= g <= steps:
                weights(g - 1, part)
            if g < steps:
                scores(g, part)

    pl.when(my_chip == 0)(functools.partial(finish, "second"))
    pl.when(my_chip > 0)(functools.partial(finish, "both"))
    for cp in sends:
        cp.wait_send()

    @pl.when(odd)
    def _():
        for t in range(1, chips):
            for cp in forward(t):
                cp.wait_send()


def solution(mesh):
    n = mesh.shape["ctx"]
    row_spec = P(("dp", "ctx"), None)
    id_spec = P(("dp", "ctx"))

    def per_device(x, pos, seg, w_dq, w_uq, w_qr, w_dkv, w_kr, w_uk, w_uv, w_out, gain_q, gain_kv):
        rows, width = x.shape
        pairs = w_uq.shape[1] // LANES
        keys = n * rows
        kv_rank = w_dkv.shape[1]
        rope = w_kr.shape[1]
        bf, f32 = jnp.bfloat16, jnp.float32
        args = (x, pos.reshape(1, rows), w_dq, w_uq, w_qr, w_dkv, w_kr.T, w_uk, w_uv, w_out,
                gain_q, gain_kv)
        scratch = [pltpu.VMEM(a.shape, a.dtype) for a in args]
        scratch += [
            pltpu.VMEM((n, rows + PACK_ROWS // PACKS, kv_rank), bf),
            pltpu.VMEM((2, rows, kv_rank), f32),
            pltpu.VMEM((rows, w_dq.shape[1]), bf),
            pltpu.VMEM((pairs, 2 * rows, LANES + rope), bf),
            pltpu.VMEM((pairs, 2, LANES, keys // 2), bf),
            pltpu.VMEM((2, rope, keys // 2), bf),
            pltpu.VMEM((pairs, 2, keys // 2, LANES), bf),
            pltpu.VMEM((3 * rows, keys // 2), f32),
            pltpu.VMEM((rows, w_uv.shape[1]), bf),
            pltpu.VMEM((2, GROUP, 3 * rows, keys // 2), f32),
            pltpu.VMEM((2, GROUP, 3 * rows, keys // 2), bf),
            pltpu.VMEM((2, GROUP, 2 * rows, LANES), f32),
            pltpu.VMEM((rows, width), f32),
            pltpu.VMEM((pairs, rows, LANES), f32),
            pltpu.VMEM((pairs, rows, LANES), bf),
            pltpu.VMEM((pairs, rows, LANES), f32),
            pltpu.SemaphoreType.DMA((len(args) - 2 + len(KV_CUTS) - 1 + pairs // GROUP,)),
            pltpu.SemaphoreType.DMA((n // 2 + n - 2,)),
            pltpu.SemaphoreType.DMA((n,)),
        ]
        return pl.pallas_call(
            functools.partial(layer_kernel, n),
            out_shape=pltpu.VMEM(x.shape, bf),
            in_specs=[pl.BlockSpec(memory_space=pltpu.HBM)] * len(args),
            out_specs=pl.BlockSpec(memory_space=pltpu.VMEM),
            scratch_shapes=scratch,
            compiler_params=pltpu.CompilerParams(collective_id=0, has_side_effects=True, vmem_limit_bytes=62000000),
        )(*args)

    return jax.shard_map(per_device, mesh=mesh, in_specs=(row_spec, id_spec, id_spec) + (P(),) * 10, out_specs=row_spec, check_vma=False)
```

```python
import functools
import math

import jax
import jax.numpy as jnp
import numpy as np
from jax import lax
from jax.experimental import pallas as pl
from jax.experimental.pallas import tpu as pltpu
from jax.sharding import PartitionSpec as P

NORM_EPS = 1e-6
MASKED = -1e30
LANES = 128
PACK_ROWS = 16
PACKS = 2
GROUP = 4
KV_CUTS = (0, 2, 4, 6, 8, 10)
MESH = pl.DeviceIdType.MESH
NT = (((1,), (1,)), ((), ()))


def mm(a, b, dims=(((1,), (0,)), ((), ()))):
    return lax.dot_general(a, b, dims, preferred_element_type=jnp.float32)


def rms_norm(vals, gain):
    mean_sq = jnp.mean(vals * vals, axis=-1, keepdims=True)
    return (vals * lax.rsqrt(mean_sq + NORM_EPS) * gain).astype(jnp.bfloat16)


def iota(shape, dim):
    return lax.broadcasted_iota(jnp.int32, shape, dim)


def layer_kernel(n, x_h, pos_h, wdq_h, wuq_h, wqr_h, wdkv_h, wkr_h, wuk_h, wuv_h, wout_h, gq_h, gkv_h, y_v,
                 x_v, pos_v, wdq_v, wuq_v, wqr_v, wdkv_v, wkr_v, wuk_v, wuv_v, wout_v, gq_v, gkv_v,
                 lat, kv_v, cq_v, qcat, kt_v, krt_v, v_v, bias_v, o_v, s_v, p_v, l_v, y_sum, fs_v, fp_v, fl_v, in_sem, send_sem, recv_sem):
    rows, width = x_v.shape
    kv_rank = wdkv_v.shape[1]
    rope = wkr_v.shape[0]
    half_rope = rope // 2
    pairs = kt_v.shape[0]
    nope = LANES // 2
    half = rows // 2
    chips = n // 2
    keys = chips * rows
    pack_rows = PACK_ROWS // PACKS
    steps = pairs // GROUP
    deep = GROUP * LANES
    panel = 2 * LANES

    me = lax.axis_index("ctx")
    my_chip = me // 2
    partner = me + 1 - 2 * lax.rem(me, 2)
    odd = lax.rem(me, 2) == 1

    def chip_at(slot):
        return jnp.where(slot == 0, my_chip, jnp.where(slot > my_chip, slot, slot - 1))


    fetches = []

    def fetch(src, dst):
        fetches.append(pltpu.make_async_copy(src, dst, in_sem.at[len(fetches)]))
        return fetches[-1]

    def start(*copies):
        for cp in copies:
            cp.start()

    get_pos = fetch(pos_h, pos_v)
    get_x = fetch(x_h, x_v)
    get_wkr = fetch(wkr_h, wkr_v)
    depth = 2 * LANES
    cuts = [width // depth * c // 10 * depth for c in KV_CUTS]
    get_wdkv = [fetch(wdkv_h.at[pl.ds(lo, hi - lo)], wdkv_v.at[pl.ds(lo, hi - lo)]) for lo, hi in zip(cuts, cuts[1:])]
    get_gkv = fetch(gkv_h, gkv_v)
    get_gq = fetch(gq_h, gq_v)
    get_wdq = fetch(wdq_h, wdq_v)
    get_wuq = fetch(wuq_h, wuq_v)
    get_wqr = fetch(wqr_h, wqr_v)
    get_wuk = fetch(wuk_h, wuk_v)
    get_wuv = fetch(wuv_h, wuv_v)
    get_wout = [fetch(wout_h.at[pl.ds(g * deep, deep)], wout_v.at[pl.ds(g * deep, deep)]) for g in range(steps)]
    start(get_pos, get_x, get_wkr, get_gkv, *get_wdkv, get_gq, get_wdq, get_wuq, get_wqr, get_wuk, get_wuv, *get_wout)

    barrier = pltpu.get_barrier_semaphore()
    pl.semaphore_signal(barrier, inc=1, device_id={"ctx": partner}, device_id_type=MESH)

    @pl.when(odd)
    def _():
        for t in range(1, chips):
            for d in range(2):
                pl.semaphore_signal(barrier, inc=1, device_id={"ctx": 2 * chip_at(t) + d}, device_id_type=MESH)

    get_pos.wait()
    get_x.wait()
    get_wkr.wait()
    pos_row = pos_v[...].astype(jnp.float32)

    def pos_of(count, index):
        spot = iota((count, rows), 1) == index(iota((count, rows), 0))
        return jnp.sum(jnp.where(spot, jnp.broadcast_to(pos_row, (count, rows)), 0.0), axis=1, keepdims=True)

    lane = iota((rows, LANES), 1)
    freq_id = lax.rem(lane[:1], half_rope)
    inv_freq = jnp.zeros((1, LANES), jnp.float32)
    for f in range(half_rope):
        inv_freq = jnp.where(freq_id == f, float(np.float32(10000.0 ** (-2.0 * f / rope))), inv_freq)
    angles = pos_of(rows, lambda r: r) * inv_freq
    first = lax.rem(lane, rope) < half_rope
    cos_tab = jnp.cos(angles)
    sin_tab = jnp.sin(angles)
    sin_tab = jnp.where(first, -sin_tab, sin_tab)

    def rope_lanes(a):
        other = jnp.where(first, pltpu.roll(a, LANES - half_rope, 1), pltpu.roll(a, half_rope, 1))
        return (a * cos_tab + other * sin_tab).astype(jnp.bfloat16)

    count = 2 * rows
    q_pos = pos_of(count, lambda r: lax.rem(r, half) + jnp.where(r >= rows, half, 0)).astype(jnp.int32)
    q_row = iota((count, 1), 0)
    q_seq = jnp.where(q_row < rows, half * me, half * (2 * n - 1 - me)) + lax.rem(q_row, half)
    q_first = q_seq - q_pos
    col = iota((1, keys), 1)
    slot = col // rows
    swapped = slot + 1 - 2 * lax.rem(slot, 2)
    inner = lax.rem(col, rows)

    def key_seq(slot, late):
        dev = 2 * chip_at(slot) + inner // half
        return half * jnp.where(late, 2 * n - 1 - dev, dev) + lax.rem(inner, half)

    def visible(seq, lo, hi):
        return jnp.where((seq >= lo) & (seq <= hi), 0.0, MASKED)

    bias_v[:count] = visible(key_seq(slot, False), q_first, q_seq)
    bias_v[count:] = visible(key_seq(swapped, True), q_first[rows:], q_seq[rows:])

    kr = mm(x_v[...], wkr_v[...], NT)
    for get in get_wdkv:
        get.wait()
    for i in range(2):
        at = slice(i * width // 2, (i + 1) * width // 2)
        kv_v[i] = mm(x_v[:, at], wdkv_v[at])
    turn = lax.rem(me, 2)
    kv = kv_v[turn] + kv_v[1 - turn]
    get_gkv.wait()
    c_kv = rms_norm(kv, gkv_v[...].astype(jnp.float32).reshape(1, -1))
    lat[me, :rows, :] = c_kv
    kr = rope_lanes(jnp.concatenate([kr] * (LANES // rope), axis=1))
    packed = jnp.zeros((PACK_ROWS, LANES), jnp.float32)
    kr = kr.astype(jnp.float32)
    part = iota((PACK_ROWS, LANES), 1) // rope
    for s in range(rows // PACK_ROWS):
        packed = jnp.where(part == s, kr[s * PACK_ROWS:(s + 1) * PACK_ROWS], packed)
    for i in range(PACKS):
        lat[me, rows:, i * LANES:(i + 1) * LANES] = packed[i * pack_rows:(i + 1) * pack_rows].astype(jnp.bfloat16)

    pl.semaphore_wait(barrier, chips)

    def push(block, peer, index):
        return pltpu.make_async_remote_copy(src_ref=lat.at[block], dst_ref=lat.at[block], send_sem=send_sem.at[index],
                                            recv_sem=recv_sem.at[block], device_id={"ctx": peer}, device_id_type=MESH)

    sends = [push(me, 2 * chip_at(t) + 1, t) for t in range(1, chips)] + [push(me, partner, 0)]
    start(*sends)

    def forward(t):
        return [push(2 * chip_at(t) + d, partner, chips + 2 * (t - 1) + d) for d in range(2)]

    def relay(t):
        for d, cp in enumerate(forward(t)):
            push(2 * chip_at(t) + d, me, 0).wait_recv()
            cp.start()

    get_gq.wait()
    get_wdq.wait()
    cq_v[...] = rms_norm(mm(x_v[...], wdq_v[...]), gq_v[...].astype(jnp.float32).reshape(1, -1))
    low = lane < nope
    zero = jnp.zeros((rows, LANES), jnp.bfloat16)

    def put_query(head, cols, t):
        at = head % 2 * half
        qcat[head // 2, at:at + half, cols] = t[:half]
        qcat[head // 2, rows + at:rows + at + half, cols] = t[half:]

    get_wuq.wait()
    for c in range(pairs // 4):
        q = mm(cq_v[...], wuq_v[:, c * 4 * LANES:(c + 1) * 4 * LANES]).astype(jnp.bfloat16)
        for i in range(4):
            t = q[:, i * LANES:(i + 1) * LANES]
            put_query(2 * (c * 4 + i), slice(0, LANES), jnp.where(low, t, zero))
            put_query(2 * (c * 4 + i) + 1, slice(0, LANES), jnp.where(low, zero, t))
    get_wqr.wait()
    per = LANES // rope
    for c in range(pairs // per):
        q = mm(cq_v[...], wqr_v[:, c * 2 * LANES:(c + 1) * 2 * LANES])
        for i in range(2):
            t = rope_lanes(q[:, i * LANES:(i + 1) * LANES])
            for s in range(per):
                put_query((c * 2 + i) * per + s, slice(LANES, 2 * LANES), jnp.where(lane // rope == s, t, zero))

    same = lax.rem(iota((LANES, LANES), 0), rope) == lax.rem(iota((LANES, LANES), 1), rope)
    same = jnp.where(same, 1.0, 0.0).astype(jnp.bfloat16)

    def up_project(slots):
        pieces, packs = [], []
        groups = half // PACK_ROWS
        for t in slots:
            chip = chip_at(t)
            block = lat[pl.ds(2 * chip, 2), :rows]
            tails = [lat[2 * chip + d, rows:].astype(jnp.float32) for d in range(2)]
            tails = [jnp.concatenate([a[:, i * LANES:(i + 1) * LANES] for i in range(PACKS)], axis=0) for a in tails]
            for p in [t % 2, 1 - t % 2]:
                pieces.append(block[:, p * half:(p + 1) * half].reshape(rows, kv_rank))
                packs += [jnp.where(part == p * groups + s, tails[d], 0.0).astype(jnp.bfloat16) for d in range(2) for s in range(groups)]
        c_all = jnp.concatenate(pieces, axis=0)
        krt = mm(same, jnp.concatenate(packs, axis=0), NT).astype(jnp.bfloat16)
        spots = [((t + i) % 2, (t - t % 2 + i) * rows, (2 * j + i) * rows) for j, t in enumerate(slots) for i in range(2)]
        for p, at, src in spots:
            krt_v[p, :, at:at + rows] = krt[:, src:src + rows]
        for c in range(pairs // 2):
            cols = slice(c * 2 * LANES, (c + 1) * 2 * LANES)
            k = mm(c_all, wuk_v[:, cols]).astype(jnp.bfloat16)
            for i in range(2):
                kt = k[:, i * LANES:(i + 1) * LANES].T
                for p, at, src in spots:
                    kt_v[2 * c + i, p, :, at:at + rows] = kt[:, src:src + rows]
        for c in range(pairs // 2):
            cols = slice(c * 2 * LANES, (c + 1) * 2 * LANES)
            v = mm(c_all, wuv_v[:, cols]).astype(jnp.bfloat16)
            for i in range(2):
                for p, at, src in spots:
                    v_v[2 * c + i, p, at:at + rows] = v[src:src + rows, i * LANES:(i + 1) * LANES]

    get_wuk.wait()
    get_wuv.wait()
    factor = (nope + rope) ** -0.5 * math.log2(math.e)

    def scores(g, part):
        for i in range(GROUP):
            p = g * GROUP + i
            top = rows if part == "second" else 0
            early = jnp.concatenate([kt_v[p, 0], krt_v[0]], axis=0)
            late = jnp.concatenate([kt_v[p, 1], krt_v[1]], axis=0)
            s_v[g % 2, i, top:count] = mm(qcat[p, top:], early) * factor + bias_v[top:count]
            s_v[g % 2, i, count:] = mm(qcat[p, rows:], late) * factor + bias_v[count:]

    def halves(a, op):
        return op(a[:, :LANES], a[:, LANES:])

    def weights(g, part):
        for i in range(GROUP):
            if part != "second":
                a = s_v[g % 2, i, :rows]
                m_a = jnp.max(halves(a, jnp.maximum), axis=1, keepdims=True)
                a = jnp.exp2(a - m_a)
                p_v[g % 2, i, :rows] = a.astype(jnp.bfloat16)
                l_a = jnp.sum(halves(a, jnp.add), axis=1, keepdims=True)
                l_v[g % 2, i, :rows] = jnp.broadcast_to(1.0 / l_a, (rows, LANES))
            b, c = s_v[g % 2, i, rows:count], s_v[g % 2, i, count:]
            m_b = jnp.max(jnp.maximum(halves(b, jnp.maximum), halves(c, jnp.maximum)), axis=1, keepdims=True)
            b, c = jnp.exp2(b - m_b), jnp.exp2(c - m_b)
            p_v[g % 2, i, rows:count] = b.astype(jnp.bfloat16)
            p_v[g % 2, i, count:] = c.astype(jnp.bfloat16)
            l_b = jnp.sum(halves(b, jnp.add) + halves(c, jnp.add), axis=1, keepdims=True)
            l_v[g % 2, i, rows:] = jnp.broadcast_to(1.0 / l_b, (rows, LANES))

    def values(g, part):
        for i in range(GROUP):
            cols = slice((g * GROUP + i) * LANES, (g * GROUP + i + 1) * LANES)
            o = mm(p_v[g % 2, i, rows if part == "second" else 0:count], v_v[g * GROUP + i, 0])
            o_b = (o[-rows:] + mm(p_v[g % 2, i, count:], v_v[g * GROUP + i, 1])) * l_v[g % 2, i, rows:]
            o_v[half:, cols] = jnp.where(low[:half], o_b[:half], o_b[half:]).astype(jnp.bfloat16)
            if part != "second":
                o_a = o[:rows] * l_v[g % 2, i, :rows]
                o_v[:half, cols] = jnp.where(low[:half], o_a[:half], o_a[half:]).astype(jnp.bfloat16)

    def project(g):
        for c in range(width // panel):
            cols = slice(c * panel, (c + 1) * panel)
            y = mm(o_v[:, g * deep:(g + 1) * deep], wout_v[g * deep:(g + 1) * deep, cols])
            if g > 0:
                y += y_sum[:, cols]
            if g + 1 < steps:
                y_sum[:, cols] = y
            else:
                y_v[:, cols] = y.astype(jnp.bfloat16)

    def first_queries():
        for p in range(pairs):
            own = jnp.concatenate([kt_v[p, 0, :, :LANES], krt_v[0, :, :LANES]], axis=0)
            fs_v[p] = mm(qcat[p, :rows], own) * factor + bias_v[:rows, :LANES]
        for p in range(pairs):
            a = fs_v[p]
            a = jnp.exp2(a - jnp.max(a, axis=1, keepdims=True))
            fp_v[p] = a.astype(jnp.bfloat16)
            fl_v[p] = jnp.broadcast_to(1.0 / jnp.sum(a, axis=1, keepdims=True), (rows, LANES))
        for p in range(pairs):
            o = mm(fp_v[p], v_v[p, 0, :LANES]) * fl_v[p]
            o_v[:half, p * LANES:(p + 1) * LANES] = jnp.where(low[:half], o[:half], o[half:]).astype(jnp.bfloat16)

    def receive(t):
        for d in range(2):
            push(2 * chip_at(t) + d, me, 0).wait_recv()

    even = jnp.logical_not(odd)
    push(partner, me, 0).wait_recv()
    pl.when(odd)(lambda: relay(1))
    pl.when(even)(lambda: receive(1))
    up_project([0, 1])
    pl.when(my_chip == 0)(first_queries)

    @pl.when(odd)
    def _():
        for t in range(2, chips):
            relay(t)

    for t in range(2, chips):
        pl.when(even)(functools.partial(receive, t))
        up_project([t])

    def finish(part):
        for g in range(steps + 3):
            if g == 3:
                for get in get_wout:
                    get.wait()
            if g >= 3:
                project(g - 3)
            if 2 <= g < steps + 2:
                values(g - 2, part)
            if 1 <= g <= steps:
                weights(g - 1, part)
            if g < steps:
                scores(g, part)

    pl.when(my_chip == 0)(functools.partial(finish, "second"))
    pl.when(my_chip > 0)(functools.partial(finish, "both"))
    for cp in sends:
        cp.wait_send()

    @pl.when(odd)
    def _():
        for t in range(1, chips):
            for cp in forward(t):
                cp.wait_send()


def solution(mesh):
    n = mesh.shape["ctx"]
    row_spec = P(("dp", "ctx"), None)
    id_spec = P(("dp", "ctx"))

    def per_device(x, pos, seg, w_dq, w_uq, w_qr, w_dkv, w_kr, w_uk, w_uv, w_out, gain_q, gain_kv):
        rows, width = x.shape
        pairs = w_uq.shape[1] // LANES
        keys = n * rows
        kv_rank = w_dkv.shape[1]
        bf, f32 = jnp.bfloat16, jnp.float32
        args = (x, pos.reshape(1, rows), w_dq, w_uq, w_qr, w_dkv, w_kr.T, w_uk, w_uv, w_out,
                gain_q, gain_kv)
        scratch = [pltpu.VMEM(a.shape, a.dtype) for a in args]
        scratch += [
            pltpu.VMEM((n, rows + PACK_ROWS // PACKS, kv_rank), bf),
            pltpu.VMEM((2, rows, kv_rank), f32),
            pltpu.VMEM((rows, w_dq.shape[1]), bf),
            pltpu.VMEM((pairs, 2 * rows, 2 * LANES), bf),
            pltpu.VMEM((pairs, 2, LANES, keys // 2), bf),
            pltpu.VMEM((2, LANES, keys // 2), bf),
            pltpu.VMEM((pairs, 2, keys // 2, LANES), bf),
            pltpu.VMEM((3 * rows, keys // 2), f32),
            pltpu.VMEM((rows, w_uv.shape[1]), bf),
            pltpu.VMEM((2, GROUP, 3 * rows, keys // 2), f32),
            pltpu.VMEM((2, GROUP, 3 * rows, keys // 2), bf),
            pltpu.VMEM((2, GROUP, 2 * rows, LANES), f32),
            pltpu.VMEM((rows, width), f32),
            pltpu.VMEM((pairs, rows, LANES), f32),
            pltpu.VMEM((pairs, rows, LANES), bf),
            pltpu.VMEM((pairs, rows, LANES), f32),
            pltpu.SemaphoreType.DMA((len(args) - 2 + len(KV_CUTS) - 1 + pairs // GROUP,)),
            pltpu.SemaphoreType.DMA((n // 2 + n - 2,)),
            pltpu.SemaphoreType.DMA((n,)),
        ]
        return pl.pallas_call(
            functools.partial(layer_kernel, n),
            out_shape=pltpu.VMEM(x.shape, bf),
            in_specs=[pl.BlockSpec(memory_space=pltpu.HBM)] * len(args),
            out_specs=pl.BlockSpec(memory_space=pltpu.VMEM),
            scratch_shapes=scratch,
            compiler_params=pltpu.CompilerParams(collective_id=0, has_side_effects=True, vmem_limit_bytes=62000000),
        )(*args)

    return jax.shard_map(per_device, mesh=mesh, in_specs=(row_spec, id_spec, id_spec) + (P(),) * 10, out_specs=row_spec, check_vma=False)
```

```python
import functools
import math

import jax
import jax.numpy as jnp
import numpy as np
from jax import lax
from jax.experimental import pallas as pl
from jax.experimental.pallas import tpu as pltpu
from jax.sharding import PartitionSpec as P

NORM_EPS = 1e-6
MASKED = -1e30
LANES = 128
PACK_ROWS = 16
PACKS = 2
GROUP = 4
KV_CUTS = (0, 2, 4, 6, 8, 10)
MESH = pl.DeviceIdType.MESH
NT = (((1,), (1,)), ((), ()))


def mm(a, b, dims=(((1,), (0,)), ((), ()))):
    return lax.dot_general(a, b, dims, preferred_element_type=jnp.float32)


def rms_norm(vals, gain):
    mean_sq = jnp.mean(vals * vals, axis=-1, keepdims=True)
    return (vals * lax.rsqrt(mean_sq + NORM_EPS) * gain).astype(jnp.bfloat16)


def iota(shape, dim):
    return lax.broadcasted_iota(jnp.int32, shape, dim)


def layer_kernel(n, x_h, pos_h, wdq_h, wuq_h, wqr_h, wdkv_h, wkr_h, wuk_h, wuv_h, wout_h, gq_h, gkv_h, y_v,
                 x_v, pos_v, wdq_v, wuq_v, wqr_v, wdkv_v, wkr_v, wuk_v, wuv_v, wout_v, gq_v, gkv_v,
                 lat, kv_v, cq_v, qcat, kt_v, krt_v, v_v, bias_v, o_v, s_v, p_v, l_v, y_sum, fs_v, fp_v, fl_v, in_sem, send_sem, recv_sem):
    rows, width = x_v.shape
    kv_rank = wdkv_v.shape[1]
    rope = wkr_v.shape[0]
    half_rope = rope // 2
    pairs = kt_v.shape[0]
    nope = LANES // 2
    half = rows // 2
    chips = n // 2
    keys = chips * rows
    pack_rows = PACK_ROWS // PACKS
    steps = pairs // GROUP
    deep = GROUP * LANES
    panel = 2 * LANES

    me = lax.axis_index("ctx")
    my_chip = me // 2
    partner = me + 1 - 2 * lax.rem(me, 2)
    odd = lax.rem(me, 2) == 1

    def chip_at(slot):
        return jnp.where(slot == 0, my_chip, jnp.where(slot > my_chip, slot, slot - 1))


    fetches = []

    def fetch(src, dst):
        fetches.append(pltpu.make_async_copy(src, dst, in_sem.at[len(fetches)]))
        return fetches[-1]

    def start(*copies):
        for cp in copies:
            cp.start()

    get_pos = fetch(pos_h, pos_v)
    get_x = fetch(x_h, x_v)
    get_wkr = fetch(wkr_h, wkr_v)
    depth = 2 * LANES
    cuts = [width // depth * c // 10 * depth for c in KV_CUTS]
    get_wdkv = [fetch(wdkv_h.at[pl.ds(lo, hi - lo)], wdkv_v.at[pl.ds(lo, hi - lo)]) for lo, hi in zip(cuts, cuts[1:])]
    get_gkv = fetch(gkv_h, gkv_v)
    get_gq = fetch(gq_h, gq_v)
    get_wdq = fetch(wdq_h, wdq_v)
    get_wuq = fetch(wuq_h, wuq_v)
    get_wqr = fetch(wqr_h, wqr_v)
    get_wuk = fetch(wuk_h, wuk_v)
    get_wuv = fetch(wuv_h, wuv_v)
    get_wout = [fetch(wout_h.at[pl.ds(g * deep, deep)], wout_v.at[pl.ds(g * deep, deep)]) for g in range(steps)]
    start(get_pos, get_x, get_wkr, get_gkv, *get_wdkv, get_gq, get_wdq, get_wuq, get_wqr, get_wuk, get_wuv, *get_wout)

    barrier = pltpu.get_barrier_semaphore()
    pl.semaphore_signal(barrier, inc=1, device_id={"ctx": partner}, device_id_type=MESH)

    @pl.when(odd)
    def _():
        for t in range(1, chips):
            for d in range(2):
                pl.semaphore_signal(barrier, inc=1, device_id={"ctx": 2 * chip_at(t) + d}, device_id_type=MESH)

    get_pos.wait()
    get_x.wait()
    get_wkr.wait()
    pos_row = pos_v[...].astype(jnp.float32)

    def pos_of(count, index):
        spot = iota((count, rows), 1) == index(iota((count, rows), 0))
        return jnp.sum(jnp.where(spot, jnp.broadcast_to(pos_row, (count, rows)), 0.0), axis=1, keepdims=True)

    lane = iota((rows, LANES), 1)
    freq_id = lax.rem(lane[:1], half_rope)
    inv_freq = jnp.zeros((1, LANES), jnp.float32)
    for f in range(half_rope):
        inv_freq = jnp.where(freq_id == f, float(np.float32(10000.0 ** (-2.0 * f / rope))), inv_freq)
    angles = pos_of(rows, lambda r: r) * inv_freq
    first = lax.rem(lane, rope) < half_rope
    cos_tab = jnp.cos(angles)
    sin_tab = jnp.sin(angles)
    sin_tab = jnp.where(first, -sin_tab, sin_tab)

    def rope_lanes(a):
        other = jnp.where(first, pltpu.roll(a, LANES - half_rope, 1), pltpu.roll(a, half_rope, 1))
        return (a * cos_tab + other * sin_tab).astype(jnp.bfloat16)

    count = 2 * rows
    q_pos = pos_of(count, lambda r: lax.rem(r, half) + jnp.where(r >= rows, half, 0)).astype(jnp.int32)
    q_row = iota((count, 1), 0)
    q_seq = jnp.where(q_row < rows, half * me, half * (2 * n - 1 - me)) + lax.rem(q_row, half)
    q_first = q_seq - q_pos
    col = iota((1, keys), 1)
    slot = col // rows
    swapped = slot + 1 - 2 * lax.rem(slot, 2)
    inner = lax.rem(col, rows)

    def key_seq(slot, late):
        dev = 2 * chip_at(slot) + inner // half
        return half * jnp.where(late, 2 * n - 1 - dev, dev) + lax.rem(inner, half)

    def visible(seq, lo, hi):
        return jnp.where((seq >= lo) & (seq <= hi), 0.0, MASKED)

    bias_v[:count] = visible(key_seq(slot, False), q_first, q_seq)
    bias_v[count:] = visible(key_seq(swapped, True), q_first[rows:], q_seq[rows:])

    kr = mm(x_v[...], wkr_v[...], NT)
    for get in get_wdkv:
        get.wait()
    for i in range(2):
        at = slice(i * width // 2, (i + 1) * width // 2)
        kv_v[i] = mm(x_v[:, at], wdkv_v[at])
    turn = lax.rem(me, 2)
    kv = kv_v[turn] + kv_v[1 - turn]
    get_gkv.wait()
    c_kv = rms_norm(kv, gkv_v[...].astype(jnp.float32).reshape(1, -1))
    lat[me, :rows, :] = c_kv
    kr = rope_lanes(jnp.concatenate([kr] * (LANES // rope), axis=1))
    packed = jnp.zeros((PACK_ROWS, LANES), jnp.float32)
    kr = kr.astype(jnp.float32)
    part = iota((PACK_ROWS, LANES), 1) // rope
    for s in range(rows // PACK_ROWS):
        packed = jnp.where(part == s, kr[s * PACK_ROWS:(s + 1) * PACK_ROWS], packed)
    for i in range(PACKS):
        lat[me, rows:, i * LANES:(i + 1) * LANES] = packed[i * pack_rows:(i + 1) * pack_rows].astype(jnp.bfloat16)

    pl.semaphore_wait(barrier, chips)

    def push(block, peer, index):
        return pltpu.make_async_remote_copy(src_ref=lat.at[block], dst_ref=lat.at[block], send_sem=send_sem.at[index],
                                            recv_sem=recv_sem.at[block], device_id={"ctx": peer}, device_id_type=MESH)

    sends = [push(me, 2 * chip_at(t) + 1, t) for t in range(1, chips)] + [push(me, partner, 0)]
    start(*sends)

    def forward(t):
        return [push(2 * chip_at(t) + d, partner, chips + 2 * (t - 1) + d) for d in range(2)]

    def relay(t):
        for d, cp in enumerate(forward(t)):
            push(2 * chip_at(t) + d, me, 0).wait_recv()
            cp.start()

    get_gq.wait()
    get_wdq.wait()
    cq_v[...] = rms_norm(mm(x_v[...], wdq_v[...]), gq_v[...].astype(jnp.float32).reshape(1, -1))
    low = lane < nope
    zero = jnp.zeros((rows, LANES), jnp.bfloat16)

    def put_query(head, cols, t):
        at = head % 2 * half
        qcat[head // 2, at:at + half, cols] = t[:half]
        qcat[head // 2, rows + at:rows + at + half, cols] = t[half:]

    get_wuq.wait()
    for c in range(pairs // 4):
        q = mm(cq_v[...], wuq_v[:, c * 4 * LANES:(c + 1) * 4 * LANES]).astype(jnp.bfloat16)
        for i in range(4):
            t = q[:, i * LANES:(i + 1) * LANES]
            put_query(2 * (c * 4 + i), slice(0, LANES), jnp.where(low, t, zero))
            put_query(2 * (c * 4 + i) + 1, slice(0, LANES), jnp.where(low, zero, t))
    get_wqr.wait()
    per = LANES // rope
    for c in range(pairs // per):
        q = mm(cq_v[...], wqr_v[:, c * 2 * LANES:(c + 1) * 2 * LANES])
        for i in range(2):
            t = rope_lanes(q[:, i * LANES:(i + 1) * LANES])
            for s in range(per):
                put_query((c * 2 + i) * per + s, slice(LANES, LANES + rope), t[:, s * rope:(s + 1) * rope])

    same = iota((rope, LANES), 0) == lax.rem(iota((rope, LANES), 1), rope)
    same = jnp.where(same, 1.0, 0.0).astype(jnp.bfloat16)

    def up_project(slots):
        pieces, packs = [], []
        groups = half // PACK_ROWS
        for t in slots:
            chip = chip_at(t)
            block = lat[pl.ds(2 * chip, 2), :rows]
            tails = [lat[2 * chip + d, rows:].astype(jnp.float32) for d in range(2)]
            tails = [jnp.concatenate([a[:, i * LANES:(i + 1) * LANES] for i in range(PACKS)], axis=0) for a in tails]
            for p in [t % 2, 1 - t % 2]:
                pieces.append(block[:, p * half:(p + 1) * half].reshape(rows, kv_rank))
                packs += [jnp.where(part == p * groups + s, tails[d], 0.0).astype(jnp.bfloat16) for d in range(2) for s in range(groups)]
        c_all = jnp.concatenate(pieces, axis=0)
        krt = mm(same, jnp.concatenate(packs, axis=0), NT).astype(jnp.bfloat16)
        spots = [((t + i) % 2, (t - t % 2 + i) * rows, (2 * j + i) * rows) for j, t in enumerate(slots) for i in range(2)]
        for p, at, src in spots:
            krt_v[p, :, at:at + rows] = krt[:, src:src + rows]
        for c in range(pairs // 2):
            cols = slice(c * 2 * LANES, (c + 1) * 2 * LANES)
            k = mm(c_all, wuk_v[:, cols]).astype(jnp.bfloat16)
            for i in range(2):
                kt = k[:, i * LANES:(i + 1) * LANES].T
                for p, at, src in spots:
                    kt_v[2 * c + i, p, :, at:at + rows] = kt[:, src:src + rows]
        for c in range(pairs // 2):
            cols = slice(c * 2 * LANES, (c + 1) * 2 * LANES)
            v = mm(c_all, wuv_v[:, cols]).astype(jnp.bfloat16)
            for i in range(2):
                for p, at, src in spots:
                    v_v[2 * c + i, p, at:at + rows] = v[src:src + rows, i * LANES:(i + 1) * LANES]

    get_wuk.wait()
    get_wuv.wait()
    factor = (nope + rope) ** -0.5 * math.log2(math.e)

    def scores(g, part):
        for i in range(GROUP):
            p = g * GROUP + i
            top = rows if part == "second" else 0
            early = jnp.concatenate([kt_v[p, 0], krt_v[0]], axis=0)
            late = jnp.concatenate([kt_v[p, 1], krt_v[1]], axis=0)
            s_v[g % 2, i, top:count] = mm(qcat[p, top:], early) * factor + bias_v[top:count]
            s_v[g % 2, i, count:] = mm(qcat[p, rows:], late) * factor + bias_v[count:]

    def halves(a, op):
        return op(a[:, :LANES], a[:, LANES:])

    def weights(g, part):
        for i in range(GROUP):
            if part != "second":
                a = s_v[g % 2, i, :rows]
                m_a = jnp.max(halves(a, jnp.maximum), axis=1, keepdims=True)
                a = jnp.exp2(a - m_a)
                p_v[g % 2, i, :rows] = a.astype(jnp.bfloat16)
                l_a = jnp.sum(halves(a, jnp.add), axis=1, keepdims=True)
                l_v[g % 2, i, :rows] = jnp.broadcast_to(1.0 / l_a, (rows, LANES))
            b, c = s_v[g % 2, i, rows:count], s_v[g % 2, i, count:]
            m_b = jnp.max(jnp.maximum(halves(b, jnp.maximum), halves(c, jnp.maximum)), axis=1, keepdims=True)
            b, c = jnp.exp2(b - m_b), jnp.exp2(c - m_b)
            p_v[g % 2, i, rows:count] = b.astype(jnp.bfloat16)
            p_v[g % 2, i, count:] = c.astype(jnp.bfloat16)
            l_b = jnp.sum(halves(b, jnp.add) + halves(c, jnp.add), axis=1, keepdims=True)
            l_v[g % 2, i, rows:] = jnp.broadcast_to(1.0 / l_b, (rows, LANES))

    def values(g, part):
        for i in range(GROUP):
            cols = slice((g * GROUP + i) * LANES, (g * GROUP + i + 1) * LANES)
            o = mm(p_v[g % 2, i, rows if part == "second" else 0:count], v_v[g * GROUP + i, 0])
            o_b = (o[-rows:] + mm(p_v[g % 2, i, count:], v_v[g * GROUP + i, 1])) * l_v[g % 2, i, rows:]
            o_v[half:, cols] = jnp.where(low[:half], o_b[:half], o_b[half:]).astype(jnp.bfloat16)
            if part != "second":
                o_a = o[:rows] * l_v[g % 2, i, :rows]
                o_v[:half, cols] = jnp.where(low[:half], o_a[:half], o_a[half:]).astype(jnp.bfloat16)

    def project(g):
        for c in range(width // panel):
            cols = slice(c * panel, (c + 1) * panel)
            y = mm(o_v[:, g * deep:(g + 1) * deep], wout_v[g * deep:(g + 1) * deep, cols])
            if g > 0:
                y += y_sum[:, cols]
            if g + 1 < steps:
                y_sum[:, cols] = y
            else:
                y_v[:, cols] = y.astype(jnp.bfloat16)

    def first_queries():
        for p in range(pairs):
            own = jnp.concatenate([kt_v[p, 0, :, :rows], krt_v[0, :, :rows]], axis=0)
            fs_v[p] = mm(qcat[p, :rows], own) * factor + bias_v[:rows, :rows]
        for p in range(pairs):
            a = fs_v[p]
            a = jnp.exp2(a - jnp.max(a, axis=1, keepdims=True))
            fp_v[p] = a.astype(jnp.bfloat16)
            fl_v[p] = jnp.broadcast_to(1.0 / jnp.sum(a, axis=1, keepdims=True), (rows, LANES))
        for p in range(pairs):
            o = mm(fp_v[p], v_v[p, 0, :rows]) * fl_v[p]
            o_v[:half, p * LANES:(p + 1) * LANES] = jnp.where(low[:half], o[:half], o[half:]).astype(jnp.bfloat16)

    def receive(t):
        for d in range(2):
            push(2 * chip_at(t) + d, me, 0).wait_recv()

    even = jnp.logical_not(odd)
    push(partner, me, 0).wait_recv()

    @pl.when(odd)
    def _():
        relay(1)
        up_project([0, 1])
        pl.when(my_chip == 0)(first_queries)
        for t in range(2, chips):
            relay(t)

    @pl.when(even)
    def _():
        up_project([0])
        pl.when(my_chip == 0)(first_queries)
        receive(1)
        up_project([1])

    for t in range(2, chips):
        pl.when(even)(functools.partial(receive, t))
        up_project([t])

    def finish(part):
        for g in range(steps + 3):
            if g == 3:
                for get in get_wout:
                    get.wait()
            if g >= 3:
                project(g - 3)
            if 2 <= g < steps + 2:
                values(g - 2, part)
            if 1 <= g <= steps:
                weights(g - 1, part)
            if g < steps:
                scores(g, part)

    pl.when(my_chip == 0)(functools.partial(finish, "second"))
    pl.when(my_chip > 0)(functools.partial(finish, "both"))
    for cp in sends:
        cp.wait_send()

    @pl.when(odd)
    def _():
        for t in range(1, chips):
            for cp in forward(t):
                cp.wait_send()


def solution(mesh):
    n = mesh.shape["ctx"]
    row_spec = P(("dp", "ctx"), None)
    id_spec = P(("dp", "ctx"))

    def per_device(x, pos, seg, w_dq, w_uq, w_qr, w_dkv, w_kr, w_uk, w_uv, w_out, gain_q, gain_kv):
        rows, width = x.shape
        pairs = w_uq.shape[1] // LANES
        keys = n * rows
        kv_rank = w_dkv.shape[1]
        rope = w_kr.shape[1]
        bf, f32 = jnp.bfloat16, jnp.float32
        args = (x, pos.reshape(1, rows), w_dq, w_uq, w_qr, w_dkv, w_kr.T, w_uk, w_uv, w_out,
                gain_q, gain_kv)
        scratch = [pltpu.VMEM(a.shape, a.dtype) for a in args]
        scratch += [
            pltpu.VMEM((n, rows + PACK_ROWS // PACKS, kv_rank), bf),
            pltpu.VMEM((2, rows, kv_rank), f32),
            pltpu.VMEM((rows, w_dq.shape[1]), bf),
            pltpu.VMEM((pairs, 2 * rows, LANES + rope), bf),
            pltpu.VMEM((pairs, 2, LANES, keys // 2), bf),
            pltpu.VMEM((2, rope, keys // 2), bf),
            pltpu.VMEM((pairs, 2, keys // 2, LANES), bf),
            pltpu.VMEM((3 * rows, keys // 2), f32),
            pltpu.VMEM((rows, w_uv.shape[1]), bf),
            pltpu.VMEM((2, GROUP, 3 * rows, keys // 2), f32),
            pltpu.VMEM((2, GROUP, 3 * rows, keys // 2), bf),
            pltpu.VMEM((2, GROUP, 2 * rows, LANES), f32),
            pltpu.VMEM((rows, width), f32),
            pltpu.VMEM((pairs, rows, rows), f32),
            pltpu.VMEM((pairs, rows, rows), bf),
            pltpu.VMEM((pairs, rows, LANES), f32),
            pltpu.SemaphoreType.DMA((len(args) - 2 + len(KV_CUTS) - 1 + pairs // GROUP,)),
            pltpu.SemaphoreType.DMA((n // 2 + n - 2,)),
            pltpu.SemaphoreType.DMA((n,)),
        ]
        return pl.pallas_call(
            functools.partial(layer_kernel, n),
            out_shape=pltpu.VMEM(x.shape, bf),
            in_specs=[pl.BlockSpec(memory_space=pltpu.HBM)] * len(args),
            out_specs=pl.BlockSpec(memory_space=pltpu.VMEM),
            scratch_shapes=scratch,
            compiler_params=pltpu.CompilerParams(collective_id=0, has_side_effects=True, vmem_limit_bytes=62000000),
        )(*args)

    return jax.shard_map(per_device, mesh=mesh, in_specs=(row_spec, id_spec, id_spec) + (P(),) * 10, out_specs=row_spec, check_vma=False)
```

```python
import functools
import math

import jax
import jax.numpy as jnp
import numpy as np
from jax import lax
from jax.experimental import pallas as pl
from jax.experimental.pallas import tpu as pltpu
from jax.sharding import PartitionSpec as P

NORM_EPS = 1e-6
MASKED = -1e30
LANES = 128
PACK_ROWS = 16
PACKS = 2
GROUP = 4
KV_CUTS = (0, 2, 4, 6, 8, 10)
MESH = pl.DeviceIdType.MESH
NT = (((1,), (1,)), ((), ()))


def mm(a, b, dims=(((1,), (0,)), ((), ()))):
    return lax.dot_general(a, b, dims, preferred_element_type=jnp.float32)


def rms_norm(vals, gain):
    mean_sq = jnp.mean(vals * vals, axis=-1, keepdims=True)
    return (vals * lax.rsqrt(mean_sq + NORM_EPS) * gain).astype(jnp.bfloat16)


def iota(shape, dim):
    return lax.broadcasted_iota(jnp.int32, shape, dim)


def layer_kernel(n, x_h, pos_h, wdq_h, wuq_h, wqr_h, wdkv_h, wkr_h, wuk_h, wuv_h, wout_h, gq_h, gkv_h, y_v,
                 x_v, pos_v, wdq_v, wuq_v, wqr_v, wdkv_v, wkr_v, wuk_v, wuv_v, wout_v, gq_v, gkv_v,
                 lat, kv_v, cq_v, qcat, kt_v, krt_v, v_v, bias_v, o_v, s_v, p_v, l_v, y_sum, fs_v, fp_v, fl_v, in_sem, send_sem, recv_sem):
    rows, width = x_v.shape
    kv_rank = wdkv_v.shape[1]
    rope = wkr_v.shape[0]
    half_rope = rope // 2
    pairs = kt_v.shape[0]
    nope = LANES // 2
    half = rows // 2
    chips = n // 2
    keys = chips * rows
    pack_rows = PACK_ROWS // PACKS
    steps = pairs // GROUP
    deep = GROUP * LANES
    panel = 2 * LANES

    me = lax.axis_index("ctx")
    my_chip = me // 2
    partner = me + 1 - 2 * lax.rem(me, 2)
    odd = lax.rem(me, 2) == 1

    def chip_at(slot):
        return jnp.where(slot == 0, my_chip, jnp.where(slot > my_chip, slot, slot - 1))


    fetches = []

    def fetch(src, dst):
        fetches.append(pltpu.make_async_copy(src, dst, in_sem.at[len(fetches)]))
        return fetches[-1]

    def start(*copies):
        for cp in copies:
            cp.start()

    get_pos = fetch(pos_h, pos_v)
    get_x = fetch(x_h, x_v)
    get_wkr = fetch(wkr_h, wkr_v)
    depth = 2 * LANES
    cuts = [width // depth * c // 10 * depth for c in KV_CUTS]
    get_wdkv = [fetch(wdkv_h.at[pl.ds(lo, hi - lo)], wdkv_v.at[pl.ds(lo, hi - lo)]) for lo, hi in zip(cuts, cuts[1:])]
    get_gkv = fetch(gkv_h, gkv_v)
    get_gq = fetch(gq_h, gq_v)
    get_wdq = fetch(wdq_h, wdq_v)
    get_wuq = fetch(wuq_h, wuq_v)
    get_wqr = fetch(wqr_h, wqr_v)
    get_wuk = fetch(wuk_h, wuk_v)
    get_wuv = fetch(wuv_h, wuv_v)
    get_wout = [fetch(wout_h.at[pl.ds(g * deep, deep)], wout_v.at[pl.ds(g * deep, deep)]) for g in range(steps)]
    start(get_pos, get_x, get_wkr, get_gkv, *get_wdkv, get_gq, get_wdq, get_wuq, get_wqr, get_wuk, get_wuv, *get_wout)

    barrier = pltpu.get_barrier_semaphore()
    pl.semaphore_signal(barrier, inc=1, device_id={"ctx": partner}, device_id_type=MESH)

    @pl.when(odd)
    def _():
        for t in range(1, chips):
            for d in range(2):
                pl.semaphore_signal(barrier, inc=1, device_id={"ctx": 2 * chip_at(t) + d}, device_id_type=MESH)

    get_pos.wait()
    get_x.wait()
    get_wkr.wait()
    pos_row = pos_v[...].astype(jnp.float32)

    def pos_of(count, index):
        spot = iota((count, rows), 1) == index(iota((count, rows), 0))
        return jnp.sum(jnp.where(spot, jnp.broadcast_to(pos_row, (count, rows)), 0.0), axis=1, keepdims=True)

    lane = iota((rows, LANES), 1)
    freq_id = lax.rem(lane[:1], half_rope)
    inv_freq = jnp.zeros((1, LANES), jnp.float32)
    for f in range(half_rope):
        inv_freq = jnp.where(freq_id == f, float(np.float32(10000.0 ** (-2.0 * f / rope))), inv_freq)
    angles = pos_of(rows, lambda r: r) * inv_freq
    first = lax.rem(lane, rope) < half_rope
    cos_tab = jnp.cos(angles)
    sin_tab = jnp.sin(angles)
    sin_tab = jnp.where(first, -sin_tab, sin_tab)

    def rope_lanes(a):
        other = jnp.where(first, pltpu.roll(a, LANES - half_rope, 1), pltpu.roll(a, half_rope, 1))
        return (a * cos_tab + other * sin_tab).astype(jnp.bfloat16)

    count = 2 * rows
    q_pos = pos_of(count, lambda r: lax.rem(r, half) + jnp.where(r >= rows, half, 0)).astype(jnp.int32)
    q_row = iota((count, 1), 0)
    q_seq = jnp.where(q_row < rows, half * me, half * (2 * n - 1 - me)) + lax.rem(q_row, half)
    q_first = q_seq - q_pos
    col = iota((1, keys), 1)
    slot = col // rows
    swapped = slot + 1 - 2 * lax.rem(slot, 2)
    inner = lax.rem(col, rows)

    def key_seq(slot, late):
        dev = 2 * chip_at(slot) + inner // half
        return half * jnp.where(late, 2 * n - 1 - dev, dev) + lax.rem(inner, half)

    def visible(seq, lo, hi):
        return jnp.where((seq >= lo) & (seq <= hi), 0.0, MASKED)

    bias_v[:count] = visible(key_seq(slot, False), q_first, q_seq)
    bias_v[count:] = visible(key_seq(swapped, True), q_first[rows:], q_seq[rows:])

    kr = mm(x_v[...], wkr_v[...], NT)
    for get in get_wdkv:
        get.wait()
    for i in range(2):
        at = slice(i * width // 2, (i + 1) * width // 2)
        kv_v[i] = mm(x_v[:, at], wdkv_v[at])
    turn = lax.rem(me, 2)
    kv = kv_v[turn] + kv_v[1 - turn]
    get_gkv.wait()
    c_kv = rms_norm(kv, gkv_v[...].astype(jnp.float32).reshape(1, -1))
    lat[me, :rows, :] = c_kv
    kr = rope_lanes(jnp.concatenate([kr] * (LANES // rope), axis=1))
    packed = jnp.zeros((PACK_ROWS, LANES), jnp.float32)
    kr = kr.astype(jnp.float32)
    part = iota((PACK_ROWS, LANES), 1) // rope
    for s in range(rows // PACK_ROWS):
        packed = jnp.where(part == s, kr[s * PACK_ROWS:(s + 1) * PACK_ROWS], packed)
    for i in range(PACKS):
        lat[me, rows:, i * LANES:(i + 1) * LANES] = packed[i * pack_rows:(i + 1) * pack_rows].astype(jnp.bfloat16)

    pl.semaphore_wait(barrier, chips)

    def push(block, peer, index):
        return pltpu.make_async_remote_copy(src_ref=lat.at[block], dst_ref=lat.at[block], send_sem=send_sem.at[index],
                                            recv_sem=recv_sem.at[block], device_id={"ctx": peer}, device_id_type=MESH)

    sends = [push(me, 2 * chip_at(t) + 1, t) for t in range(1, chips)] + [push(me, partner, 0)]
    start(*sends)

    def forward(t):
        return [push(2 * chip_at(t) + d, partner, chips + 2 * (t - 1) + d) for d in range(2)]

    def relay(t):
        for d, cp in enumerate(forward(t)):
            push(2 * chip_at(t) + d, me, 0).wait_recv()
            cp.start()

    get_gq.wait()
    get_wdq.wait()
    cq_v[...] = rms_norm(mm(x_v[...], wdq_v[...]), gq_v[...].astype(jnp.float32).reshape(1, -1))
    low = lane < nope
    zero = jnp.zeros((rows, LANES), jnp.bfloat16)

    def put_query(head, cols, t):
        at = head % 2 * half
        qcat[head // 2, at:at + half, cols] = t[:half]
        qcat[head // 2, rows + at:rows + at + half, cols] = t[half:]

    get_wuq.wait()
    for c in range(pairs // 4):
        q = mm(cq_v[...], wuq_v[:, c * 4 * LANES:(c + 1) * 4 * LANES]).astype(jnp.bfloat16)
        for i in range(4):
            t = q[:, i * LANES:(i + 1) * LANES]
            put_query(2 * (c * 4 + i), slice(0, LANES), jnp.where(low, t, zero))
            put_query(2 * (c * 4 + i) + 1, slice(0, LANES), jnp.where(low, zero, t))
    get_wqr.wait()
    per = LANES // rope
    for c in range(pairs // per):
        q = mm(cq_v[...], wqr_v[:, c * 2 * LANES:(c + 1) * 2 * LANES])
        for i in range(2):
            t = rope_lanes(q[:, i * LANES:(i + 1) * LANES])
            for s in range(per):
                put_query((c * 2 + i) * per + s, slice(LANES, LANES + rope), t[:, s * rope:(s + 1) * rope])

    same = iota((rope, LANES), 0) == lax.rem(iota((rope, LANES), 1), rope)
    same = jnp.where(same, 1.0, 0.0).astype(jnp.bfloat16)

    def up_project(slots):
        pieces, packs = [], []
        groups = half // PACK_ROWS
        for t in slots:
            chip = chip_at(t)
            block = lat[pl.ds(2 * chip, 2), :rows]
            tails = [lat[2 * chip + d, rows:].astype(jnp.float32) for d in range(2)]
            tails = [jnp.concatenate([a[:, i * LANES:(i + 1) * LANES] for i in range(PACKS)], axis=0) for a in tails]
            for p in [t % 2, 1 - t % 2]:
                pieces.append(block[:, p * half:(p + 1) * half].reshape(rows, kv_rank))
                packs += [jnp.where(part == p * groups + s, tails[d], 0.0).astype(jnp.bfloat16) for d in range(2) for s in range(groups)]
        c_all = jnp.concatenate(pieces, axis=0)
        krt = mm(same, jnp.concatenate(packs, axis=0), NT).astype(jnp.bfloat16)
        spots = [((t + i) % 2, (t - t % 2 + i) * rows, (2 * j + i) * rows) for j, t in enumerate(slots) for i in range(2)]
        for p, at, src in spots:
            krt_v[p, :, at:at + rows] = krt[:, src:src + rows]
        for c in range(pairs // 2):
            cols = slice(c * 2 * LANES, (c + 1) * 2 * LANES)
            k = mm(c_all, wuk_v[:, cols]).astype(jnp.bfloat16)
            for i in range(2):
                kt = k[:, i * LANES:(i + 1) * LANES].T
                for p, at, src in spots:
                    kt_v[2 * c + i, p, :, at:at + rows] = kt[:, src:src + rows]
        for c in range(pairs // 2):
            cols = slice(c * 2 * LANES, (c + 1) * 2 * LANES)
            v = mm(c_all, wuv_v[:, cols]).astype(jnp.bfloat16)
            for i in range(2):
                for p, at, src in spots:
                    v_v[2 * c + i, p, at:at + rows] = v[src:src + rows, i * LANES:(i + 1) * LANES]

    get_wuk.wait()
    get_wuv.wait()
    factor = (nope + rope) ** -0.5 * math.log2(math.e)

    def scores(g, part):
        for i in range(GROUP):
            p = g * GROUP + i
            top = rows if part == "second" else 0
            early = jnp.concatenate([kt_v[p, 0], krt_v[0]], axis=0)
            late = jnp.concatenate([kt_v[p, 1], krt_v[1]], axis=0)
            s_v[g % 2, i, top:count] = mm(qcat[p, top:], early) * factor + bias_v[top:count]
            s_v[g % 2, i, count:] = mm(qcat[p, rows:], late) * factor + bias_v[count:]

    def halves(a, op):
        return op(a[:, :LANES], a[:, LANES:])

    def weights(g, part):
        for i in range(GROUP):
            if part != "second":
                a = s_v[g % 2, i, :rows]
                m_a = jnp.max(halves(a, jnp.maximum), axis=1, keepdims=True)
                a = jnp.exp2(a - m_a)
                p_v[g % 2, i, :rows] = a.astype(jnp.bfloat16)
                l_a = jnp.sum(halves(a, jnp.add), axis=1, keepdims=True)
                l_v[g % 2, i, :rows] = jnp.broadcast_to(1.0 / l_a, (rows, LANES))
            b, c = s_v[g % 2, i, rows:count], s_v[g % 2, i, count:]
            m_b = jnp.max(jnp.maximum(halves(b, jnp.maximum), halves(c, jnp.maximum)), axis=1, keepdims=True)
            b, c = jnp.exp2(b - m_b), jnp.exp2(c - m_b)
            p_v[g % 2, i, rows:count] = b.astype(jnp.bfloat16)
            p_v[g % 2, i, count:] = c.astype(jnp.bfloat16)
            l_b = jnp.sum(halves(b, jnp.add) + halves(c, jnp.add), axis=1, keepdims=True)
            l_v[g % 2, i, rows:] = jnp.broadcast_to(1.0 / l_b, (rows, LANES))

    def values(g, part):
        for i in range(GROUP):
            cols = slice((g * GROUP + i) * LANES, (g * GROUP + i + 1) * LANES)
            o = mm(p_v[g % 2, i, rows if part == "second" else 0:count], v_v[g * GROUP + i, 0])
            o_b = (o[-rows:] + mm(p_v[g % 2, i, count:], v_v[g * GROUP + i, 1])) * l_v[g % 2, i, rows:]
            o_v[half:, cols] = jnp.where(low[:half], o_b[:half], o_b[half:]).astype(jnp.bfloat16)
            if part != "second":
                o_a = o[:rows] * l_v[g % 2, i, :rows]
                o_v[:half, cols] = jnp.where(low[:half], o_a[:half], o_a[half:]).astype(jnp.bfloat16)

    def project(g):
        for c in range(width // panel):
            cols = slice(c * panel, (c + 1) * panel)
            y = mm(o_v[:, g * deep:(g + 1) * deep], wout_v[g * deep:(g + 1) * deep, cols])
            if g > 0:
                y += y_sum[:, cols]
            if g + 1 < steps:
                y_sum[:, cols] = y
            else:
                y_v[:, cols] = y.astype(jnp.bfloat16)

    def first_queries():
        for p in range(pairs):
            own = jnp.concatenate([kt_v[p, 0, :, :rows], krt_v[0, :, :rows]], axis=0)
            fs_v[p] = mm(qcat[p, :rows], own) * factor + bias_v[:rows, :rows]
        for p in range(pairs):
            a = fs_v[p]
            a = jnp.exp2(a - jnp.max(a, axis=1, keepdims=True))
            fp_v[p] = a.astype(jnp.bfloat16)
            fl_v[p] = jnp.broadcast_to(1.0 / jnp.sum(a, axis=1, keepdims=True), (rows, LANES))
        for p in range(pairs):
            o = mm(fp_v[p], v_v[p, 0, :rows]) * fl_v[p]
            o_v[:half, p * LANES:(p + 1) * LANES] = jnp.where(low[:half], o[:half], o[half:]).astype(jnp.bfloat16)

    def receive(t):
        for d in range(2):
            push(2 * chip_at(t) + d, me, 0).wait_recv()

    even = jnp.logical_not(odd)
    push(partner, me, 0).wait_recv()

    @pl.when(odd)
    def _():
        relay(1)
        up_project([0, 1])
        for t in range(2, chips):
            relay(t)

    @pl.when(even)
    def _():
        up_project([0])
        pl.when(me == 0)(first_queries)
        receive(1)
        up_project([1])

    for t in range(2, chips):
        pl.when(even)(functools.partial(receive, t))
        up_project([t])

    def finish(part):
        for g in range(steps + 3):
            if g == 3:
                for get in get_wout:
                    get.wait()
            if g >= 3:
                project(g - 3)
            if 2 <= g < steps + 2:
                values(g - 2, part)
            if 1 <= g <= steps:
                weights(g - 1, part)
            if g < steps:
                scores(g, part)

    pl.when(me == 0)(functools.partial(finish, "second"))
    pl.when(me > 0)(functools.partial(finish, "both"))
    for cp in sends:
        cp.wait_send()

    @pl.when(odd)
    def _():
        for t in range(1, chips):
            for cp in forward(t):
                cp.wait_send()


def solution(mesh):
    n = mesh.shape["ctx"]
    row_spec = P(("dp", "ctx"), None)
    id_spec = P(("dp", "ctx"))

    def per_device(x, pos, seg, w_dq, w_uq, w_qr, w_dkv, w_kr, w_uk, w_uv, w_out, gain_q, gain_kv):
        rows, width = x.shape
        pairs = w_uq.shape[1] // LANES
        keys = n * rows
        kv_rank = w_dkv.shape[1]
        rope = w_kr.shape[1]
        bf, f32 = jnp.bfloat16, jnp.float32
        args = (x, pos.reshape(1, rows), w_dq, w_uq, w_qr, w_dkv, w_kr.T, w_uk, w_uv, w_out,
                gain_q, gain_kv)
        scratch = [pltpu.VMEM(a.shape, a.dtype) for a in args]
        scratch += [
            pltpu.VMEM((n, rows + PACK_ROWS // PACKS, kv_rank), bf),
            pltpu.VMEM((2, rows, kv_rank), f32),
            pltpu.VMEM((rows, w_dq.shape[1]), bf),
            pltpu.VMEM((pairs, 2 * rows, LANES + rope), bf),
            pltpu.VMEM((pairs, 2, LANES, keys // 2), bf),
            pltpu.VMEM((2, rope, keys // 2), bf),
            pltpu.VMEM((pairs, 2, keys // 2, LANES), bf),
            pltpu.VMEM((3 * rows, keys // 2), f32),
            pltpu.VMEM((rows, w_uv.shape[1]), bf),
            pltpu.VMEM((2, GROUP, 3 * rows, keys // 2), f32),
            pltpu.VMEM((2, GROUP, 3 * rows, keys // 2), bf),
            pltpu.VMEM((2, GROUP, 2 * rows, LANES), f32),
            pltpu.VMEM((rows, width), f32),
            pltpu.VMEM((pairs, rows, rows), f32),
            pltpu.VMEM((pairs, rows, rows), bf),
            pltpu.VMEM((pairs, rows, LANES), f32),
            pltpu.SemaphoreType.DMA((len(args) - 2 + len(KV_CUTS) - 1 + pairs // GROUP,)),
            pltpu.SemaphoreType.DMA((n // 2 + n - 2,)),
            pltpu.SemaphoreType.DMA((n,)),
        ]
        return pl.pallas_call(
            functools.partial(layer_kernel, n),
            out_shape=pltpu.VMEM(x.shape, bf),
            in_specs=[pl.BlockSpec(memory_space=pltpu.HBM)] * len(args),
            out_specs=pl.BlockSpec(memory_space=pltpu.VMEM),
            scratch_shapes=scratch,
            compiler_params=pltpu.CompilerParams(collective_id=0, has_side_effects=True, vmem_limit_bytes=62000000),
        )(*args)

    return jax.shard_map(per_device, mesh=mesh, in_specs=(row_spec, id_spec, id_spec) + (P(),) * 10, out_specs=row_spec, check_vma=False)
```

```python
import functools
import math

import jax
import jax.numpy as jnp
import numpy as np
from jax import lax
from jax.experimental import pallas as pl
from jax.experimental.pallas import tpu as pltpu
from jax.sharding import PartitionSpec as P

NORM_EPS = 1e-6
MASKED = -1e30
LANES = 128
PACK_ROWS = 16
PACKS = 2
GROUP = 4
KV_CUTS = (0, 2, 4, 6, 8, 10)
MESH = pl.DeviceIdType.MESH
NT = (((1,), (1,)), ((), ()))


def mm(a, b, dims=(((1,), (0,)), ((), ()))):
    return lax.dot_general(a, b, dims, preferred_element_type=jnp.float32)


def rms_norm(vals, gain):
    mean_sq = jnp.mean(vals * vals, axis=-1, keepdims=True)
    return (vals * lax.rsqrt(mean_sq + NORM_EPS) * gain).astype(jnp.bfloat16)


def iota(shape, dim):
    return lax.broadcasted_iota(jnp.int32, shape, dim)


def layer_kernel(n, x_h, pos_h, wdq_h, wuq_h, wqr_h, wdkv_h, wkr_h, wuk_h, wuv_h, wout_h, gq_h, gkv_h, y_v,
                 x_v, pos_v, wdq_v, wuq_v, wqr_v, wdkv_v, wkr_v, wuk_v, wuv_v, wout_v, gq_v, gkv_v,
                 lat, kv_v, cq_v, qcat, kt_v, krt_v, v_v, bias_v, o_v, s_v, p_v, l_v, y_sum, in_sem, send_sem, recv_sem):
    rows, width = x_v.shape
    kv_rank = wdkv_v.shape[1]
    rope = wkr_v.shape[0]
    half_rope = rope // 2
    pairs = kt_v.shape[0]
    nope = LANES // 2
    half = rows // 2
    chips = n // 2
    keys = chips * rows
    pack_rows = PACK_ROWS // PACKS
    steps = pairs // GROUP
    deep = GROUP * LANES
    panel = 2 * LANES

    me = lax.axis_index("ctx")
    my_chip = me // 2
    partner = me + 1 - 2 * lax.rem(me, 2)
    odd = lax.rem(me, 2) == 1

    def chip_at(slot):
        return jnp.where(slot == 0, my_chip, jnp.where(slot > my_chip, slot, slot - 1))


    fetches = []

    def fetch(src, dst):
        fetches.append(pltpu.make_async_copy(src, dst, in_sem.at[len(fetches)]))
        return fetches[-1]

    def start(*copies):
        for cp in copies:
            cp.start()

    get_pos = fetch(pos_h, pos_v)
    get_x = fetch(x_h, x_v)
    get_wkr = fetch(wkr_h, wkr_v)
    depth = 2 * LANES
    cuts = [width // depth * c // 10 * depth for c in KV_CUTS]
    get_wdkv = [fetch(wdkv_h.at[pl.ds(lo, hi - lo)], wdkv_v.at[pl.ds(lo, hi - lo)]) for lo, hi in zip(cuts, cuts[1:])]
    get_gkv = fetch(gkv_h, gkv_v)
    get_gq = fetch(gq_h, gq_v)
    get_wdq = fetch(wdq_h, wdq_v)
    get_wuq = fetch(wuq_h, wuq_v)
    get_wqr = fetch(wqr_h, wqr_v)
    get_wuk = fetch(wuk_h, wuk_v)
    get_wuv = fetch(wuv_h, wuv_v)
    get_wout = [fetch(wout_h.at[pl.ds(g * deep, deep)], wout_v.at[pl.ds(g * deep, deep)]) for g in range(steps)]
    start(get_pos, get_x, get_wkr, get_gkv, *get_wdkv, get_gq, get_wdq, get_wuq, get_wqr, get_wuk, get_wuv, *get_wout)

    barrier = pltpu.get_barrier_semaphore()
    pl.semaphore_signal(barrier, inc=1, device_id={"ctx": partner}, device_id_type=MESH)

    @pl.when(odd)
    def _():
        for t in range(1, chips):
            for d in range(2):
                pl.semaphore_signal(barrier, inc=1, device_id={"ctx": 2 * chip_at(t) + d}, device_id_type=MESH)

    get_pos.wait()
    get_x.wait()
    get_wkr.wait()
    pos_row = pos_v[...].astype(jnp.float32)

    def pos_of(count, index):
        spot = iota((count, rows), 1) == index(iota((count, rows), 0))
        return jnp.sum(jnp.where(spot, jnp.broadcast_to(pos_row, (count, rows)), 0.0), axis=1, keepdims=True)

    lane = iota((rows, LANES), 1)
    freq_id = lax.rem(lane[:1], half_rope)
    inv_freq = jnp.zeros((1, LANES), jnp.float32)
    for f in range(half_rope):
        inv_freq = jnp.where(freq_id == f, float(np.float32(10000.0 ** (-2.0 * f / rope))), inv_freq)
    angles = pos_of(rows, lambda r: r) * inv_freq
    first = lax.rem(lane, rope) < half_rope
    cos_tab = jnp.cos(angles)
    sin_tab = jnp.sin(angles)
    sin_tab = jnp.where(first, -sin_tab, sin_tab)

    def rope_lanes(a):
        other = jnp.where(first, pltpu.roll(a, LANES - half_rope, 1), pltpu.roll(a, half_rope, 1))
        return (a * cos_tab + other * sin_tab).astype(jnp.bfloat16)

    count = 2 * rows
    q_pos = pos_of(count, lambda r: lax.rem(r, half) + jnp.where(r >= rows, half, 0)).astype(jnp.int32)
    q_row = iota((count, 1), 0)
    q_seq = jnp.where(q_row < rows, half * me, half * (2 * n - 1 - me)) + lax.rem(q_row, half)
    q_first = q_seq - q_pos
    col = iota((1, keys), 1)
    slot = col // rows
    swapped = slot + 1 - 2 * lax.rem(slot, 2)
    inner = lax.rem(col, rows)

    def key_seq(slot, late):
        dev = 2 * chip_at(slot) + inner // half
        return half * jnp.where(late, 2 * n - 1 - dev, dev) + lax.rem(inner, half)

    def visible(seq, lo, hi):
        return jnp.where((seq >= lo) & (seq <= hi), 0.0, MASKED)

    bias_v[:count] = visible(key_seq(slot, False), q_first, q_seq)
    bias_v[count:] = visible(key_seq(swapped, True), q_first[rows:], q_seq[rows:])

    kr = mm(x_v[...], wkr_v[...], NT)
    for get in get_wdkv:
        get.wait()
    for i in range(2):
        at = slice(i * width // 2, (i + 1) * width // 2)
        kv_v[i] = mm(x_v[:, at], wdkv_v[at])
    turn = lax.rem(me, 2)
    kv = kv_v[turn] + kv_v[1 - turn]
    get_gkv.wait()
    c_kv = rms_norm(kv, gkv_v[...].astype(jnp.float32).reshape(1, -1))
    lat[me, :rows, :] = c_kv
    kr = rope_lanes(jnp.concatenate([kr] * (LANES // rope), axis=1))
    packed = jnp.zeros((PACK_ROWS, LANES), jnp.float32)
    kr = kr.astype(jnp.float32)
    part = iota((PACK_ROWS, LANES), 1) // rope
    for s in range(rows // PACK_ROWS):
        packed = jnp.where(part == s, kr[s * PACK_ROWS:(s + 1) * PACK_ROWS], packed)
    for i in range(PACKS):
        lat[me, rows:, i * LANES:(i + 1) * LANES] = packed[i * pack_rows:(i + 1) * pack_rows].astype(jnp.bfloat16)

    pl.semaphore_wait(barrier, chips)

    def push(block, peer, index):
        return pltpu.make_async_remote_copy(src_ref=lat.at[block], dst_ref=lat.at[block], send_sem=send_sem.at[index],
                                            recv_sem=recv_sem.at[block], device_id={"ctx": peer}, device_id_type=MESH)

    sends = [push(me, 2 * chip_at(t) + 1, t) for t in range(1, chips)] + [push(me, partner, 0)]
    start(*sends)

    def forward(t):
        return [push(2 * chip_at(t) + d, partner, chips + 2 * (t - 1) + d) for d in range(2)]

    def relay(t):
        for d, cp in enumerate(forward(t)):
            push(2 * chip_at(t) + d, me, 0).wait_recv()
            cp.start()

    get_gq.wait()
    get_wdq.wait()
    cq_v[...] = rms_norm(mm(x_v[...], wdq_v[...]), gq_v[...].astype(jnp.float32).reshape(1, -1))
    low = lane < nope
    zero = jnp.zeros((rows, LANES), jnp.bfloat16)

    def put_query(head, cols, t):
        at = head % 2 * half
        qcat[head // 2, at:at + half, cols] = t[:half]
        qcat[head // 2, rows + at:rows + at + half, cols] = t[half:]

    get_wuq.wait()
    for c in range(pairs // 4):
        q = mm(cq_v[...], wuq_v[:, c * 4 * LANES:(c + 1) * 4 * LANES]).astype(jnp.bfloat16)
        for i in range(4):
            t = q[:, i * LANES:(i + 1) * LANES]
            put_query(2 * (c * 4 + i), slice(0, LANES), jnp.where(low, t, zero))
            put_query(2 * (c * 4 + i) + 1, slice(0, LANES), jnp.where(low, zero, t))
    get_wqr.wait()
    per = LANES // rope
    for c in range(pairs // per):
        q = mm(cq_v[...], wqr_v[:, c * 2 * LANES:(c + 1) * 2 * LANES])
        for i in range(2):
            t = rope_lanes(q[:, i * LANES:(i + 1) * LANES])
            for s in range(per):
                put_query((c * 2 + i) * per + s, slice(LANES, LANES + rope), t[:, s * rope:(s + 1) * rope])

    same = iota((rope, LANES), 0) == lax.rem(iota((rope, LANES), 1), rope)
    same = jnp.where(same, 1.0, 0.0).astype(jnp.bfloat16)

    def up_project(slots):
        pieces, packs = [], []
        groups = half // PACK_ROWS
        for t in slots:
            chip = chip_at(t)
            block = lat[pl.ds(2 * chip, 2), :rows]
            tails = [lat[2 * chip + d, rows:].astype(jnp.float32) for d in range(2)]
            tails = [jnp.concatenate([a[:, i * LANES:(i + 1) * LANES] for i in range(PACKS)], axis=0) for a in tails]
            for p in [t % 2, 1 - t % 2]:
                pieces.append(block[:, p * half:(p + 1) * half].reshape(rows, kv_rank))
                packs += [jnp.where(part == p * groups + s, tails[d], 0.0).astype(jnp.bfloat16) for d in range(2) for s in range(groups)]
        c_all = jnp.concatenate(pieces, axis=0)
        krt = mm(same, jnp.concatenate(packs, axis=0), NT).astype(jnp.bfloat16)
        spots = [((t + i) % 2, (t - t % 2 + i) * rows, (2 * j + i) * rows) for j, t in enumerate(slots) for i in range(2)]
        for p, at, src in spots:
            krt_v[p, :, at:at + rows] = krt[:, src:src + rows]
        for c in range(pairs // 2):
            cols = slice(c * 2 * LANES, (c + 1) * 2 * LANES)
            k = mm(c_all, wuk_v[:, cols]).astype(jnp.bfloat16)
            for i in range(2):
                kt = k[:, i * LANES:(i + 1) * LANES].T
                for p, at, src in spots:
                    kt_v[2 * c + i, p, :, at:at + rows] = kt[:, src:src + rows]
        for c in range(pairs // 2):
            cols = slice(c * 2 * LANES, (c + 1) * 2 * LANES)
            v = mm(c_all, wuv_v[:, cols]).astype(jnp.bfloat16)
            for i in range(2):
                for p, at, src in spots:
                    v_v[2 * c + i, p, at:at + rows] = v[src:src + rows, i * LANES:(i + 1) * LANES]

    get_wuk.wait()
    get_wuv.wait()
    def receive(t):
        for d in range(2):
            push(2 * chip_at(t) + d, me, 0).wait_recv()

    even = jnp.logical_not(odd)
    push(partner, me, 0).wait_recv()
    pl.when(odd)(lambda: relay(1))
    pl.when(even)(lambda: receive(1))
    up_project([0, 1])

    @pl.when(odd)
    def _():
        for t in range(2, chips):
            relay(t)

    for t in range(2, chips):
        pl.when(even)(functools.partial(receive, t))
        up_project([t])

    factor = (nope + rope) ** -0.5 * math.log2(math.e)

    def scores(g):
        for i in range(GROUP):
            p = g * GROUP + i
            early = jnp.concatenate([kt_v[p, 0], krt_v[0]], axis=0)
            late = jnp.concatenate([kt_v[p, 1], krt_v[1]], axis=0)
            s_v[g % 2, i, :count] = mm(qcat[p], early) * factor + bias_v[:count]
            s_v[g % 2, i, count:] = mm(qcat[p, rows:], late) * factor + bias_v[count:]

    def halves(a, op):
        return op(a[:, :LANES], a[:, LANES:])

    def weights(g):
        for i in range(GROUP):
            a, b, c = s_v[g % 2, i, :rows], s_v[g % 2, i, rows:count], s_v[g % 2, i, count:]
            m_a = jnp.max(halves(a, jnp.maximum), axis=1, keepdims=True)
            m_b = jnp.max(jnp.maximum(halves(b, jnp.maximum), halves(c, jnp.maximum)), axis=1, keepdims=True)
            a, b, c = jnp.exp2(a - m_a), jnp.exp2(b - m_b), jnp.exp2(c - m_b)
            p_v[g % 2, i, :rows] = a.astype(jnp.bfloat16)
            p_v[g % 2, i, rows:count] = b.astype(jnp.bfloat16)
            p_v[g % 2, i, count:] = c.astype(jnp.bfloat16)
            l_a = jnp.sum(halves(a, jnp.add), axis=1, keepdims=True)
            l_b = jnp.sum(halves(b, jnp.add) + halves(c, jnp.add), axis=1, keepdims=True)
            l_v[g % 2, i, :rows] = jnp.broadcast_to(1.0 / l_a, (rows, LANES))
            l_v[g % 2, i, rows:] = jnp.broadcast_to(1.0 / l_b, (rows, LANES))

    def values(g):
        for i in range(GROUP):
            cols = slice((g * GROUP + i) * LANES, (g * GROUP + i + 1) * LANES)
            o = mm(p_v[g % 2, i, :count], v_v[g * GROUP + i, 0])
            o_a = o[:rows] * l_v[g % 2, i, :rows]
            o_b = (o[rows:] + mm(p_v[g % 2, i, count:], v_v[g * GROUP + i, 1])) * l_v[g % 2, i, rows:]
            o_v[:half, cols] = jnp.where(low[:half], o_a[:half], o_a[half:]).astype(jnp.bfloat16)
            o_v[half:, cols] = jnp.where(low[:half], o_b[:half], o_b[half:]).astype(jnp.bfloat16)

    def project(g):
        for c in range(width // panel):
            cols = slice(c * panel, (c + 1) * panel)
            y = mm(o_v[:, g * deep:(g + 1) * deep], wout_v[g * deep:(g + 1) * deep, cols])
            if g > 0:
                y += y_sum[:, cols]
            if g + 1 < steps:
                y_sum[:, cols] = y
            else:
                y_v[:, cols] = y.astype(jnp.bfloat16)

    for g in range(steps + 3):
        if g == 3:
            for get in get_wout:
                get.wait()
        if g >= 3:
            project(g - 3)
        if 2 <= g < steps + 2:
            values(g - 2)
        if 1 <= g <= steps:
            weights(g - 1)
        if g < steps:
            scores(g)
    for cp in sends:
        cp.wait_send()

    @pl.when(odd)
    def _():
        for t in range(1, chips):
            for cp in forward(t):
                cp.wait_send()


def solution(mesh):
    n = mesh.shape["ctx"]
    row_spec = P(("dp", "ctx"), None)
    id_spec = P(("dp", "ctx"))

    def per_device(x, pos, seg, w_dq, w_uq, w_qr, w_dkv, w_kr, w_uk, w_uv, w_out, gain_q, gain_kv):
        rows, width = x.shape
        pairs = w_uq.shape[1] // LANES
        keys = n * rows
        kv_rank = w_dkv.shape[1]
        rope = w_kr.shape[1]
        bf, f32 = jnp.bfloat16, jnp.float32
        args = (x, pos.reshape(1, rows), w_dq, w_uq, w_qr, w_dkv, w_kr.T, w_uk, w_uv, w_out,
                gain_q, gain_kv)
        scratch = [pltpu.VMEM(a.shape, a.dtype) for a in args]
        scratch += [
            pltpu.VMEM((n, rows + PACK_ROWS // PACKS, kv_rank), bf),
            pltpu.VMEM((2, rows, kv_rank), f32),
            pltpu.VMEM((rows, w_dq.shape[1]), bf),
            pltpu.VMEM((pairs, 2 * rows, LANES + rope), bf),
            pltpu.VMEM((pairs, 2, LANES, keys // 2), bf),
            pltpu.VMEM((2, rope, keys // 2), bf),
            pltpu.VMEM((pairs, 2, keys // 2, LANES), bf),
            pltpu.VMEM((3 * rows, keys // 2), f32),
            pltpu.VMEM((rows, w_uv.shape[1]), bf),
            pltpu.VMEM((2, GROUP, 3 * rows, keys // 2), f32),
            pltpu.VMEM((2, GROUP, 3 * rows, keys // 2), bf),
            pltpu.VMEM((2, GROUP, 2 * rows, LANES), f32),
            pltpu.VMEM((rows, width), f32),
            pltpu.SemaphoreType.DMA((len(args) - 2 + len(KV_CUTS) - 1 + pairs // GROUP,)),
            pltpu.SemaphoreType.DMA((n // 2 + n - 2,)),
            pltpu.SemaphoreType.DMA((n,)),
        ]
        return pl.pallas_call(
            functools.partial(layer_kernel, n),
            out_shape=pltpu.VMEM(x.shape, bf),
            in_specs=[pl.BlockSpec(memory_space=pltpu.HBM)] * len(args),
            out_specs=pl.BlockSpec(memory_space=pltpu.VMEM),
            scratch_shapes=scratch,
            compiler_params=pltpu.CompilerParams(collective_id=0, has_side_effects=True, vmem_limit_bytes=62000000),
        )(*args)

    return jax.shard_map(per_device, mesh=mesh, in_specs=(row_spec, id_spec, id_spec) + (P(),) * 10, out_specs=row_spec, check_vma=False)
```
